128 devices in a mesh: dp: 16 (over x_hi, z, core), tensor: 8 (over y, x_lo).
Axes of the slice: x: 4 (x_hi: 2, x_lo: 2; x = x_hi * 2 + x_lo), y: 4, z: 4, core: 2. Of those that a mesh axis runs over, the one named last changes fastest.
Arguments:
- latents: bfloat16 [176, 256, 640], P('dp', 'tensor'), may hold values from -6 to 6
- cotangent: bfloat16 [176, 256, 640], P('dp', 'tensor'), may hold values from -6 to 6
- trunc_steps: int32 [16], replicated, may hold values from 30 to 40, as said below
- timesteps: int32 [176], replicated, may hold values from 100 to 900
- tile_map: int32 [176], replicated, may hold values from 0 to 175, as said below
- gain: float32 [640], replicated, may hold values from 0.5 to 1.5
- w_value: bfloat16 [640, 2560], P(None, 'tensor'), may hold values from -0.25 to 0.25
- w_gate: bfloat16 [640, 2560], P(None, 'tensor'), may hold values from -0.25 to 0.25
- w_out: bfloat16 [640, 2560], P(None, 'tensor'), may hold values from -0.125 to 0.125
Outputs:
- placed_grad: bfloat16 [176, 256, 640], P('dp', 'tensor')
- grad_value: float32 [640, 2560], P('dp', 'tensor')
- grad_gate: float32 [640, 2560], P('dp', 'tensor')
- grad_out_proj: float32 [640, 2560], P('dp', 'tensor')
- grad_gain: float32 [640], replicated
The draws below stay inside these ranges and needn't reach their ends.
Inputs may be any that keep to these rules, and one draw needn't show every extreme that they name: trunc_steps lies in 30 to 40, so a prompt has 1 to 11 live slots, its lowest ones. tile_map is a permutation of 0 to 175. Output slots g * 11 to g * 11 + 10 form group g; the live items go to the lowest slots of the groups, and each group receives the floor or the ceiling of (number of live items) / 16 of them.
All inputs are finite; a program needn't handle non-finite values.
Results may differ from the reference program's by a relative error of at most 0.0068.
Values may be sent and summed in bfloat16 or wider, within the bound.
No kernel may reach another device: no remote copies, remote signals or barrier semaphores. Data moves between devices by JAX's collectives and lax.ppermute only.
A program may use at most 64 MiB of HBM per device.

```python
import jax
import jax.numpy as jnp
from jax import lax

C = 640
FI = 2560
ROWS = 256
SLOTS = 11
PROMPTS = 16
ITEMS = 176


def chain_plan(key):
    steps = jax.random.randint(jax.random.fold_in(key, 11), (PROMPTS,), 30, 41).astype(jnp.int32)
    item_ids = jnp.arange(ITEMS, dtype=jnp.int32)
    live = (item_ids % SLOTS < jnp.repeat(steps, SLOTS) - 29).astype(jnp.int32)
    shuffled = jax.random.permutation(jax.random.fold_in(key, 12), ITEMS).astype(jnp.int32)
    ranking = (1 - live) * ITEMS + shuffled
    ordering = jnp.argsort(ranking, stable=True).astype(jnp.int32)
    groups = ITEMS // SLOTS
    slot_of = item_ids % groups * SLOTS + item_ids // groups
    tile_map = jnp.zeros((ITEMS,), jnp.int32).at[ordering].set(slot_of.astype(jnp.int32))
    return (steps, tile_map)


def draw_trunc_steps(key, part):
    return chain_plan(key)[0]


def draw_tile_map(key, part):
    return chain_plan(key)[1]


def with_ends(result, own_key, low, top_value):
    longest = result.shape.index(max(result.shape))
    spots = []
    for shift in (0, 1):
        where = [jax.random.randint(jax.random.fold_in(own_key, axis), (), 0, length) for axis, length in enumerate(result.shape)]
        where[longest] = (where[longest] + shift) % result.shape[longest]
        spots.append(tuple(where))
    return result.at[spots[0]].set(low).at[spots[1]].set(top_value)


def block_scale(rng, extent, cuts, low, high):
    def one(dim, parts):
        draws = jax.random.uniform(jax.random.fold_in(jax.random.fold_in(rng, 6), dim), (parts,), jnp.float32, low / len(cuts), high / len(cuts))
        return jnp.repeat(jnp.exp(draws), extent[dim] // parts).reshape((-1,) + (1,) * (len(extent) - dim - 1))

    level = one(*cuts[0])
    for cut in cuts[1:]:
        level = level * one(*cut)
    return level


def bell_draw(stream_key, dims, scale, reach, cuts=(), held_as=jnp.bfloat16):
    drawn = scale * jax.random.normal(stream_key, dims, jnp.float32)
    if cuts:
        drawn = drawn * block_scale(stream_key, dims, cuts, -0.22, 0.18)
    return jnp.clip(drawn, -reach, reach).astype(held_as)


def setup_inputs(seed: int = 0) -> dict:
    key_of = jax.random.split(jax.random.key(seed), 10)
    return {
        "latents": bell_draw(key_of[0], (ITEMS, ROWS, C), 1.0, 6.0, ((0, 16), (1, 8))),
        "cotangent": bell_draw(key_of[1], (ITEMS, ROWS, C), 1.0, 6.0, ((0, 16), (1, 8))),
        "trunc_steps": draw_trunc_steps(jax.random.fold_in(key_of[9], 71), 0),
        "timesteps": with_ends(jax.random.randint(key_of[3], (ITEMS,), 100, 901), jax.random.fold_in(key_of[3], 1), 100, 900).astype(jnp.int32),
        "tile_map": draw_tile_map(jax.random.fold_in(key_of[9], 71), 0),
        "gain": jnp.clip(1.0 + 0.1 * jax.random.normal(key_of[5], (C,), jnp.float32), 0.5, 1.5),
        "w_value": bell_draw(key_of[6], (C, FI), C ** -0.5, 0.25, ((1, 8),)),
        "w_gate": bell_draw(key_of[7], (C, FI), C ** -0.5, 0.25, ((1, 8),)),
        "w_out": bell_draw(key_of[8], (C, FI), FI ** -0.5, 0.125, ((1, 8),)),
    }


eps = 1e-05

def alpha_bars():
    betas = jnp.linspace(0.00085 ** 0.5, 0.012 ** 0.5, 1000, dtype=jnp.float32) ** 2
    return jnp.exp(jnp.cumsum(jnp.log1p(-betas)))

def gelu_parts(inputs):
    cdf = 0.5 * (1.0 + lax.erf(inputs * 0.7071067811865476))
    density = jnp.exp(-0.5 * inputs * inputs) * 0.3989422804014327
    return (inputs * cdf, cdf + inputs * density)

def item_backward(normed, grad_tile, w_value, w_gate, w_out):
    values_proj = jnp.dot(normed, w_value, preferred_element_type=jnp.float32)
    gate_proj = jnp.dot(normed, w_gate, preferred_element_type=jnp.float32)
    gelu_gate, gelu_slope = gelu_parts(gate_proj)
    hidden = (values_proj * gelu_gate).astype(jnp.bfloat16)
    d_hidden = jnp.dot(grad_tile, w_out, preferred_element_type=jnp.float32)
    d_value = (d_hidden * gelu_gate).astype(jnp.bfloat16)
    d_gate = (d_hidden * values_proj * gelu_slope).astype(jnp.bfloat16)
    first_dims = (((0,), (0,)), ((), ()))
    last_dims = (((1,), (1,)), ((), ()))
    grad_wv = lax.dot_general(normed, d_value, first_dims, preferred_element_type=jnp.float32)
    grad_wg = lax.dot_general(normed, d_gate, first_dims, preferred_element_type=jnp.float32)
    grad_wo = lax.dot_general(grad_tile, hidden, first_dims, preferred_element_type=jnp.float32)
    d_normed = lax.dot_general(d_value, w_value, last_dims, preferred_element_type=jnp.float32)
    d_normed = d_normed + lax.dot_general(d_gate, w_gate, last_dims, preferred_element_type=jnp.float32)
    return (grad_wv, grad_wg, grad_wo, d_normed)

def reference(latents, cotangent, trunc_steps, timesteps, tile_map, gain, w_value, w_gate, w_out):
    total = latents.shape[0]
    item_ids = jnp.arange(total, dtype=jnp.int32)
    live = item_ids % SLOTS < jnp.repeat(trunc_steps, SLOTS) - 29
    noise_scale = jnp.sqrt(1.0 - alpha_bars()[timesteps])
    width = latents.shape[2]
    inner = w_value.shape[1]

    def one_item(carry, inputs):
        tile, cot_tile, item_scale, is_live = inputs
        x_float = tile.astype(jnp.float32)
        row_mean = lax.optimization_barrier(jnp.mean(x_float, axis=-1, keepdims=True))
        centred = x_float - row_mean
        row_var = lax.optimization_barrier(jnp.mean(centred * centred, axis=-1, keepdims=True))
        inv_std = lax.rsqrt(row_var + eps)
        x_hat = centred * inv_std
        normed = (x_hat * gain).astype(jnp.bfloat16)
        grad_tile = (cot_tile.astype(jnp.float32) * item_scale).astype(jnp.bfloat16)

        def run(unused):
            grad_wv, grad_wg, grad_wo, d_normed = item_backward(normed, grad_tile, w_value, w_gate, w_out)
            d_hat = d_normed * gain
            input_grad = grad_tile.astype(jnp.float32) + inv_std * (d_hat - lax.optimization_barrier(jnp.mean(d_hat, axis=-1, keepdims=True)) - x_hat * lax.optimization_barrier(jnp.mean(d_hat * x_hat, axis=-1, keepdims=True)))
            gain_part = lax.optimization_barrier(jnp.sum(d_normed * x_hat, axis=0))
            return (grad_wv, grad_wg, grad_wo, gain_part, input_grad.astype(jnp.bfloat16))

        def skip(unused):
            zero_w = jnp.zeros((width, inner), jnp.float32)
            return (zero_w, zero_w, zero_w, jnp.zeros((width,), jnp.float32), jnp.zeros(tile.shape, jnp.bfloat16))
        grad_wv, grad_wg, grad_wo, gain_part, input_grad = lax.cond(is_live, run, skip, None)
        carry = (carry[0] + grad_wv, carry[1] + grad_wg, carry[2] + grad_wo, carry[3] + gain_part)
        return (carry, input_grad)
    zero_w = jnp.zeros((width, inner), jnp.float32)
    init = (zero_w, zero_w, zero_w, jnp.zeros((width,), jnp.float32))
    sums, input_grads = lax.scan(one_item, init, (latents, cotangent, noise_scale, live))
    placed_grad = jnp.zeros(latents.shape, jnp.bfloat16).at[tile_map.astype(jnp.int32)].set(input_grads)
    return (placed_grad, sums[0], sums[1], sums[2], sums[3])
```

```python
import functools

import jax
import jax.numpy as jnp
import numpy as np
from jax import lax
from jax.experimental import pallas as pl
from jax.experimental.pallas import tpu as pltpu
from jax.sharding import Mesh
from jax.sharding import PartitionSpec as P


TENSOR = ("y", "xl")
DP = ("xh", "z", "c")
EPS = 1e-05
PLACES = 3
BF = jnp.bfloat16
F32 = jnp.float32

VMEM = pltpu.MemorySpace.VMEM
SMEM = pltpu.MemorySpace.SMEM


def noise_table():
    betas = np.linspace(0.00085**0.5, 0.012**0.5, 1000) ** 2
    abar = np.exp(np.cumsum(np.log1p(-betas)))
    return jnp.asarray(np.sqrt(1.0 - abar), F32)


def swap(x, axis):
    return lax.ppermute(x, axis, [(0, 1), (1, 0)])


def ring(x, axis, step):
    return lax.ppermute(x, axis, [(i, (i + step) % 4) for i in range(4)])


def vmem(n):
    return [pl.BlockSpec(memory_space=VMEM)] * n


def smem(n):
    return [pl.BlockSpec(memory_space=SMEM)] * n


def index_kernel(meta, trunc, tmap, dest_g, dest_r, src_p, src_r, most, cnt):
    me = meta[0]

    def clear(i, _):
        cnt[i] = 0
        return 0

    lax.fori_loop(0, 256, clear, 0)

    def prompt(p, top):
        alive = trunc[p] - 29

        def slot(k, top):
            m = tmap[p * 11 + k]
            g = lax.div(m, 11)
            s = m - g * 11
            live = k < alive
            at = p * 16 + g
            r = cnt[at]

            @pl.when(live)
            def _():
                cnt[at] = r + 1

            rank = jnp.where(live, r, -1)

            @pl.when(p == me)
            def _():
                dest_g[k] = g
                dest_r[k] = rank

            @pl.when(g == me)
            def _():
                src_p[s] = p
                src_r[s] = rank

            return jnp.maximum(top, rank + 1)

        return lax.fori_loop(0, 11, slot, top)

    most[0] = lax.fori_loop(0, 16, prompt, jnp.int32(0))


def index_work(meta, trunc, tmap):
    i11 = jax.ShapeDtypeStruct((11,), jnp.int32)
    return pl.pallas_call(
        index_kernel,
        out_shape=(i11, i11, i11, i11, jax.ShapeDtypeStruct((1,), jnp.int32)),
        in_specs=smem(3),
        out_specs=tuple(smem(5)),
        scratch_shapes=[pltpu.SMEM((256,), jnp.int32)],
        name="routes",
    )(meta, trunc, tmap)


def normalise(tile):
    x = tile.astype(F32)
    centred = x - jnp.mean(x, axis=-1, keepdims=True)
    inv_std = lax.rsqrt(jnp.mean(centred * centred, axis=-1, keepdims=True) + EPS)
    return centred * inv_std, inv_std


def prologue_kernel(meta, trunc, times, table, lat, cot, gain, wv, wg, wo, rows, wt, half):
    me = meta[0]
    alive = trunc[me] - 29
    for k in range(11):
        scale = jnp.where(k < alive, table[times[me * 11 + k]], 0.0)
        x_hat, _ = normalise(lat[k])
        rows[0, k] = (x_hat * gain[...]).astype(BF)
        rows[1, k] = (cot[k].astype(F32) * scale).astype(BF)
    for j, w in enumerate((wv, wg, wo)):
        wt[j] = w[...].T
    start = pl.multiple_of(meta[1] * 160, 16)
    half[...] = wt[:, pl.ds(start, 160), :]


def prologue(meta, trunc, times, table, lat, cot, gain, wv, wg, wo):
    return pl.pallas_call(
        prologue_kernel,
        out_shape=(
            jax.ShapeDtypeStruct((2, 11, 32, 640), BF),
            jax.ShapeDtypeStruct((3, 320, 640), BF),
            jax.ShapeDtypeStruct((3, 160, 640), BF),
        ),
        in_specs=smem(4) + vmem(6),
        out_specs=tuple(vmem(3)),
        name="prologue",
    )(meta, trunc, times, table, lat, cot, gain, wv, wg, wo)


def block_kernel(meta, n_ref, g_ref, wv, wg, wo, dn, mine, send, tn, tg, keep):
    step = pl.program_id(0)
    last = (((1,), (1,)), ((), ()))
    plain = (((1,), (0,)), ((), ()))

    def dot(a, b, dims):
        return lax.dot_general(a, b, dims, preferred_element_type=F32)

    @pl.when(step == 0)
    def _():
        tn[...] = n_ref[...].T
        tg[...] = g_ref[...].T

    normed = n_ref[...]
    grad = g_ref[...]
    value = dot(normed, wv[...], last)
    gate = dot(normed, wg[...], last)
    d_hidden = dot(grad, wo[...], last)
    cdf = 0.5 * (1.0 + lax.erf(gate * 0.7071067811865476))
    density = jnp.exp(-0.5 * gate * gate) * 0.3989422804014327
    gelu = gate * cdf
    hidden = (value * gelu).astype(BF)
    d_value = (d_hidden * gelu).astype(BF)
    d_gate = (d_hidden * value * (cdf + gate * density)).astype(BF)
    part = dot(d_value, wv[...], plain) + dot(d_gate, wg[...], plain)

    @pl.when(step == 0)
    def _():
        dn[...] = part

    @pl.when(step > 0)
    def _():
        dn[...] += part

    c = meta[1]
    for j, (left, right) in enumerate(((tn, d_value), (tn, d_gate), (tg, hidden))):
        keep[...] = dot(left[...], right, plain).reshape(8, 2, 40, 256)
        mine[j] = keep[:, c].astype(BF)
        send[j] = keep[:, 1 - c].astype(BF)


def block(meta, normed, grad, wv, wg, wo):
    whole = pl.BlockSpec((704, 640), lambda i: (0, 0))
    chunk = pl.BlockSpec((256, 640), lambda i: (i, 0))
    out = pl.BlockSpec((3, 8, 40, 256), lambda i: (0, 0, 0, i))
    return pl.pallas_call(
        block_kernel,
        grid=(5,),
        out_shape=(
            jax.ShapeDtypeStruct((704, 640), F32),
            jax.ShapeDtypeStruct((3, 8, 40, 1280), BF),
            jax.ShapeDtypeStruct((3, 8, 40, 1280), BF),
        ),
        in_specs=smem(1) + [whole, whole, chunk, chunk, chunk],
        out_specs=(whole, out, out),
        scratch_shapes=[
            pltpu.VMEM((640, 704), BF),
            pltpu.VMEM((640, 704), BF),
            pltpu.VMEM((8, 2, 40, 256), F32),
        ],
        compiler_params=pltpu.CompilerParams(vmem_limit_bytes=48 * 2**20),
        name="block",
    )(meta, normed, grad, wv, wg, wo)


def finish_kernel(dest_g, dest_r, dn, got, lat, grad, gain, own, packed, gain_sum):
    gsum = jnp.zeros((1, 640), F32)
    for k in range(11):
        x_hat, inv_std = normalise(lat[k])
        d_normed = dn[k] + got[k].astype(F32)
        gsum = gsum + jnp.sum(d_normed * x_hat, axis=0, keepdims=True)
        d_hat = d_normed * gain[...]
        out = grad[k].astype(F32) + inv_std * (
            d_hat
            - jnp.mean(d_hat, axis=-1, keepdims=True)
            - x_hat * jnp.mean(d_hat * x_hat, axis=-1, keepdims=True)
        )
        out = out.astype(BF)
        rank = dest_r[k]
        own[k] = jnp.where(rank >= 0, out, jnp.zeros_like(out))

        @pl.when((rank >= 0) & (rank < PLACES))
        def _():
            packed[dest_g[k] * PLACES + rank] = out

    gain_sum[...] = gsum


def finish(dest_g, dest_r, dn, got, lat, grad, gain):
    return pl.pallas_call(
        finish_kernel,
        out_shape=(
            jax.ShapeDtypeStruct((11, 32, 640), BF),
            jax.ShapeDtypeStruct((16 * PLACES, 32, 640), BF),
            jax.ShapeDtypeStruct((1, 640), F32),
        ),
        in_specs=smem(2) + vmem(5),
        out_specs=tuple(vmem(3)),
        name="finish",
    )(dest_g, dest_r, dn, got, lat, grad, gain)


def unpack_kernel(src_p, src_r, came, placed, blank, sems):
    blank[...] = jnp.zeros_like(blank)
    for s in range(11):
        rank = src_r[s]

        @pl.when((rank >= 0) & (rank < PLACES))
        def _():
            pltpu.make_async_copy(
                came.at[src_p[s] * PLACES + rank], placed.at[s], sems.at[s]
            ).start()

        @pl.when((rank < 0) | (rank >= PLACES))
        def _():
            pltpu.make_async_copy(blank, placed.at[s], sems.at[s]).start()

    for s in range(11):
        pltpu.make_async_copy(blank, placed.at[s], sems.at[s]).wait()


def unpack(src_p, src_r, came):
    return pl.pallas_call(
        unpack_kernel,
        out_shape=jax.ShapeDtypeStruct((11, 32, 640), BF),
        in_specs=smem(2) + [pl.BlockSpec(memory_space=pl.ANY)],
        out_specs=pl.BlockSpec(memory_space=pl.ANY),
        scratch_shapes=[pltpu.VMEM((32, 640), BF), pltpu.SemaphoreType.DMA((11,))],
        name="unpack",
    )(src_p, src_r, came)


def gather_weights(wt, half, c):
    below = ring(half, "y", 1)
    above = ring(half, "y", -1)
    far_lo = ring(below[:, :80], "y", 1)
    far_hi = ring(above[:, 80:], "y", -1)
    far = jnp.concatenate([far_lo, far_hi], axis=1)

    def joined(x):
        y = swap(x, "c")
        return jnp.where(
            c == 0, jnp.concatenate([x, y], axis=1), jnp.concatenate([y, x], axis=1)
        )

    return wt, joined(far), joined(above), joined(below)


def reduce_ring(near, axis, cut):
    own, far, up, down = near
    n = far.shape[cut] // 2

    def lo(x):
        return lax.slice_in_dim(x, 0, n, axis=cut)

    def hi(x):
        return lax.slice_in_dim(x, n, 2 * n, axis=cut)

    got_lo = ring(lo(far).astype(BF), axis, 1).astype(F32)
    got_hi = ring(hi(far).astype(BF), axis, -1).astype(F32)
    up = jnp.concatenate([lo(up) + got_lo, hi(up)], axis=cut).astype(BF)
    down = jnp.concatenate([lo(down), hi(down) + got_hi], axis=cut).astype(BF)
    return own + ring(up, axis, 1).astype(F32) + ring(down, axis, -1).astype(F32)


def reduce_weights(mine, send):
    both = mine.astype(F32) + swap(send, "c").astype(F32)
    own = reduce_ring([both[..., 320 * s : 320 * s + 320] for s in range(4)], "y", 1)
    own = own.reshape(3, 2, 4, 40, 320)
    z = lax.axis_index("z")
    near = [
        lax.dynamic_index_in_dim(own, (z + d) % 4, axis=2, keepdims=False) for d in (0, 2, 1, 3)
    ]
    own = reduce_ring(near, "z", 1)
    xh = lax.axis_index("xh")
    keep = lax.dynamic_index_in_dim(own, xh, axis=1, keepdims=False)
    give = lax.dynamic_index_in_dim(own, 1 - xh, axis=1, keepdims=False)
    return keep + swap(give.astype(BF), "xh").astype(F32)


def sum_everywhere(g):
    g = g + swap(g, "c")
    for axis in ("y", "z"):
        down = ring(g, axis, 1)
        up = ring(g, axis, -1)
        far = ring(down, axis, 1)
        g = (g + far) + (down + up)
    g = g + swap(g, "xh")
    return g + swap(g, "xl")


def route(packed):
    return lax.all_to_all(packed, DP, 0, 0, tiled=True)


def more_rounds(placed, own, most, dest_g, dest_r, src_p, src_r):
    def more(state):
        return state[0] * PLACES < most[0]

    def one(state):
        t, placed = state
        rank = dest_r - t * PLACES
        here = (rank >= 0) & (rank < PLACES) & (dest_r >= 0)
        place = jnp.where(here, dest_g * PLACES + rank, -1)
        hit = place[None, :] == jnp.arange(16 * PLACES, dtype=jnp.int32)[:, None]
        pick = jnp.sum(jnp.where(hit, jnp.arange(11, dtype=jnp.int32)[None, :], 0), axis=1)
        came = route(jnp.take(own, pick, axis=0))
        rank = src_r - t * PLACES
        here = (rank >= 0) & (rank < PLACES) & (src_r >= 0)
        new = jnp.take(came, jnp.where(here, src_p * PLACES + rank, 0), axis=0)
        return t + 1, jnp.where(here[:, None, None], new, placed)

    return lax.while_loop(more, one, (jnp.int32(1), placed))[1]


def per_device(latents, cotangent, trunc, times, tmap, gain, w_value, w_gate, w_out):
    c = lax.axis_index("c")
    meta = jnp.stack([lax.axis_index(DP), c]).astype(jnp.int32)
    gain = gain[None, :]
    dest_g, dest_r, src_p, src_r, most = index_work(meta, trunc, tmap)
    rows, wt, half = prologue(
        meta, trunc, times, noise_table(), latents, cotangent, gain, w_value, w_gate, w_out
    )
    other = swap(rows, "xl")
    shards = gather_weights(wt, half, c)
    wv, wg, wo = (jnp.concatenate([s[j] for s in shards], axis=0) for j in range(3))
    both = jnp.concatenate([rows.reshape(2, 352, 640), other.reshape(2, 352, 640)], axis=1)
    dn, mine, send = block(meta, both[0], both[1], wv, wg, wo)
    dn = dn.reshape(2, 11, 32, 640)
    got = swap(dn[1].astype(BF), "xl")
    own, packed, gain_sum = finish(dest_g, dest_r, dn[0], got, latents, rows[1], gain)
    placed = unpack(src_p, src_r, route(packed))
    placed = more_rounds(placed, own, most, dest_g, dest_r, src_p, src_r)
    grads = reduce_weights(mine, send)
    return placed, grads[0], grads[1], grads[2], sum_everywhere(gain_sum)[0]


def solution(mesh):
    split = Mesh(mesh.devices.reshape(2, 4, 2, 4, 2), ("xh", "z", "c", "y", "xl"))
    tiles = P(DP, TENSOR, None)
    weights = P(None, TENSOR)
    return jax.shard_map(
        per_device,
        mesh=split,
        in_specs=(tiles, tiles, P(), P(), P(), P(), weights, weights, weights),
        out_specs=(tiles, P(DP, TENSOR), P(DP, TENSOR), P(DP, TENSOR), P()),
        check_vma=False,
    )
```

```python
import functools

import jax
import jax.numpy as jnp
import numpy as np
from jax import lax
from jax.experimental import pallas as pl
from jax.experimental.pallas import tpu as pltpu
from jax.sharding import Mesh
from jax.sharding import PartitionSpec as P


TENSOR = ("y", "xl")
DP = ("xh", "z", "c")
EPS = 1e-05
PLACES = 3
BF = jnp.bfloat16
F32 = jnp.float32

VMEM = pltpu.MemorySpace.VMEM
SMEM = pltpu.MemorySpace.SMEM


def noise_table():
    betas = np.linspace(0.00085**0.5, 0.012**0.5, 1000) ** 2
    abar = np.exp(np.cumsum(np.log1p(-betas)))
    return jnp.asarray(np.sqrt(1.0 - abar), F32)


def swap(x, axis):
    return lax.ppermute(x, axis, [(0, 1), (1, 0)])


def ring(x, axis, step):
    return lax.ppermute(x, axis, [(i, (i + step) % 4) for i in range(4)])


def vmem(n):
    return [pl.BlockSpec(memory_space=VMEM)] * n


def smem(n):
    return [pl.BlockSpec(memory_space=SMEM)] * n


def index_kernel(meta, trunc, tmap, dest_g, dest_r, src_p, src_r, most, cnt):
    me = meta[0]

    def clear(i, _):
        cnt[i] = 0
        return 0

    lax.fori_loop(0, 256, clear, 0)

    def prompt(p, top):
        alive = trunc[p] - 29

        def slot(k, top):
            m = tmap[p * 11 + k]
            g = lax.div(m, 11)
            s = m - g * 11
            live = k < alive
            at = p * 16 + g
            r = cnt[at]

            @pl.when(live)
            def _():
                cnt[at] = r + 1

            rank = jnp.where(live, r, -1)

            @pl.when(p == me)
            def _():
                dest_g[k] = g
                dest_r[k] = rank

            @pl.when(g == me)
            def _():
                src_p[s] = p
                src_r[s] = rank

            return jnp.maximum(top, rank + 1)

        return lax.fori_loop(0, 11, slot, top)

    most[0] = lax.fori_loop(0, 16, prompt, jnp.int32(0))


def index_work(meta, trunc, tmap):
    i11 = jax.ShapeDtypeStruct((11,), jnp.int32)
    return pl.pallas_call(
        index_kernel,
        out_shape=(i11, i11, i11, i11, jax.ShapeDtypeStruct((1,), jnp.int32)),
        in_specs=smem(3),
        out_specs=tuple(smem(5)),
        scratch_shapes=[pltpu.SMEM((256,), jnp.int32)],
        name="routes",
    )(meta, trunc, tmap)


def halves_kernel(meta, wv, wg, wo, half, sems):
    start = pl.multiple_of(meta[1] * 160, 16)
    copies = [
        pltpu.make_async_copy(w.at[pl.ds(start, 160), :], half.at[j], sems.at[j])
        for j, w in enumerate((wv, wg, wo))
    ]
    for copy in copies:
        copy.start()
    for copy in copies:
        copy.wait()


def halves(meta, wv, wg, wo):
    anywhere = pl.BlockSpec(memory_space=pl.ANY)
    return pl.pallas_call(
        halves_kernel,
        out_shape=jax.ShapeDtypeStruct((3, 160, 640), BF),
        in_specs=smem(1) + [anywhere] * 3,
        out_specs=anywhere,
        scratch_shapes=[pltpu.SemaphoreType.DMA((3,))],
        name="halves",
    )(meta, wv, wg, wo)


def normalise(tile):
    x = tile.astype(F32)
    centred = x - jnp.mean(x, axis=-1, keepdims=True)
    inv_std = lax.rsqrt(jnp.mean(centred * centred, axis=-1, keepdims=True) + EPS)
    return centred * inv_std, inv_std


def prologue_kernel(meta, trunc, times, table, lat, cot, gain, rows):
    me = meta[0]
    alive = trunc[me] - 29
    for k in range(11):
        scale = jnp.where(k < alive, table[times[me * 11 + k]], 0.0)
        x_hat, _ = normalise(lat[k])
        rows[0, k] = (x_hat * gain[...]).astype(BF)
        rows[1, k] = (cot[k].astype(F32) * scale).astype(BF)


def prologue(meta, trunc, times, table, lat, cot, gain):
    return pl.pallas_call(
        prologue_kernel,
        out_shape=jax.ShapeDtypeStruct((2, 11, 32, 640), BF),
        in_specs=smem(4) + vmem(3),
        out_specs=vmem(1)[0],
        name="prologue",
    )(meta, trunc, times, table, lat, cot, gain)


LAST = (((1,), (1,)), ((), ()))
PLAIN = (((1,), (0,)), ((), ()))


def dot(a, b, dims=PLAIN):
    return lax.dot_general(a, b, dims, preferred_element_type=F32)


def load_rows(own, other, rows, turned):
    for j in range(2):
        rows[j, :352] = own[j]
        rows[j, 352:] = other[j]
        turned[j] = rows[j].T


def hidden_part(rows, w, acts, start, width):
    span = slice(start, start + width)
    value = dot(rows[0], w[0, span], LAST)
    gate = dot(rows[0], w[1, span], LAST)
    d_hidden = dot(rows[1], w[2, span], LAST)
    cdf = 0.5 * (1.0 + lax.erf(gate * 0.7071067811865476))
    density = jnp.exp(-0.5 * gate * gate) * 0.3989422804014327
    gelu = gate * cdf
    acts[0, :, span] = (d_hidden * gelu).astype(BF)
    acts[1, :, span] = (d_hidden * value * (cdf + gate * density)).astype(BF)
    acts[2, :, span] = (value * gelu).astype(BF)


def near_kernel(meta, own, other, wv, wg, wo, below, below2, above, above2, dn, mine, send,
                rows, turned, w, acts, keep):
    c = meta[1]
    here = pl.multiple_of(c * 160, 16)
    there = pl.multiple_of((1 - c) * 160, 16)
    load_rows(own, other, rows, turned)
    for j, ref in enumerate((wv, wg, wo)):
        w[j, :320] = ref[...]
        w[j, pl.ds(320 + here, 160)] = above[j]
        w[j, pl.ds(320 + there, 160)] = above2[j]
        w[j, pl.ds(640 + here, 160)] = below[j]
        w[j, pl.ds(640 + there, 160)] = below2[j]
    for start, width in ((0, 256), (256, 256), (512, 256), (768, 192)):
        hidden_part(rows, w, acts, start, width)
    dn[...] = dot(acts[0], w[0]) + dot(acts[1], w[1])
    for j in range(3):
        keep[...] = dot(turned[j // 2], acts[j]).reshape(8, 2, 40, 960)
        for out, side in ((mine, c), (send, 1 - c)):
            both = keep[:, side].reshape(320, 960)
            out[0, j] = both[:, :320].reshape(8, 40, 320).astype(BF)
            mid = pltpu.roll(both[:, 256:640], 320, 1)[:, :320]
            out[1, j] = mid.reshape(8, 40, 320).astype(BF)
            out[2, j] = both[:, 640:].reshape(8, 40, 320).astype(BF)


def near_block(meta, own, other, wv, wg, wo, below, below2, above, above2):
    grads = jax.ShapeDtypeStruct((3, 3, 8, 40, 320), BF)
    return pl.pallas_call(
        near_kernel,
        out_shape=(jax.ShapeDtypeStruct((704, 640), F32), grads, grads),
        in_specs=smem(1) + vmem(9),
        out_specs=tuple(vmem(3)),
        scratch_shapes=[
            pltpu.VMEM((2, 704, 640), BF),
            pltpu.VMEM((2, 640, 704), BF),
            pltpu.VMEM((3, 960, 640), BF),
            pltpu.VMEM((3, 704, 960), BF),
            pltpu.VMEM((8, 2, 40, 960), F32),
        ],
        compiler_params=pltpu.CompilerParams(vmem_limit_bytes=56 * 2**20),
        name="near_block",
    )(meta, own, other, wv, wg, wo, below, below2, above, above2)


def split_gain(g):
    g = jnp.broadcast_to(g, (8, 640))
    low = g[:, :320]
    high = pltpu.roll(g[:, 256:], 320, 1)[:, :320]
    row = lax.broadcasted_iota(jnp.int32, (8, 320), 0)
    value = jnp.where(row % 2 == 0, low, high)
    top = value.astype(BF).astype(F32)
    return jnp.where(row < 2, top, jnp.where(row < 4, value - top, 0.0))


def resplit(pair):
    top = pair.astype(BF).astype(F32)
    return jnp.concatenate([top, pair - top, jnp.zeros((4, 320), F32)], axis=0)


def joined(rows):
    rows = rows.astype(F32)
    return rows[0:2] + rows[2:4]


def far_kernel(meta, own, other, gain, near_dn, first, second, dn, dn_send, mine, send,
               rows, turned, w, acts, keep):
    c = meta[1]
    here = pl.multiple_of(c * 160, 16)
    there = pl.multiple_of((1 - c) * 160, 16)
    load_rows(own, other, rows, turned)
    for j in range(3):
        w[j, pl.ds(here, 160)] = first[j]
        w[j, pl.ds(there, 160)] = second[j]
    hidden_part(rows, w, acts, 0, 320)
    total = near_dn[...] + dot(acts[0], w[0]) + dot(acts[1], w[1])
    dn[...] = total[:352]
    dn_send[...] = total[352:].astype(BF)
    gsum = jnp.sum(total * rows[0].astype(F32), axis=0, keepdims=True) / gain[...]
    tail = split_gain(gsum).astype(BF)
    for j in range(3):
        keep[...] = dot(turned[j // 2], acts[j]).reshape(8, 2, 40, 320)
        for out, side in ((mine, c), (send, 1 - c)):
            out[320 * j : 320 * j + 320] = keep[:, side].reshape(320, 320).astype(BF)
    mine[960:] = tail
    send[960:] = tail


def far_block(meta, own, other, gain, near_dn, first, second):
    grads = jax.ShapeDtypeStruct((968, 320), BF)
    return pl.pallas_call(
        far_kernel,
        out_shape=(
            jax.ShapeDtypeStruct((352, 640), F32),
            jax.ShapeDtypeStruct((352, 640), BF),
            grads,
            grads,
        ),
        in_specs=smem(1) + vmem(6),
        out_specs=tuple(vmem(4)),
        scratch_shapes=[
            pltpu.VMEM((2, 704, 640), BF),
            pltpu.VMEM((2, 640, 704), BF),
            pltpu.VMEM((3, 320, 640), BF),
            pltpu.VMEM((3, 704, 320), BF),
            pltpu.VMEM((8, 2, 40, 320), F32),
        ],
        compiler_params=pltpu.CompilerParams(vmem_limit_bytes=56 * 2**20),
        name="far_block",
    )(meta, own, other, gain, near_dn, first, second)


def finish_kernel(dest_g, dest_r, dn, got, lat, grad, gain, own, packed, sems):
    def sent(k):
        rank = dest_r[k]
        return (rank >= 0) & (rank < PLACES)

    for k in range(11):
        x_hat, inv_std = normalise(lat[k])
        d_hat = (dn[k] + got[k].astype(F32)) * gain[...]
        out = grad[k].astype(F32) + inv_std * (
            d_hat
            - jnp.mean(d_hat, axis=-1, keepdims=True)
            - x_hat * jnp.mean(d_hat * x_hat, axis=-1, keepdims=True)
        )
        own[k] = jnp.where(dest_r[k] >= 0, out, 0.0).astype(BF)

        @pl.when(sent(k))
        def _():
            place = dest_g[k] * PLACES + dest_r[k]
            pltpu.make_async_copy(own.at[k], packed.at[place], sems.at[k]).start()

    for k in range(11):

        @pl.when(sent(k))
        def _():
            pltpu.make_async_copy(own.at[k], packed.at[0], sems.at[k]).wait()


def finish(dest_g, dest_r, dn, got, lat, grad, gain):
    return pl.pallas_call(
        finish_kernel,
        out_shape=(
            jax.ShapeDtypeStruct((11, 32, 640), BF),
            jax.ShapeDtypeStruct((16 * PLACES, 32, 640), BF),
        ),
        in_specs=smem(2) + vmem(5),
        out_specs=(vmem(1)[0], pl.BlockSpec(memory_space=pl.ANY)),
        scratch_shapes=[pltpu.SemaphoreType.DMA((11,))],
        name="finish",
    )(dest_g, dest_r, dn, got, lat, grad, gain)


def unpack_kernel(src_p, src_r, came, placed, blank, sems):
    blank[...] = jnp.zeros_like(blank)
    for s in range(11):
        rank = src_r[s]

        @pl.when((rank >= 0) & (rank < PLACES))
        def _():
            pltpu.make_async_copy(
                came.at[src_p[s] * PLACES + rank], placed.at[s], sems.at[s]
            ).start()

        @pl.when((rank < 0) | (rank >= PLACES))
        def _():
            pltpu.make_async_copy(blank, placed.at[s], sems.at[s]).start()

    for s in range(11):
        pltpu.make_async_copy(blank, placed.at[s], sems.at[s]).wait()


def unpack(src_p, src_r, came):
    return pl.pallas_call(
        unpack_kernel,
        out_shape=jax.ShapeDtypeStruct((11, 32, 640), BF),
        in_specs=smem(2) + [pl.BlockSpec(memory_space=pl.ANY)],
        out_specs=pl.BlockSpec(memory_space=pl.ANY),
        scratch_shapes=[pltpu.VMEM((32, 640), BF), pltpu.SemaphoreType.DMA((11,))],
        name="unpack",
    )(src_p, src_r, came)


def local(kernel, out_shapes, name, scalars, *arrays):
    return pl.pallas_call(
        kernel,
        out_shape=tuple(jax.ShapeDtypeStruct(s, d) for s, d in out_shapes),
        in_specs=smem(1) + vmem(len(arrays)),
        out_specs=tuple(vmem(len(out_shapes))),
        name=name,
    )(scalars, *arrays)


def over_cores_kernel(meta, mine, got, lower, upper):
    both = (mine[:960].astype(F32) + got[:960].astype(F32)).reshape(3, 8, 40, 320)
    tail = resplit(joined(mine[960:]) + joined(got[960:])).astype(BF)
    lower[:480] = both[:, :4].reshape(480, 320).astype(BF)
    upper[:480] = both[:, 4:].reshape(480, 320).astype(BF)
    lower[480:] = tail
    upper[480:] = tail


def near_sums_kernel(meta, mine, got, from_down, from_up, up, down):
    for out, s, came, half in ((up, 1, from_down, 0), (down, 2, from_up, 4)):
        for j in range(3):
            x = mine[s, j].astype(F32) + got[s, j].astype(F32)
            add = came[160 * j : 160 * j + 160].astype(F32).reshape(4, 40, 320)
            keep = slice(4 - half, 8 - half)
            at = 320 * j + 40 * half
            out[at : at + 160] = (x[half : half + 4] + add).reshape(160, 320).astype(BF)
            at = 320 * j + 160 - 40 * half
            out[at : at + 160] = x[keep].reshape(160, 320).astype(BF)
    up[960:] = from_down[480:]
    down[960:] = from_up[480:]


def own_y_kernel(meta, mine, got, ring_down, ring_up, tail_own, tail_down, tail_up,
                 own, lower, upper, tail):
    x = mine[0].astype(F32) + got[0].astype(F32)
    x = x + ring_down[:960].astype(F32).reshape(3, 8, 40, 320)
    x = x + ring_up[:960].astype(F32).reshape(3, 8, 40, 320)
    own[...] = x.reshape(3, 2, 4, 40, 320)
    gain = joined(tail_own[480:]) + joined(ring_down[960:])
    gain = gain + (joined(tail_down[480:]) + joined(tail_up[480:]))
    rows = resplit(gain).astype(BF)
    far = lax.rem(meta[2] + 2, 4)
    lower[:120] = own[:, 0, far].reshape(120, 320).astype(BF)
    upper[:120] = own[:, 1, far].reshape(120, 320).astype(BF)
    lower[120:] = rows
    upper[120:] = rows
    tail[...] = rows


def near_z_kernel(meta, own, from_down, from_up, up, down):
    for out, step, came, half in ((up, 1, from_down, 0), (down, 3, from_up, 1)):
        at = lax.rem(meta[2] + step, 4)
        for j in range(3):
            add = came[40 * j : 40 * j + 40].astype(F32)
            out[80 * j + 40 * half : 80 * j + 40 * half + 40] = (own[j, half, at] + add).astype(BF)
            out[80 * j + 40 - 40 * half : 80 * j + 80 - 40 * half] = own[j, 1 - half, at].astype(BF)
    up[240:] = from_down[120:]
    down[240:] = from_up[120:]


def own_z_kernel(meta, own, ring_down, ring_up, tail_own, tail_down, tail_up, keep, give, sums):
    sums[...] = own[:, :, meta[2]]
    sums[...] += ring_down[:240].astype(F32).reshape(3, 2, 40, 320)
    sums[...] += ring_up[:240].astype(F32).reshape(3, 2, 40, 320)
    gain = joined(tail_own[...]) + joined(ring_down[240:])
    gain = gain + (joined(tail_down[120:]) + joined(tail_up[120:]))
    rows = resplit(gain)
    keep[:120] = sums[:, meta[3]].reshape(120, 320)
    give[:120] = sums[:, 1 - meta[3]].reshape(120, 320).astype(BF)
    keep[120:] = rows
    give[120:] = rows.astype(BF)


def last_kernel(meta, keep, got, value, gate, out, tail):
    for j, ref in enumerate((value, gate, out)):
        ref[...] = keep[40 * j : 40 * j + 40] + got[40 * j : 40 * j + 40].astype(F32)
    tail[...] = resplit(joined(keep[120:]) + joined(got[120:]))


def reduce_weights(meta, near_mine, near_got, far_mine, far_got):
    half = ((488, 320), BF)
    whole = ((968, 320), BF)
    lower, upper = local(over_cores_kernel, (half, half), "over_cores", meta, far_mine, far_got)
    from_down = ring(lower, "y", 1)
    from_up = ring(upper, "y", -1)
    up, down = local(
        near_sums_kernel, (whole, whole), "near_sums", meta, near_mine, near_got, from_down, from_up
    )
    ring_down = ring(up, "y", 1)
    ring_up = ring(down, "y", -1)
    z_half = ((128, 320), BF)
    own, lower, upper, tail = local(
        own_y_kernel,
        (((3, 2, 4, 40, 320), F32), z_half, z_half, ((8, 320), BF)),
        "own_y", meta, near_mine, near_got, ring_down, ring_up, lower, from_down, from_up,
    )
    from_down = ring(lower, "z", 1)
    from_up = ring(upper, "z", -1)
    z_whole = ((248, 320), BF)
    up, down = local(near_z_kernel, (z_whole, z_whole), "near_z", meta, own, from_down, from_up)
    ring_down = ring(up, "z", 1)
    ring_up = ring(down, "z", -1)
    keep, give, _ = local(
        own_z_kernel,
        (((128, 320), F32), ((128, 320), BF), ((3, 2, 40, 320), F32)),
        "own_z", meta, own, ring_down, ring_up, tail, from_down, from_up,
    )
    got = swap(give, "xh")
    out = ((40, 320), F32)
    value, gate, proj, tail = local(
        last_kernel, (out, out, out, ((8, 320), F32)), "last", meta, keep, got
    )
    tail = tail + swap(tail, "xl")
    return value, gate, proj, (tail[0:2] + tail[2:4]).reshape(640)


def route(packed):
    return lax.all_to_all(packed, DP, 0, 0, tiled=True)


def more_rounds(placed, own, most, dest_g, dest_r, src_p, src_r):
    def more(state):
        return state[0] * PLACES < most[0]

    def one(state):
        t, placed = state
        rank = dest_r - t * PLACES
        here = (rank >= 0) & (rank < PLACES) & (dest_r >= 0)
        place = jnp.where(here, dest_g * PLACES + rank, -1)
        hit = place[None, :] == jnp.arange(16 * PLACES, dtype=jnp.int32)[:, None]
        pick = jnp.sum(jnp.where(hit, jnp.arange(11, dtype=jnp.int32)[None, :], 0), axis=1)
        came = route(jnp.take(own, pick, axis=0))
        rank = src_r - t * PLACES
        here = (rank >= 0) & (rank < PLACES) & (src_r >= 0)
        new = jnp.take(came, jnp.where(here, src_p * PLACES + rank, 0), axis=0)
        return t + 1, jnp.where(here[:, None, None], new, placed)

    return lax.while_loop(more, one, (jnp.int32(1), placed))[1]


def per_device(latents, cotangent, trunc, times, tmap, gain, w_value, w_gate, w_out):
    meta = jnp.stack([lax.axis_index(a) for a in (DP, "c", "z", "xh")]).astype(jnp.int32)
    gain = gain[None, :]
    wv, wg, wo = w_value.T, w_gate.T, w_out.T
    half = halves(meta, wv, wg, wo)
    below = ring(half, "y", 1)
    above = ring(half, "y", -1)
    rows = prologue(meta, trunc, times, noise_table(), latents, cotangent, gain)
    other = swap(rows, "xl")
    routes = index_work(meta, trunc, tmap)
    below, above, routes = lax.optimization_barrier((below, above, routes))
    dest_g, dest_r, src_p, src_r, most = routes
    below2 = swap(below, "c")
    above2 = swap(above, "c")
    first = ring(below, "y", 1)
    second = ring(above2, "y", -1)
    rows2 = rows.reshape(2, 352, 640)
    other = other.reshape(2, 352, 640)
    near_dn, near_mine, near_send = near_block(
        meta, rows2, other, wv, wg, wo, below, below2, above, above2
    )
    near_got = swap(near_send, "c")
    dn, dn_send, far_mine, far_send = far_block(meta, rows2, other, gain, near_dn, first, second)
    got = swap(dn_send, "xl")
    far_got = swap(far_send, "c")
    tiles = (11, 32, 640)
    own, packed = finish(
        dest_g, dest_r, dn.reshape(tiles), got.reshape(tiles), latents, rows[1], gain
    )
    placed = unpack(src_p, src_r, route(packed))
    placed = more_rounds(placed, own, most, dest_g, dest_r, src_p, src_r)
    grads = reduce_weights(meta, near_mine, near_got, far_mine, far_got)
    return placed, *grads


def solution(mesh):
    split = Mesh(mesh.devices.reshape(2, 4, 2, 4, 2), ("xh", "z", "c", "y", "xl"))
    tiles = P(DP, TENSOR, None)
    weights = P(None, TENSOR)
    return jax.shard_map(
        per_device,
        mesh=split,
        in_specs=(tiles, tiles, P(), P(), P(), P(), weights, weights, weights),
        out_specs=(tiles, P(DP, TENSOR), P(DP, TENSOR), P(DP, TENSOR), P()),
        check_vma=False,
    )
```

```python
import jax
import jax.numpy as jnp
import numpy as np
from jax import lax
from jax.experimental import pallas as pl
from jax.experimental.pallas import tpu as pltpu
from jax.sharding import Mesh
from jax.sharding import PartitionSpec as P


TENSOR = ("y", "xl")
DP = ("xh", "z", "c")
EPS = 1e-05
PLACES = 3
BF = jnp.bfloat16
F32 = jnp.float32

VMEM = pltpu.MemorySpace.VMEM
SMEM = pltpu.MemorySpace.SMEM


def noise_table():
    betas = np.linspace(0.00085**0.5, 0.012**0.5, 1000) ** 2
    abar = np.exp(np.cumsum(np.log1p(-betas)))
    return jnp.asarray(np.sqrt(1.0 - abar), F32)


def swap(x, axis):
    return lax.ppermute(x, axis, [(0, 1), (1, 0)])


def ring(x, axis, step):
    return lax.ppermute(x, axis, [(i, (i + step) % 4) for i in range(4)])


def vmem(n):
    return [pl.BlockSpec(memory_space=VMEM)] * n


def smem(n):
    return [pl.BlockSpec(memory_space=SMEM)] * n


def index_kernel(meta, trunc, tmap, dest_g, dest_r, src_p, src_r, most, cnt):
    me = meta[0]

    def clear(i, _):
        cnt[i] = 0
        return 0

    lax.fori_loop(0, 256, clear, 0)

    def prompt(p, top):
        alive = trunc[p] - 29

        def slot(k, top):
            m = tmap[p * 11 + k]
            g = lax.div(m, 11)
            s = m - g * 11
            live = k < alive
            at = p * 16 + g
            r = cnt[at]

            @pl.when(live)
            def _():
                cnt[at] = r + 1

            rank = jnp.where(live, r, -1)

            @pl.when(p == me)
            def _():
                dest_g[k] = g
                dest_r[k] = rank

            @pl.when(g == me)
            def _():
                src_p[s] = p
                src_r[s] = rank

            return jnp.maximum(top, rank + 1)

        return lax.fori_loop(0, 11, slot, top)

    most[0] = lax.fori_loop(0, 16, prompt, jnp.int32(0))


def index_work(meta, trunc, tmap):
    i11 = jax.ShapeDtypeStruct((11,), jnp.int32)
    return pl.pallas_call(
        index_kernel,
        out_shape=(i11, i11, i11, i11, jax.ShapeDtypeStruct((1,), jnp.int32)),
        in_specs=smem(3),
        out_specs=tuple(smem(5)),
        scratch_shapes=[pltpu.SMEM((256,), jnp.int32)],
        name="routes",
    )(meta, trunc, tmap)


def halves_kernel(meta, wv, wg, wo, half):
    for j, w in enumerate((wv, wg, wo)):
        half[j] = w[...]


def halves(meta, wv, wg, wo):
    mine = pl.BlockSpec((160, 640), lambda i, meta: (meta[1], 0))
    return pl.pallas_call(
        halves_kernel,
        grid_spec=pltpu.PrefetchScalarGridSpec(
            num_scalar_prefetch=1,
            grid=(1,),
            in_specs=[mine] * 3,
            out_specs=pl.BlockSpec((3, 160, 640), lambda i, meta: (0, 0, 0)),
        ),
        out_shape=jax.ShapeDtypeStruct((3, 160, 640), BF),
        name="halves",
    )(meta, wv, wg, wo)


def normalise(tile):
    x = tile.astype(F32)
    centred = x - jnp.mean(x, axis=-1, keepdims=True)
    inv_std = lax.rsqrt(jnp.mean(centred * centred, axis=-1, keepdims=True) + EPS)
    return centred * inv_std, inv_std


def prologue_kernel(meta, trunc, times, table, lat, cot, gain, rows):
    me = meta[0]
    alive = trunc[me] - 29
    for k in range(11):
        scale = jnp.where(k < alive, table[times[me * 11 + k]], 0.0)
        x_hat, _ = normalise(lat[k])
        rows[0, k] = (x_hat * gain[...]).astype(BF)
        rows[1, k] = (cot[k].astype(F32) * scale).astype(BF)


def prologue(meta, trunc, times, table, lat, cot, gain):
    return pl.pallas_call(
        prologue_kernel,
        out_shape=jax.ShapeDtypeStruct((2, 11, 32, 640), BF),
        in_specs=smem(4) + vmem(3),
        out_specs=vmem(1)[0],
        name="prologue",
    )(meta, trunc, times, table, lat, cot, gain)


LAST = (((1,), (1,)), ((), ()))
PLAIN = (((1,), (0,)), ((), ()))


def dot(a, b, dims=PLAIN):
    return lax.dot_general(a, b, dims, preferred_element_type=F32)


def load_rows(own, other, rows, turned):
    for j in range(2):
        rows[j, :352] = own[j]
        rows[j, 352:] = other[j]
        turned[j] = rows[j].T


def hidden_part(rows, w, acts, start, width):
    span = slice(start, start + width)
    value = dot(rows[0], w[0, span], LAST)
    gate = dot(rows[0], w[1, span], LAST)
    d_hidden = dot(rows[1], w[2, span], LAST)
    cdf = 0.5 * (1.0 + lax.erf(gate * 0.7071067811865476))
    density = jnp.exp(-0.5 * gate * gate) * 0.3989422804014327
    gelu = gate * cdf
    acts[0, :, span] = (d_hidden * gelu).astype(BF)
    acts[1, :, span] = (d_hidden * value * (cdf + gate * density)).astype(BF)
    acts[2, :, span] = (value * gelu).astype(BF)


def near_kernel(meta, own, other, wv, wg, wo, below, below2, above, above2, dn, mine, send,
                rows, turned, w, acts, keep):
    c = meta[1]
    here = pl.multiple_of(c * 160, 16)
    there = pl.multiple_of((1 - c) * 160, 16)
    load_rows(own, other, rows, turned)
    for j, ref in enumerate((wv, wg, wo)):
        w[j, :320] = ref[...]
        w[j, pl.ds(320 + here, 160)] = above[j]
        w[j, pl.ds(320 + there, 160)] = above2[j]
        w[j, pl.ds(640 + here, 160)] = below[j]
        w[j, pl.ds(640 + there, 160)] = below2[j]
    for start, width in ((0, 256), (256, 256), (512, 256), (768, 192)):
        hidden_part(rows, w, acts, start, width)
    dn[...] = dot(acts[0], w[0]) + dot(acts[1], w[1])
    for j in range(3):
        keep[...] = dot(turned[j // 2], acts[j]).reshape(8, 2, 40, 960)
        for out, side in ((mine, c), (send, 1 - c)):
            both = keep[:, side].reshape(320, 960)
            out[0, j] = both[:, :320].reshape(8, 40, 320).astype(BF)
            mid = pltpu.roll(both[:, 256:640], 320, 1)[:, :320]
            out[1, j] = mid.reshape(8, 40, 320).astype(BF)
            out[2, j] = both[:, 640:].reshape(8, 40, 320).astype(BF)


def near_block(meta, own, other, wv, wg, wo, below, below2, above, above2):
    grads = jax.ShapeDtypeStruct((3, 3, 8, 40, 320), BF)
    return pl.pallas_call(
        near_kernel,
        out_shape=(jax.ShapeDtypeStruct((704, 640), F32), grads, grads),
        in_specs=smem(1) + vmem(9),
        out_specs=tuple(vmem(3)),
        scratch_shapes=[
            pltpu.VMEM((2, 704, 640), BF),
            pltpu.VMEM((2, 640, 704), BF),
            pltpu.VMEM((3, 960, 640), BF),
            pltpu.VMEM((3, 704, 960), BF),
            pltpu.VMEM((8, 2, 40, 960), F32),
        ],
        compiler_params=pltpu.CompilerParams(vmem_limit_bytes=56 * 2**20),
        name="near_block",
    )(meta, own, other, wv, wg, wo, below, below2, above, above2)


def split_gain(g):
    g = jnp.broadcast_to(g, (8, 640))
    low = g[:, :320]
    high = pltpu.roll(g[:, 256:], 320, 1)[:, :320]
    row = lax.broadcasted_iota(jnp.int32, (8, 320), 0)
    value = jnp.where(row % 2 == 0, low, high)
    top = value.astype(BF).astype(F32)
    return jnp.where(row < 2, top, jnp.where(row < 4, value - top, 0.0))


def resplit(g):
    row = lax.broadcasted_iota(jnp.int32, (8, 320), 0)
    value = jnp.where(row < 2, g, pltpu.roll(g, 2, 0))
    top = value.astype(BF).astype(F32)
    return jnp.where(row < 2, top, jnp.where(row < 4, value - top, 0.0))


def joined(rows):
    rows = rows.astype(F32)
    return rows + pltpu.roll(rows, 6, 0)


def far_kernel(meta, own, other, gain, near_dn, first, second, dn, dn_send, mine, send,
               rows, turned, w, acts, keep):
    c = meta[1]
    here = pl.multiple_of(c * 160, 16)
    there = pl.multiple_of((1 - c) * 160, 16)
    load_rows(own, other, rows, turned)
    for j in range(3):
        w[j, pl.ds(here, 160)] = first[j]
        w[j, pl.ds(there, 160)] = second[j]
    hidden_part(rows, w, acts, 0, 320)
    total = near_dn[...] + dot(acts[0], w[0]) + dot(acts[1], w[1])
    dn[...] = total[:352]
    dn_send[...] = total[352:].astype(BF)
    gsum = jnp.sum(total * rows[0].astype(F32), axis=0, keepdims=True) / gain[...]
    tail = split_gain(gsum).astype(BF)
    for j in range(3):
        keep[...] = dot(turned[j // 2], acts[j]).reshape(8, 2, 40, 320)
        for out, side in ((mine, c), (send, 1 - c)):
            out[8 * j : 8 * j + 8] = keep[:, side].astype(BF)
    for out in (mine, send):
        out[24] = jnp.zeros((40, 320), BF)
        out[24, :8] = tail


def far_block(meta, own, other, gain, near_dn, first, second):
    grads = jax.ShapeDtypeStruct((25, 40, 320), BF)
    return pl.pallas_call(
        far_kernel,
        out_shape=(
            jax.ShapeDtypeStruct((352, 640), F32),
            jax.ShapeDtypeStruct((352, 640), BF),
            grads,
            grads,
        ),
        in_specs=smem(1) + vmem(6),
        out_specs=tuple(vmem(4)),
        scratch_shapes=[
            pltpu.VMEM((2, 704, 640), BF),
            pltpu.VMEM((2, 640, 704), BF),
            pltpu.VMEM((3, 320, 640), BF),
            pltpu.VMEM((3, 704, 320), BF),
            pltpu.VMEM((8, 2, 40, 320), F32),
        ],
        compiler_params=pltpu.CompilerParams(vmem_limit_bytes=56 * 2**20),
        name="far_block",
    )(meta, own, other, gain, near_dn, first, second)


def finish_kernel(dest_g, dest_r, dn, got, lat, grad, gain, own, packed, sems):
    def sent(k):
        rank = dest_r[k]
        return (rank >= 0) & (rank < PLACES)

    for k in range(11):
        x_hat, inv_std = normalise(lat[k])
        d_hat = (dn[k] + got[k].astype(F32)) * gain[...]
        out = grad[1, k].astype(F32) + inv_std * (
            d_hat
            - jnp.mean(d_hat, axis=-1, keepdims=True)
            - x_hat * jnp.mean(d_hat * x_hat, axis=-1, keepdims=True)
        )
        own[k] = jnp.where(dest_r[k] >= 0, out, 0.0).astype(BF)

        @pl.when(sent(k))
        def _():
            place = dest_g[k] * PLACES + dest_r[k]
            pltpu.make_async_copy(own.at[k], packed.at[place], sems.at[k]).start()

    for k in range(11):

        @pl.when(sent(k))
        def _():
            pltpu.make_async_copy(own.at[k], packed.at[0], sems.at[k]).wait()


def finish(dest_g, dest_r, dn, got, lat, grad, gain):
    return pl.pallas_call(
        finish_kernel,
        out_shape=(
            jax.ShapeDtypeStruct((11, 32, 640), BF),
            jax.ShapeDtypeStruct((16 * PLACES, 32, 640), BF),
        ),
        in_specs=smem(2) + vmem(5),
        out_specs=(vmem(1)[0], pl.BlockSpec(memory_space=pl.ANY)),
        scratch_shapes=[pltpu.SemaphoreType.DMA((11,))],
        name="finish",
    )(dest_g, dest_r, dn, got, lat, grad, gain)


def unpack_kernel(src_p, src_r, came, placed, blank, sems):
    blank[...] = jnp.zeros_like(blank)
    for s in range(11):
        rank = src_r[s]

        @pl.when((rank >= 0) & (rank < PLACES))
        def _():
            pltpu.make_async_copy(
                came.at[src_p[s] * PLACES + rank], placed.at[s], sems.at[s]
            ).start()

        @pl.when((rank < 0) | (rank >= PLACES))
        def _():
            pltpu.make_async_copy(blank, placed.at[s], sems.at[s]).start()

    for s in range(11):
        pltpu.make_async_copy(blank, placed.at[s], sems.at[s]).wait()


def unpack(src_p, src_r, came):
    return pl.pallas_call(
        unpack_kernel,
        out_shape=jax.ShapeDtypeStruct((11, 32, 640), BF),
        in_specs=smem(2) + [pl.BlockSpec(memory_space=pl.ANY)],
        out_specs=pl.BlockSpec(memory_space=pl.ANY),
        scratch_shapes=[pltpu.VMEM((32, 640), BF), pltpu.SemaphoreType.DMA((11,))],
        name="unpack",
    )(src_p, src_r, came)


def local(kernel, out_shapes, *arrays):
    return pl.pallas_call(
        kernel,
        out_shape=tuple(jax.ShapeDtypeStruct(s, d) for s, d in out_shapes),
        in_specs=vmem(len(arrays)),
        out_specs=tuple(vmem(len(out_shapes))),
        compiler_params=pltpu.CompilerParams(vmem_limit_bytes=32 * 2**20),
    )(*arrays)


def near_sums_kernel(mine, got, own, up, down):
    own[...] = mine[0].astype(F32) + got[0].astype(F32)
    up[...] = (mine[1].astype(F32) + got[1].astype(F32)).astype(BF)
    down[...] = (mine[2].astype(F32) + got[2].astype(F32)).astype(BF)


def far_sums_kernel(mine, got, lower, upper, tail):
    for j in range(3):
        for out, at in ((lower, 8 * j), (upper, 8 * j + 4)):
            out[j] = (mine[at : at + 4].astype(F32) + got[at : at + 4].astype(F32)).astype(BF)
    tail[...] = joined(mine[24, :8]) + joined(got[24, :8])


def over_y_kernel(own, from_down, from_up, far_lower, far_upper, g0, g1, g2, g3, out):
    for j in range(3):
        for half, far in ((0, far_lower), (4, far_upper)):
            at = slice(half, half + 4)
            x = own[j, at] + from_down[j, at].astype(F32)
            x = x + (from_up[j, at].astype(F32) + far[j].astype(F32))
            out[at, 5 * j : 5 * j + 5] = x.astype(BF).reshape(4, 5, 8, 320)
    tail = resplit((g0[...] + g1[...]) + (g2[...] + g3[...])).astype(BF)
    for k in range(8):
        out[k, 15] = tail


def last_kernel(parts, value, gate, out, tail):
    total = parts[0].astype(F32)
    for k in range(1, 8):
        total = total + parts[k].astype(F32)
    for j, ref in enumerate((value, gate, out)):
        ref[...] = total[5 * j : 5 * j + 5].reshape(40, 320)
    tail[...] = joined(total[15])


def reduce_weights(near_mine, near_got, far_mine, far_got):
    grads = (3, 8, 40, 320)
    half = (3, 4, 40, 320)
    row = ((8, 320), F32)
    own, up, down = local(
        near_sums_kernel, ((grads, F32), (grads, BF), (grads, BF)), near_mine, near_got
    )
    from_down = ring(up, "y", 1)
    from_up = ring(down, "y", -1)
    lower, upper, tail = local(
        far_sums_kernel, ((half, BF), (half, BF), row), far_mine, far_got
    )
    lower = ring(lower, "y", 1)
    upper = ring(upper, "y", -1)
    lower = ring(lower, "y", 1)
    upper = ring(upper, "y", -1)
    tail = tail + swap(tail, "xl")
    tails = [tail] + [ring(tail, "y", d) for d in (2, 1, -1)]
    (parts,) = local(
        over_y_kernel, (((8, 16, 8, 320), BF),),
        own, from_down, from_up, lower, upper, *tails,
    )
    parts = lax.all_to_all(parts, ("xh", "z"), 0, 0, tiled=True)
    out = ((40, 320), F32)
    value, gate, proj, tail = local(last_kernel, (out, out, out, row), parts)
    return value, gate, proj, tail[:2].reshape(640)


def route(packed):
    return lax.all_to_all(packed, DP, 0, 0, tiled=True)


def more_rounds(placed, own, most, dest_g, dest_r, src_p, src_r):
    def more(state):
        return state[0] * PLACES < most[0]

    def one(state):
        t, placed = state
        rank = dest_r - t * PLACES
        here = (rank >= 0) & (rank < PLACES) & (dest_r >= 0)
        place = jnp.where(here, dest_g * PLACES + rank, -1)
        hit = place[None, :] == jnp.arange(16 * PLACES, dtype=jnp.int32)[:, None]
        pick = jnp.sum(jnp.where(hit, jnp.arange(11, dtype=jnp.int32)[None, :], 0), axis=1)
        came = route(jnp.take(own, pick, axis=0))
        rank = src_r - t * PLACES
        here = (rank >= 0) & (rank < PLACES) & (src_r >= 0)
        new = jnp.take(came, jnp.where(here, src_p * PLACES + rank, 0), axis=0)
        return t + 1, jnp.where(here[:, None, None], new, placed)

    return lax.while_loop(more, one, (jnp.int32(1), placed))[1]


def per_device(latents, cotangent, trunc, times, tmap, gain, w_value, w_gate, w_out):
    meta = jnp.stack([lax.axis_index(a) for a in (DP, "c")]).astype(jnp.int32)
    gain = gain[None, :]
    wv, wg, wo = w_value.T, w_gate.T, w_out.T
    rows = prologue(meta, trunc, times, noise_table(), latents, cotangent, gain)
    other = swap(rows, "xl")
    half = halves(meta, wv, wg, wo)
    below = ring(half, "y", 1)
    above = ring(half, "y", -1)
    dest_g, dest_r, src_p, src_r, most = index_work(meta, trunc, tmap)
    below2 = swap(below, "c")
    above2 = swap(above, "c")
    first = ring(below, "y", 1)
    second = ring(above2, "y", -1)
    rows2 = rows.reshape(2, 352, 640)
    other = other.reshape(2, 352, 640)
    near_dn, near_mine, near_send = near_block(
        meta, rows2, other, wv, wg, wo, below, below2, above, above2
    )
    near_got = swap(near_send, "c")
    dn, dn_send, far_mine, far_send = far_block(meta, rows2, other, gain, near_dn, first, second)
    got = swap(dn_send, "xl")
    far_got = swap(far_send, "c")
    tiles = (11, 32, 640)
    own, packed = finish(
        dest_g, dest_r, dn.reshape(tiles), got.reshape(tiles), latents, rows, gain
    )
    came = route(packed)
    placed = unpack(src_p, src_r, came)
    placed = more_rounds(placed, own, most, dest_g, dest_r, src_p, src_r)
    grads = reduce_weights(near_mine, near_got, far_mine, far_got)
    return placed, *grads


def solution(mesh):
    split = Mesh(mesh.devices.reshape(2, 4, 2, 4, 2), ("xh", "z", "c", "y", "xl"))
    tiles = P(DP, TENSOR, None)
    weights = P(None, TENSOR)

    def step(*args):
        return per_device(*args)

    step = jax.shard_map(
        step,
        mesh=split,
        in_specs=(tiles, tiles, P(), P(), P(), P(), weights, weights, weights),
        out_specs=(tiles, P(DP, TENSOR), P(DP, TENSOR), P(DP, TENSOR), P()),
        check_vma=False,
    )
    return step
```

```python
import jax
import jax.numpy as jnp
import numpy as np
from jax import lax
from jax.experimental import pallas as pl
from jax.experimental.pallas import tpu as pltpu
from jax.sharding import Mesh
from jax.sharding import PartitionSpec as P


TENSOR = ("y", "xl")
DP = ("xh", "z", "c")
EPS = 1e-05
PLACES = 3
BF = jnp.bfloat16
F32 = jnp.float32

VMEM = pltpu.MemorySpace.VMEM
SMEM = pltpu.MemorySpace.SMEM


def noise_table():
    betas = np.linspace(0.00085**0.5, 0.012**0.5, 1000) ** 2
    abar = np.exp(np.cumsum(np.log1p(-betas)))
    return jnp.asarray(np.sqrt(1.0 - abar), F32)


def swap(x, axis):
    return lax.ppermute(x, axis, [(0, 1), (1, 0)])


def ring(x, axis, step):
    return lax.ppermute(x, axis, [(i, (i + step) % 4) for i in range(4)])


def vmem(n):
    return [pl.BlockSpec(memory_space=VMEM)] * n


def smem(n):
    return [pl.BlockSpec(memory_space=SMEM)] * n


def index_kernel(meta, trunc, tmap, dest_g, dest_r, src_p, src_r, most, cnt):
    me = meta[0]

    def clear(i, _):
        cnt[i] = 0
        return 0

    lax.fori_loop(0, 256, clear, 0)

    def prompt(p, top):
        alive = trunc[p] - 29

        def slot(k, top):
            m = tmap[p * 11 + k]
            g = lax.div(m, 11)
            s = m - g * 11
            live = k < alive
            at = p * 16 + g
            r = cnt[at]

            @pl.when(live)
            def _():
                cnt[at] = r + 1

            rank = jnp.where(live, r, -1)

            @pl.when(p == me)
            def _():
                dest_g[k] = g
                dest_r[k] = rank

            @pl.when(g == me)
            def _():
                src_p[s] = p
                src_r[s] = rank

            return jnp.maximum(top, rank + 1)

        return lax.fori_loop(0, 11, slot, top)

    most[0] = lax.fori_loop(0, 16, prompt, jnp.int32(0))


def index_work(meta, trunc, tmap):
    i11 = jax.ShapeDtypeStruct((11,), jnp.int32)
    return pl.pallas_call(
        index_kernel,
        out_shape=(i11, i11, i11, i11, jax.ShapeDtypeStruct((1,), jnp.int32)),
        in_specs=smem(3),
        out_specs=tuple(smem(5)),
        scratch_shapes=[pltpu.SMEM((256,), jnp.int32)],
        name="routes",
    )(meta, trunc, tmap)


def halves_kernel(meta, wv, wg, wo, half):
    for j, w in enumerate((wv, wg, wo)):
        half[j] = w[...]


def halves(meta, wv, wg, wo):
    mine = pl.BlockSpec((160, 640), lambda i, meta: (meta[1], 0))
    return pl.pallas_call(
        halves_kernel,
        grid_spec=pltpu.PrefetchScalarGridSpec(
            num_scalar_prefetch=1,
            grid=(1,),
            in_specs=[mine] * 3,
            out_specs=pl.BlockSpec((3, 160, 640), lambda i, meta: (0, 0, 0)),
        ),
        out_shape=jax.ShapeDtypeStruct((3, 160, 640), BF),
        name="halves",
    )(meta, wv, wg, wo)


def normalise(tile):
    x = tile.astype(F32)
    centred = x - jnp.mean(x, axis=-1, keepdims=True)
    inv_std = lax.rsqrt(jnp.mean(centred * centred, axis=-1, keepdims=True) + EPS)
    return centred * inv_std, inv_std


def prologue_kernel(meta, trunc, times, table, lat, cot, gain, rows):
    me = meta[0]
    alive = trunc[me] - 29
    for k in range(11):
        scale = jnp.where(k < alive, table[times[me * 11 + k]], 0.0)
        x_hat, _ = normalise(lat[k])
        rows[0, k] = (x_hat * gain[...]).astype(BF)
        rows[1, k] = (cot[k].astype(F32) * scale).astype(BF)


def prologue(meta, trunc, times, table, lat, cot, gain):
    return pl.pallas_call(
        prologue_kernel,
        out_shape=jax.ShapeDtypeStruct((2, 11, 32, 640), BF),
        in_specs=smem(4) + vmem(3),
        out_specs=vmem(1)[0],
        name="prologue",
    )(meta, trunc, times, table, lat, cot, gain)


LAST = (((1,), (1,)), ((), ()))
PLAIN = (((1,), (0,)), ((), ()))


def dot(a, b, dims=PLAIN):
    return lax.dot_general(a, b, dims, preferred_element_type=F32)


def hidden_part(rows, w, acts, start, width):
    span = slice(start, start + width)
    value = dot(rows[0], w[0, span], LAST)
    gate = dot(rows[0], w[1, span], LAST)
    d_hidden = dot(rows[1], w[2, span], LAST)
    cdf = 0.5 * (1.0 + lax.erf(gate * 0.7071067811865476))
    density = jnp.exp(-0.5 * gate * gate) * 0.3989422804014327
    gelu = gate * cdf
    acts[0, :, span] = (d_hidden * gelu).astype(BF)
    acts[1, :, span] = (d_hidden * value * (cdf + gate * density)).astype(BF)
    acts[2, :, span] = (value * gelu).astype(BF)


def pallas(kernel, out_shapes, scalars, arrays, scratch):
    return pl.pallas_call(
        kernel,
        out_shape=tuple(jax.ShapeDtypeStruct(s, d) for s, d in out_shapes),
        in_specs=smem(1) + vmem(len(arrays)),
        out_specs=tuple(vmem(len(out_shapes))),
        scratch_shapes=[pltpu.VMEM(s, d) for s, d in scratch],
        compiler_params=pltpu.CompilerParams(vmem_limit_bytes=56 * 2**20),
    )(scalars, *arrays)


def first_kernel(meta, rows, wv, wg, wo, dn, turned, grads, w, acts):
    for j, ref in enumerate((wv, wg, wo)):
        w[j] = ref[...]
    for j in range(2):
        turned[j] = rows[j].T
    hidden_part(rows, w, acts, 0, 320)
    dn[...] = dot(acts[0], w[0]) + dot(acts[1], w[1])
    for j in range(3):
        grads[j] = dot(turned[j // 2], acts[j])


def first_block(meta, rows, wv, wg, wo):
    return pallas(
        first_kernel,
        (((352, 640), F32), ((2, 640, 352), BF), ((3, 640, 320), F32)),
        meta, (rows, wv, wg, wo),
        [((3, 320, 640), BF), ((3, 352, 320), BF)],
    )


def second_kernel(meta, rows, wv, wg, wo, before, dn, turned, mine, send, w, acts, keep):
    for j, ref in enumerate((wv, wg, wo)):
        w[j] = ref[...]
    for j in range(2):
        turned[j] = rows[j].T
    hidden_part(rows, w, acts, 0, 320)
    dn[...] = dot(acts[0], w[0]) + dot(acts[1], w[1])
    c = meta[1]
    for j in range(3):
        keep[...] = (before[j] + dot(turned[j // 2], acts[j])).reshape(8, 2, 40, 320)
        mine[j] = keep[:, c].astype(BF)
        send[j] = keep[:, 1 - c].astype(BF)


def second_block(meta, rows, wv, wg, wo, before):
    grads = ((3, 8, 40, 320), BF)
    return pallas(
        second_kernel,
        (((352, 640), F32), ((2, 640, 352), BF), grads, grads),
        meta, (rows, wv, wg, wo, before),
        [((3, 320, 640), BF), ((3, 352, 320), BF), ((8, 2, 40, 320), F32)],
    )


def near_kernel(meta, own, other, below, below2, above, above2, own_dn, other_dn,
                own_turned, other_turned, dn, mine, send, rows, w, acts, keep):
    c = meta[1]
    here = pl.multiple_of(c * 160, 16)
    there = pl.multiple_of((1 - c) * 160, 16)
    for j in range(2):
        rows[j, :352] = own[j]
        rows[j, 352:] = other[j]
    for j in range(3):
        w[j, pl.ds(here, 160)] = above[j]
        w[j, pl.ds(there, 160)] = above2[j]
        w[j, pl.ds(320 + here, 160)] = below[j]
        w[j, pl.ds(320 + there, 160)] = below2[j]
    for start, width in ((0, 256), (256, 256), (512, 128)):
        hidden_part(rows, w, acts, start, width)
    for before, at in ((own_dn, slice(0, 352)), (other_dn, slice(352, 704))):
        dn[at] = before[...] + dot(acts[0, at], w[0]) + dot(acts[1, at], w[1])
    for j in range(3):
        grad = dot(own_turned[j // 2], acts[j, :352]) + dot(other_turned[j // 2], acts[j, 352:])
        keep[...] = grad.reshape(8, 2, 40, 640)
        for out, side in ((mine, c), (send, 1 - c)):
            both = keep[:, side].reshape(320, 640)
            out[0, j] = both[:, :320].reshape(8, 40, 320).astype(BF)
            high = pltpu.roll(both[:, 256:640], 320, 1)[:, :320]
            out[1, j] = high.reshape(8, 40, 320).astype(BF)


def near_block(meta, *arrays):
    grads = ((2, 3, 8, 40, 320), BF)
    return pallas(
        near_kernel,
        (((704, 640), F32), grads, grads),
        meta, arrays,
        [
            ((2, 704, 640), BF), ((3, 640, 640), BF), ((3, 704, 640), BF),
            ((8, 2, 40, 640), F32),
        ],
    )


def split_gain(g):
    g = jnp.broadcast_to(g, (8, 640))
    low = g[:, :320]
    high = pltpu.roll(g[:, 256:], 320, 1)[:, :320]
    row = lax.broadcasted_iota(jnp.int32, (8, 320), 0)
    value = jnp.where(row % 2 == 0, low, high)
    top = value.astype(BF).astype(F32)
    return jnp.where(row < 2, top, jnp.where(row < 4, value - top, 0.0))


def resplit(g):
    row = lax.broadcasted_iota(jnp.int32, (8, 320), 0)
    value = jnp.where(row < 2, g, pltpu.roll(g, 2, 0))
    top = value.astype(BF).astype(F32)
    return jnp.where(row < 2, top, jnp.where(row < 4, value - top, 0.0))


def joined(rows):
    rows = rows.astype(F32)
    return rows + pltpu.roll(rows, 6, 0)


def far_kernel(meta, own, other, gain, near_dn, first, second, own_turned, other_turned,
               dn, dn_send, mine, send, rows, w, acts, keep):
    c = meta[1]
    here = pl.multiple_of(c * 160, 16)
    there = pl.multiple_of((1 - c) * 160, 16)
    for j in range(2):
        rows[j, :352] = own[j]
        rows[j, 352:] = other[j]
    for j in range(3):
        w[j, pl.ds(here, 160)] = first[j]
        w[j, pl.ds(there, 160)] = second[j]
    hidden_part(rows, w, acts, 0, 320)
    total = near_dn[...] + dot(acts[0], w[0]) + dot(acts[1], w[1])
    dn[...] = total[:352]
    dn_send[...] = total[352:].astype(BF)
    gsum = jnp.sum(total * rows[0].astype(F32), axis=0, keepdims=True) / gain[...]
    tail = split_gain(gsum).astype(BF)
    for j in range(3):
        grad = dot(own_turned[j // 2], acts[j, :352]) + dot(other_turned[j // 2], acts[j, 352:])
        keep[...] = grad.reshape(8, 2, 40, 320)
        for out, side in ((mine, c), (send, 1 - c)):
            out[8 * j : 8 * j + 8] = keep[:, side].astype(BF)
    for out in (mine, send):
        out[24] = jnp.zeros((40, 320), BF)
        out[24, :8] = tail


def far_block(meta, *arrays):
    grads = ((25, 40, 320), BF)
    return pallas(
        far_kernel,
        (((352, 640), F32), ((352, 640), BF), grads, grads),
        meta, arrays,
        [
            ((2, 704, 640), BF), ((3, 320, 640), BF), ((3, 704, 320), BF),
            ((8, 2, 40, 320), F32),
        ],
    )


def finish_kernel(dest_g, dest_r, dn, got, lat, grad, gain, own, packed, sems):
    def sent(k):
        rank = dest_r[k]
        return (rank >= 0) & (rank < PLACES)

    for k in range(11):
        x_hat, inv_std = normalise(lat[k])
        d_hat = (dn[k] + got[k].astype(F32)) * gain[...]
        out = grad[1, k].astype(F32) + inv_std * (
            d_hat
            - jnp.mean(d_hat, axis=-1, keepdims=True)
            - x_hat * jnp.mean(d_hat * x_hat, axis=-1, keepdims=True)
        )
        own[k] = jnp.where(dest_r[k] >= 0, out, 0.0).astype(BF)

        @pl.when(sent(k))
        def _():
            place = dest_g[k] * PLACES + dest_r[k]
            pltpu.make_async_copy(own.at[k], packed.at[place], sems.at[k]).start()

    for k in range(11):

        @pl.when(sent(k))
        def _():
            pltpu.make_async_copy(own.at[k], packed.at[0], sems.at[k]).wait()


def finish(dest_g, dest_r, dn, got, lat, grad, gain):
    return pl.pallas_call(
        finish_kernel,
        out_shape=(
            jax.ShapeDtypeStruct((11, 32, 640), BF),
            jax.ShapeDtypeStruct((16 * PLACES, 32, 640), BF),
        ),
        in_specs=smem(2) + vmem(5),
        out_specs=(vmem(1)[0], pl.BlockSpec(memory_space=pl.ANY)),
        scratch_shapes=[pltpu.SemaphoreType.DMA((11,))],
        name="finish",
    )(dest_g, dest_r, dn, got, lat, grad, gain)


def unpack_kernel(src_p, src_r, came, placed, blank, sems):
    blank[...] = jnp.zeros_like(blank)
    for s in range(11):
        rank = src_r[s]

        @pl.when((rank >= 0) & (rank < PLACES))
        def _():
            pltpu.make_async_copy(
                came.at[src_p[s] * PLACES + rank], placed.at[s], sems.at[s]
            ).start()

        @pl.when((rank < 0) | (rank >= PLACES))
        def _():
            pltpu.make_async_copy(blank, placed.at[s], sems.at[s]).start()

    for s in range(11):
        pltpu.make_async_copy(blank, placed.at[s], sems.at[s]).wait()


def unpack(src_p, src_r, came):
    return pl.pallas_call(
        unpack_kernel,
        out_shape=jax.ShapeDtypeStruct((11, 32, 640), BF),
        in_specs=smem(2) + [pl.BlockSpec(memory_space=pl.ANY)],
        out_specs=pl.BlockSpec(memory_space=pl.ANY),
        scratch_shapes=[pltpu.VMEM((32, 640), BF), pltpu.SemaphoreType.DMA((11,))],
        name="unpack",
    )(src_p, src_r, came)


def local(kernel, out_shapes, *arrays):
    return pl.pallas_call(
        kernel,
        out_shape=tuple(jax.ShapeDtypeStruct(s, d) for s, d in out_shapes),
        in_specs=vmem(len(arrays)),
        out_specs=tuple(vmem(len(out_shapes))),
        compiler_params=pltpu.CompilerParams(vmem_limit_bytes=32 * 2**20),
    )(*arrays)


def near_sums_kernel(mine, got, up, down):
    up[...] = (mine[0].astype(F32) + got[0].astype(F32)).astype(BF)
    down[...] = (mine[1].astype(F32) + got[1].astype(F32)).astype(BF)


def far_sums_kernel(mine, got, lower, upper, tail):
    for j in range(3):
        for out, at in ((lower, 8 * j), (upper, 8 * j + 4)):
            out[j] = (mine[at : at + 4].astype(F32) + got[at : at + 4].astype(F32)).astype(BF)
    tail[...] = joined(mine[24, :8]) + joined(got[24, :8])


def over_y_kernel(mine, got, from_down, from_up, far_lower, far_upper, g0, g1, g2, g3, out):
    for j in range(3):
        for half, far in ((0, far_lower), (4, far_upper)):
            at = slice(half, half + 4)
            x = mine[j, at].astype(F32) + got[j, at].astype(F32)
            x = x + from_down[j, at].astype(F32)
            x = x + (from_up[j, at].astype(F32) + far[j].astype(F32))
            out[at, 5 * j : 5 * j + 5] = x.astype(BF).reshape(4, 5, 8, 320)
    tail = resplit((g0[...] + g1[...]) + (g2[...] + g3[...])).astype(BF)
    for k in range(8):
        out[k, 15] = tail


def last_kernel(parts, value, gate, out, tail):
    total = parts[0].astype(F32)
    for k in range(1, 8):
        total = total + parts[k].astype(F32)
    for j, ref in enumerate((value, gate, out)):
        ref[...] = total[5 * j : 5 * j + 5].reshape(40, 320)
    tail[...] = joined(total[15])


def reduce_weights(own_mine, own_got, near_mine, near_got, far_mine, far_got):
    grads = (3, 8, 40, 320)
    half = (3, 4, 40, 320)
    row = ((8, 320), F32)
    up, down = local(near_sums_kernel, ((grads, BF), (grads, BF)), near_mine, near_got)
    from_down = ring(up, "y", 1)
    from_up = ring(down, "y", -1)
    lower, upper, tail = local(
        far_sums_kernel, ((half, BF), (half, BF), row), far_mine, far_got
    )
    lower = ring(lower, "y", 1)
    upper = ring(upper, "y", -1)
    lower = ring(lower, "y", 1)
    upper = ring(upper, "y", -1)
    tail = tail + swap(tail, "xl")
    tails = [tail] + [ring(tail, "y", d) for d in (2, 1, -1)]
    (parts,) = local(
        over_y_kernel, (((8, 16, 8, 320), BF),),
        own_mine, own_got, from_down, from_up, lower, upper, *tails,
    )
    parts = lax.all_to_all(parts, ("xh", "z"), 0, 0, tiled=True)
    out = ((40, 320), F32)
    value, gate, proj, tail = local(last_kernel, (out, out, out, row), parts)
    return value, gate, proj, tail[:2].reshape(640)


def route(packed):
    return lax.all_to_all(packed, DP, 0, 0, tiled=True)


def more_rounds(placed, own, most, dest_g, dest_r, src_p, src_r):
    def more(state):
        return state[0] * PLACES < most[0]

    def one(state):
        t, placed = state
        rank = dest_r - t * PLACES
        here = (rank >= 0) & (rank < PLACES) & (dest_r >= 0)
        place = jnp.where(here, dest_g * PLACES + rank, -1)
        hit = place[None, :] == jnp.arange(16 * PLACES, dtype=jnp.int32)[:, None]
        pick = jnp.sum(jnp.where(hit, jnp.arange(11, dtype=jnp.int32)[None, :], 0), axis=1)
        came = route(jnp.take(own, pick, axis=0))
        rank = src_r - t * PLACES
        here = (rank >= 0) & (rank < PLACES) & (src_r >= 0)
        new = jnp.take(came, jnp.where(here, src_p * PLACES + rank, 0), axis=0)
        return t + 1, jnp.where(here[:, None, None], new, placed)

    return lax.while_loop(more, one, (jnp.int32(1), placed))[1]


def per_device(latents, cotangent, trunc, times, tmap, gain, w_value, w_gate, w_out):
    meta = jnp.stack([lax.axis_index(a) for a in (DP, "c")]).astype(jnp.int32)
    gain = gain[None, :]
    wv, wg, wo = w_value.T, w_gate.T, w_out.T
    rows = prologue(meta, trunc, times, noise_table(), latents, cotangent, gain)
    other = swap(rows, "xl")
    half = halves(meta, wv, wg, wo)
    below = ring(half, "y", 1)
    above = ring(half, "y", -1)
    dest_g, dest_r, src_p, src_r, most = index_work(meta, trunc, tmap)
    below2 = swap(below, "c")
    above2 = swap(above, "c")
    first = ring(below, "y", 1)
    second = ring(above2, "y", -1)
    rows2 = rows.reshape(2, 352, 640)
    other = other.reshape(2, 352, 640)
    own_dn, own_turned, partial = first_block(meta, rows2, wv, wg, wo)
    other_dn, other_turned, own_mine, own_send = second_block(meta, other, wv, wg, wo, partial)
    own_got = swap(own_send, "c")
    near_dn, near_mine, near_send = near_block(
        meta, rows2, other, below, below2, above, above2, own_dn, other_dn, own_turned, other_turned
    )
    near_got = swap(near_send, "c")
    dn, dn_send, far_mine, far_send = far_block(
        meta, rows2, other, gain, near_dn, first, second, own_turned, other_turned
    )
    got = swap(dn_send, "xl")
    far_got = swap(far_send, "c")
    tiles = (11, 32, 640)
    own, packed = finish(
        dest_g, dest_r, dn.reshape(tiles), got.reshape(tiles), latents, rows, gain
    )
    came = route(packed)
    placed = unpack(src_p, src_r, came)
    placed = more_rounds(placed, own, most, dest_g, dest_r, src_p, src_r)
    grads = reduce_weights(own_mine, own_got, near_mine, near_got, far_mine, far_got)
    return placed, *grads


def solution(mesh):
    split = Mesh(mesh.devices.reshape(2, 4, 2, 4, 2), ("xh", "z", "c", "y", "xl"))
    tiles = P(DP, TENSOR, None)
    weights = P(None, TENSOR)

    def step(*args):
        return per_device(*args)

    step = jax.shard_map(
        step,
        mesh=split,
        in_specs=(tiles, tiles, P(), P(), P(), P(), weights, weights, weights),
        out_specs=(tiles, P(DP, TENSOR), P(DP, TENSOR), P(DP, TENSOR), P()),
        check_vma=False,
    )
    return step
```

```python
import jax
import jax.numpy as jnp
import numpy as np
from jax import lax
from jax.experimental import pallas as pl
from jax.experimental.pallas import tpu as pltpu
from jax.sharding import Mesh
from jax.sharding import PartitionSpec as P


TENSOR = ("y", "xl")
DP = ("xh", "z", "c")
EPS = 1e-05
PLACES = 3
BF = jnp.bfloat16
F32 = jnp.float32

VMEM = pltpu.MemorySpace.VMEM
SMEM = pltpu.MemorySpace.SMEM


def noise_table():
    betas = np.linspace(0.00085**0.5, 0.012**0.5, 1000) ** 2
    abar = np.exp(np.cumsum(np.log1p(-betas)))
    return jnp.asarray(np.sqrt(1.0 - abar), F32)


def swap(x, axis):
    return lax.ppermute(x, axis, [(0, 1), (1, 0)])


def ring(x, axis, step):
    return lax.ppermute(x, axis, [(i, (i + step) % 4) for i in range(4)])


def grant(mib):
    return pltpu.CompilerParams(vmem_limit_bytes=mib * 2**20)


def vmem(n):
    return [pl.BlockSpec(memory_space=VMEM)] * n


def smem(n):
    return [pl.BlockSpec(memory_space=SMEM)] * n


def index_kernel(meta, trunc, tmap, dest_g, dest_r, src_p, src_r, most, cnt):
    me = meta[0]

    def clear(i, _):
        cnt[i] = 0
        return 0

    lax.fori_loop(0, 256, clear, 0)

    def prompt(p, top):
        alive = trunc[p] - 29

        def slot(k, top):
            m = tmap[p * 11 + k]
            g = lax.div(m, 11)
            s = m - g * 11
            live = k < alive
            at = p * 16 + g
            r = cnt[at]

            @pl.when(live)
            def _():
                cnt[at] = r + 1

            rank = jnp.where(live, r, -1)

            @pl.when(p == me)
            def _():
                dest_g[k] = g
                dest_r[k] = rank

            @pl.when(g == me)
            def _():
                src_p[s] = p
                src_r[s] = rank

            return jnp.maximum(top, rank + 1)

        return lax.fori_loop(0, 11, slot, top)

    most[0] = lax.fori_loop(0, 16, prompt, jnp.int32(0))


def index_work(meta, trunc, tmap):
    i11 = jax.ShapeDtypeStruct((11,), jnp.int32)
    return pl.pallas_call(
        index_kernel,
        out_shape=(i11, i11, i11, i11, jax.ShapeDtypeStruct((1,), jnp.int32)),
        in_specs=smem(3),
        out_specs=tuple(smem(5)),
        scratch_shapes=[pltpu.SMEM((256,), jnp.int32)],
        compiler_params=grant(1),
        name="routes",
    )(meta, trunc, tmap)


def halves_kernel(meta, wv, wg, wo, half):
    for j, w in enumerate((wv, wg, wo)):
        half[j] = w[...]


def halves(meta, wv, wg, wo):
    mine = pl.BlockSpec((160, 640), lambda i, meta: (meta[1], 0))
    return pl.pallas_call(
        halves_kernel,
        grid_spec=pltpu.PrefetchScalarGridSpec(
            num_scalar_prefetch=1,
            grid=(1,),
            in_specs=[mine] * 3,
            out_specs=pl.BlockSpec((3, 160, 640), lambda i, meta: (0, 0, 0)),
        ),
        out_shape=jax.ShapeDtypeStruct((3, 160, 640), BF),
        compiler_params=grant(6),
        name="halves",
    )(meta, wv, wg, wo)


def normalise(tile):
    x = tile.astype(F32)
    centred = x - jnp.mean(x, axis=-1, keepdims=True)
    inv_std = lax.rsqrt(jnp.mean(centred * centred, axis=-1, keepdims=True) + EPS)
    return centred * inv_std, inv_std


def prologue_kernel(meta, trunc, times, table, lat, cot, gain, rows):
    me = meta[0]
    alive = trunc[me] - 29
    for k in range(11):
        scale = jnp.where(k < alive, table[times[me * 11 + k]], 0.0)
        x_hat, _ = normalise(lat[k])
        rows[0, k] = (x_hat * gain[...]).astype(BF)
        rows[1, k] = (cot[k].astype(F32) * scale).astype(BF)


def prologue(meta, trunc, times, table, lat, cot, gain):
    return pl.pallas_call(
        prologue_kernel,
        out_shape=jax.ShapeDtypeStruct((2, 11, 32, 640), BF),
        in_specs=smem(4) + vmem(3),
        out_specs=vmem(1)[0],
        compiler_params=grant(10),
        name="prologue",
    )(meta, trunc, times, table, lat, cot, gain)


LAST = (((1,), (1,)), ((), ()))
PLAIN = (((1,), (0,)), ((), ()))


def dot(a, b, dims=PLAIN):
    return lax.dot_general(a, b, dims, preferred_element_type=F32)


def hidden_part(rows, w, acts, start, width):
    span = slice(start, start + width)
    value = dot(rows[0], w[0, span], LAST)
    gate = dot(rows[0], w[1, span], LAST)
    d_hidden = dot(rows[1], w[2, span], LAST)
    cdf = 0.5 * (1.0 + lax.erf(gate * 0.7071067811865476))
    density = jnp.exp(-0.5 * gate * gate) * 0.3989422804014327
    gelu = gate * cdf
    acts[0, :, span] = (d_hidden * gelu).astype(BF)
    acts[1, :, span] = (d_hidden * value * (cdf + gate * density)).astype(BF)
    acts[2, :, span] = (value * gelu).astype(BF)


def local(kernel, mib, out_shapes, arrays, scratch=(), scalars=()):
    out = pl.pallas_call(
        kernel,
        out_shape=tuple(jax.ShapeDtypeStruct(s, d) for s, d in out_shapes),
        in_specs=smem(len(scalars)) + vmem(len(arrays)),
        out_specs=tuple(vmem(len(out_shapes))),
        scratch_shapes=[pltpu.VMEM(s, d) for s, d in scratch],
        compiler_params=grant(mib),
    )(*scalars, *arrays)
    return out


def near_kernel(meta, own, other, wv, wg, wo, below, below2, above, above2,
                dn, acts, rows, turned, w):
    c = meta[1]
    here = pl.multiple_of(c * 160, 16)
    there = pl.multiple_of((1 - c) * 160, 16)
    for j in range(2):
        rows[j, :352] = own[j]
        rows[j, 352:] = other[j]
        turned[j] = rows[j].T
    for j, ref in enumerate((wv, wg, wo)):
        w[j, :320] = ref[...]
        w[j, pl.ds(320 + here, 160)] = above[j]
        w[j, pl.ds(320 + there, 160)] = above2[j]
        w[j, pl.ds(640 + here, 160)] = below[j]
        w[j, pl.ds(640 + there, 160)] = below2[j]
    for start, width in ((0, 256), (256, 256), (512, 256), (768, 192)):
        hidden_part(rows, w, acts, start, width)
    dn[...] = dot(acts[0], w[0]) + dot(acts[1], w[1])


def near_forward(meta, *arrays):
    return local(
        near_kernel, 18,
        (
            ((704, 640), F32), ((3, 704, 960), BF), ((2, 704, 640), BF), ((2, 640, 704), BF),
        ),
        arrays, [((3, 960, 640), BF)], (meta,),
    )


def near_grads_kernel(meta, turned, acts, mine, send, keep):
    c = meta[1]
    for j in range(3):
        keep[...] = dot(turned[j // 2], acts[j]).reshape(8, 2, 40, 960)
        for out, side in ((mine, c), (send, 1 - c)):
            both = keep[:, side].reshape(320, 960)
            out[0, j] = both[:, :320].reshape(8, 40, 320).astype(BF)
            mid = pltpu.roll(both[:, 256:640], 320, 1)[:, :320]
            out[1, j] = mid.reshape(8, 40, 320).astype(BF)
            out[2, j] = both[:, 640:].reshape(8, 40, 320).astype(BF)


def near_grads(meta, turned, acts):
    grads = ((3, 3, 8, 40, 320), BF)
    return local(
        near_grads_kernel, 14, (grads, grads), (turned, acts),
        [((8, 2, 40, 960), F32)], (meta,),
    )


def split_gain(g):
    g = jnp.broadcast_to(g, (8, 640))
    low = g[:, :320]
    high = pltpu.roll(g[:, 256:], 320, 1)[:, :320]
    row = lax.broadcasted_iota(jnp.int32, (8, 320), 0)
    value = jnp.where(row % 2 == 0, low, high)
    top = value.astype(BF).astype(F32)
    return jnp.where(row < 2, top, jnp.where(row < 4, value - top, 0.0))


def resplit(g):
    row = lax.broadcasted_iota(jnp.int32, (8, 320), 0)
    value = jnp.where(row < 2, g, pltpu.roll(g, 2, 0))
    top = value.astype(BF).astype(F32)
    return jnp.where(row < 2, top, jnp.where(row < 4, value - top, 0.0))


def joined(rows):
    rows = rows.astype(F32)
    return rows + pltpu.roll(rows, 6, 0)


def far_kernel(meta, rows, gain, near_dn, first, second, dn, dn_send, acts, tail, w):
    c = meta[1]
    here = pl.multiple_of(c * 160, 16)
    there = pl.multiple_of((1 - c) * 160, 16)
    for j in range(3):
        w[j, pl.ds(here, 160)] = first[j]
        w[j, pl.ds(there, 160)] = second[j]
    hidden_part(rows, w, acts, 0, 320)
    total = near_dn[...] + dot(acts[0], w[0]) + dot(acts[1], w[1])
    dn[...] = total[:352]
    dn_send[...] = total[352:].astype(BF)
    gsum = jnp.sum(total * rows[0].astype(F32), axis=0, keepdims=True) / gain[...]
    tail[...] = split_gain(gsum)


def far_forward(meta, *arrays):
    return local(
        far_kernel, 14,
        (((352, 640), F32), ((352, 640), BF), ((3, 704, 320), BF), ((8, 320), F32)),
        arrays, [((3, 320, 640), BF)], (meta,),
    )


def far_grads_kernel(meta, turned, acts, tail, mine, send, keep):
    c = meta[1]
    for j in range(3):
        keep[...] = dot(turned[j // 2], acts[j]).reshape(8, 2, 40, 320)
        for out, side in ((mine, c), (send, 1 - c)):
            out[8 * j : 8 * j + 8] = keep[:, side].astype(BF)
    for out in (mine, send):
        out[24] = jnp.zeros((40, 320), BF)
        out[24, :8] = tail[...].astype(BF)


def far_grads(meta, turned, acts, tail):
    grads = ((25, 40, 320), BF)
    return local(
        far_grads_kernel, 10, (grads, grads), (turned, acts, tail),
        [((8, 2, 40, 320), F32)], (meta,),
    )


def finish_kernel(dest_g, dest_r, dn, got, lat, grad, gain, own, packed, sems):
    def sent(k):
        rank = dest_r[k]
        return (rank >= 0) & (rank < PLACES)

    for k in range(11):
        x_hat, inv_std = normalise(lat[k])
        d_hat = (dn[k] + got[k].astype(F32)) * gain[...]
        out = grad[1, k].astype(F32) + inv_std * (
            d_hat
            - jnp.mean(d_hat, axis=-1, keepdims=True)
            - x_hat * jnp.mean(d_hat * x_hat, axis=-1, keepdims=True)
        )
        own[k] = jnp.where(dest_r[k] >= 0, out, 0.0).astype(BF)

        @pl.when(sent(k))
        def _():
            place = dest_g[k] * PLACES + dest_r[k]
            pltpu.make_async_copy(own.at[k], packed.at[place], sems.at[k]).start()

    for k in range(11):

        @pl.when(sent(k))
        def _():
            pltpu.make_async_copy(own.at[k], packed.at[0], sems.at[k]).wait()


def finish(dest_g, dest_r, dn, got, lat, grad, gain):
    return pl.pallas_call(
        finish_kernel,
        out_shape=(
            jax.ShapeDtypeStruct((11, 32, 640), BF),
            jax.ShapeDtypeStruct((16 * PLACES, 32, 640), BF),
        ),
        in_specs=smem(2) + vmem(5),
        out_specs=(vmem(1)[0], pl.BlockSpec(memory_space=pltpu.MemorySpace.HBM)),
        scratch_shapes=[pltpu.SemaphoreType.DMA((11,))],
        compiler_params=grant(10),
        name="finish",
    )(dest_g, dest_r, dn, got, lat, grad, gain)


def unpack_kernel(src_p, src_r, came, placed, blank, sems):
    blank[...] = jnp.zeros_like(blank)
    for s in range(11):
        rank = src_r[s]

        @pl.when((rank >= 0) & (rank < PLACES))
        def _():
            pltpu.make_async_copy(
                came.at[src_p[s] * PLACES + rank], placed.at[s], sems.at[s]
            ).start()

        @pl.when((rank < 0) | (rank >= PLACES))
        def _():
            pltpu.make_async_copy(blank, placed.at[s], sems.at[s]).start()

    for s in range(11):
        pltpu.make_async_copy(blank, placed.at[s], sems.at[s]).wait()


def unpack(src_p, src_r, came):
    return pl.pallas_call(
        unpack_kernel,
        out_shape=jax.ShapeDtypeStruct((11, 32, 640), BF),
        in_specs=smem(2) + [pl.BlockSpec(memory_space=pl.ANY)],
        out_specs=pl.BlockSpec(memory_space=pl.ANY),
        scratch_shapes=[pltpu.VMEM((32, 640), BF), pltpu.SemaphoreType.DMA((11,))],
        compiler_params=grant(2),
        name="unpack",
    )(src_p, src_r, came)


def near_sums_kernel(mine, got, own, up, down):
    own[...] = mine[0].astype(F32) + got[0].astype(F32)
    up[...] = (mine[1].astype(F32) + got[1].astype(F32)).astype(BF)
    down[...] = (mine[2].astype(F32) + got[2].astype(F32)).astype(BF)


def far_sums_kernel(mine, got, lower, upper, tail):
    for j in range(3):
        for out, at in ((lower, 8 * j), (upper, 8 * j + 4)):
            out[j] = (mine[at : at + 4].astype(F32) + got[at : at + 4].astype(F32)).astype(BF)
    tail[...] = joined(mine[24, :8]) + joined(got[24, :8])


def over_y_kernel(meta, own, from_down, from_up, far_lower, far_upper, g0, g1, g2, g3,
                  keep, up, down, far, parts):
    for j in range(3):
        for half, came in ((0, far_lower), (4, far_upper)):
            at = slice(half, half + 4)
            x = own[j, at] + from_down[j, at].astype(F32)
            x = x + (from_up[j, at].astype(F32) + came[j].astype(F32))
            parts[half // 4, :, 5 * j : 5 * j + 5] = x.reshape(4, 5, 8, 320)
    tail = resplit((g0[...] + g1[...]) + (g2[...] + g3[...]))
    for k in range(2):
        for z in range(4):
            parts[k, z, 15] = tail
    z = meta[2]
    for out, step in ((keep, 0), (up, 1), (down, 3), (far, 2)):
        out[...] = parts[:, lax.rem(z + step, 4)].astype(out.dtype)


def over_z_kernel(meta, own, down, up, far, keep, give, sums):
    sums[...] = (own[...] + far[...].astype(F32)) + (down[...].astype(F32) + up[...].astype(F32))
    for k in range(2):
        sums[k, 15] = resplit(joined(sums[k, 15]))
    keep[...] = sums[meta[3]]
    give[...] = sums[1 - meta[3]].astype(BF)


def last_kernel(keep, got, value, gate, out, tail):
    total = keep[...] + got[...].astype(F32)
    for j, ref in enumerate((value, gate, out)):
        ref[...] = total[5 * j : 5 * j + 5].reshape(40, 320)
    tail[...] = joined(total[15])


def reduce_weights(meta, near_mine, near_got, far_mine, far_got):
    grads = (3, 8, 40, 320)
    half = (3, 4, 40, 320)
    row = ((8, 320), F32)
    own, up, down = local(
        near_sums_kernel, 4, ((grads, F32), (grads, BF), (grads, BF)),
        (near_mine, near_got),
    )
    from_down = ring(up, "y", 1)
    from_up = ring(down, "y", -1)
    lower, upper, tail = local(
        far_sums_kernel, 4, ((half, BF), (half, BF), row), (far_mine, far_got)
    )
    lower = ring(lower, "y", 1)
    upper = ring(upper, "y", -1)
    lower = ring(lower, "y", 1)
    upper = ring(upper, "y", -1)
    tail = tail + swap(tail, "xl")
    tails = [tail] + [ring(tail, "y", d) for d in (2, 1, -1)]
    part = (2, 16, 8, 320)
    own, up, down, far = local(
        over_y_kernel, 6, ((part, F32), (part, BF), (part, BF), (part, BF)),
        (own, from_down, from_up, lower, upper, *tails), [((2, 4, 16, 8, 320), F32)], (meta,),
    )
    came = ring(up, "z", 1), ring(down, "z", -1), ring(far, "z", 2)
    keep, give = local(
        over_z_kernel, 4, ((part[1:], F32), (part[1:], BF)), (own, *came),
        [(part, F32)], (meta,),
    )
    got = swap(give, "xh")
    out = ((40, 320), F32)
    value, gate, proj, tail = local(last_kernel, 2, (out, out, out, row), (keep, got))
    return value, gate, proj, tail[:2].reshape(640)


def route(packed):
    return lax.all_to_all(packed, DP, 0, 0, tiled=True)


def more_rounds(placed, own, most, dest_g, dest_r, src_p, src_r):
    def more(state):
        return state[0] < most[0]

    def one(state):
        t, placed = state
        groups = jnp.arange(16, dtype=jnp.int32)
        hit = (dest_g[None, :] == groups[:, None]) & (dest_r[None, :] == t)
        pick = jnp.sum(jnp.where(hit, jnp.arange(11, dtype=jnp.int32)[None, :], 0), axis=1)
        came = route(jnp.take(own, pick, axis=0))
        here = src_r == t
        new = jnp.take(came, jnp.where(here, src_p, 0), axis=0)
        return t + 1, jnp.where(here[:, None, None], new, placed)

    return lax.while_loop(more, one, (jnp.int32(PLACES), placed))[1]


def per_device(latents, cotangent, trunc, times, tmap, gain, w_value, w_gate, w_out):
    meta = jnp.stack([lax.axis_index(a) for a in (DP, "c", "z", "xh")]).astype(jnp.int32)
    gain = gain[None, :]
    wv, wg, wo = w_value.T, w_gate.T, w_out.T
    half = halves(meta, wv, wg, wo)
    below = ring(half, "y", 1)
    above = ring(half, "y", -1)
    rows = prologue(meta, trunc, times, noise_table(), latents, cotangent, gain)
    other = swap(rows, "xl")
    dest_g, dest_r, src_p, src_r, most = index_work(meta, trunc, tmap)
    below2 = swap(below, "c")
    above2 = swap(above, "c")
    first = ring(below, "y", 1)
    second = ring(above2, "y", -1)
    rows2 = rows.reshape(2, 352, 640)
    other = other.reshape(2, 352, 640)
    near_dn, near_acts, both, turned = near_forward(
        meta, rows2, other, wv, wg, wo, below, below2, above, above2
    )
    near_mine, near_send = near_grads(meta, turned, near_acts)
    near_got = swap(near_send, "c")
    dn, dn_send, far_acts, tail = far_forward(meta, both, gain, near_dn, first, second)
    got = swap(dn_send, "xl")
    far_mine, far_send = far_grads(meta, turned, far_acts, tail)
    far_got = swap(far_send, "c")
    tiles = (11, 32, 640)
    own, packed = finish(
        dest_g, dest_r, dn.reshape(tiles), got.reshape(tiles), latents, rows, gain
    )
    came = route(packed)
    placed = unpack(src_p, src_r, came)
    placed = more_rounds(placed, own, most, dest_g, dest_r, src_p, src_r)
    grads = reduce_weights(meta, near_mine, near_got, far_mine, far_got)
    return placed, *grads


def solution(mesh):
    split = Mesh(mesh.devices.reshape(2, 4, 2, 4, 2), ("xh", "z", "c", "y", "xl"))
    tiles = P(DP, TENSOR, None)
    weights = P(None, TENSOR)

    def step(*args):
        return per_device(*args)

    step = jax.shard_map(
        step,
        mesh=split,
        in_specs=(tiles, tiles, P(), P(), P(), P(), weights, weights, weights),
        out_specs=(tiles, P(DP, TENSOR), P(DP, TENSOR), P(DP, TENSOR), P()),
        check_vma=False,
    )
    return step
```

```python
import jax
import jax.numpy as jnp
import numpy as np
from jax import lax
from jax.experimental import pallas as pl
from jax.experimental.pallas import tpu as pltpu
from jax.sharding import Mesh
from jax.sharding import PartitionSpec as P


TENSOR = ("y", "xl")
DP = ("xh", "z", "c")
EPS = 1e-05
PLACES = 3
BF = jnp.bfloat16
F32 = jnp.float32

VMEM = pltpu.MemorySpace.VMEM
SMEM = pltpu.MemorySpace.SMEM
HBM = pltpu.MemorySpace.HBM


def noise_table():
    betas = np.linspace(0.00085**0.5, 0.012**0.5, 1000) ** 2
    abar = np.exp(np.cumsum(np.log1p(-betas)))
    return jnp.asarray(np.sqrt(1.0 - abar), F32)


def swap(x, axis):
    return lax.ppermute(x, axis, [(0, 1), (1, 0)])


def ring(x, axis, step):
    return lax.ppermute(x, axis, [(i, (i + step) % 4) for i in range(4)])


def grant(mib):
    return pltpu.CompilerParams(vmem_limit_bytes=mib * 2**20)


def vmem(n):
    return [pl.BlockSpec(memory_space=VMEM)] * n


def smem(n):
    return [pl.BlockSpec(memory_space=SMEM)] * n


def index_kernel(meta, trunc, tmap, dest_g, dest_r, src_p, src_r, most, cnt):
    me = meta[0]

    def clear(i, _):
        cnt[i] = 0
        return 0

    lax.fori_loop(0, 256, clear, 0)

    def prompt(p, top):
        alive = trunc[p] - 29

        def slot(k, top):
            m = tmap[p * 11 + k]
            g = lax.div(m, 11)
            s = m - g * 11
            live = k < alive
            at = p * 16 + g
            r = cnt[at]

            @pl.when(live)
            def _():
                cnt[at] = r + 1

            rank = jnp.where(live, r, -1)

            @pl.when(p == me)
            def _():
                dest_g[k] = g
                dest_r[k] = rank

            @pl.when(g == me)
            def _():
                src_p[s] = p
                src_r[s] = rank

            return jnp.maximum(top, rank + 1)

        return lax.fori_loop(0, 11, slot, top)

    most[0] = lax.fori_loop(0, 16, prompt, jnp.int32(0))


def index_work(meta, trunc, tmap):
    i11 = jax.ShapeDtypeStruct((11,), jnp.int32)
    return pl.pallas_call(
        index_kernel,
        out_shape=(i11, i11, i11, i11, jax.ShapeDtypeStruct((1,), jnp.int32)),
        in_specs=smem(3),
        out_specs=tuple(smem(5)),
        scratch_shapes=[pltpu.SMEM((256,), jnp.int32)],
        compiler_params=grant(1),
        name="routes",
    )(meta, trunc, tmap)


def halves_kernel(meta, wv, wg, wo, half, sems):
    start = pl.multiple_of(meta[1] * 160, 16)
    copies = [
        pltpu.make_async_copy(w.at[pl.ds(start, 160), :], half.at[j], sems.at[j])
        for j, w in enumerate((wv, wg, wo))
    ]
    for copy in copies:
        copy.start()
    for copy in copies:
        copy.wait()


def halves(meta, wv, wg, wo):
    return pl.pallas_call(
        halves_kernel,
        out_shape=jax.ShapeDtypeStruct((3, 160, 640), BF),
        in_specs=smem(1) + [pl.BlockSpec(memory_space=HBM)] * 3,
        out_specs=vmem(1)[0],
        scratch_shapes=[pltpu.SemaphoreType.DMA((3,))],
        compiler_params=grant(4),
        name="halves",
    )(meta, wv, wg, wo)


def normalise(tile):
    x = tile.astype(F32)
    centred = x - jnp.mean(x, axis=-1, keepdims=True)
    inv_std = lax.rsqrt(jnp.mean(centred * centred, axis=-1, keepdims=True) + EPS)
    return centred * inv_std, inv_std


def prologue_kernel(meta, trunc, times, table, lat, cot, gain, rows):
    me = meta[0]
    alive = trunc[me] - 29
    for k in range(11):
        scale = jnp.where(k < alive, table[times[me * 11 + k]], 0.0)
        x_hat, _ = normalise(lat[k])
        rows[0, k] = (x_hat * gain[...]).astype(BF)
        rows[1, k] = (cot[k].astype(F32) * scale).astype(BF)


def prologue(meta, trunc, times, table, lat, cot, gain):
    return pl.pallas_call(
        prologue_kernel,
        out_shape=jax.ShapeDtypeStruct((2, 11, 32, 640), BF),
        in_specs=smem(4) + vmem(3),
        out_specs=vmem(1)[0],
        compiler_params=grant(10),
        name="prologue",
    )(meta, trunc, times, table, lat, cot, gain)


LAST = (((1,), (1,)), ((), ()))
PLAIN = (((1,), (0,)), ((), ()))


def dot(a, b, dims=PLAIN):
    return lax.dot_general(a, b, dims, preferred_element_type=F32)


def hidden_part(rows, w, acts, start, width):
    span = slice(start, start + width)
    value = dot(rows[0], w[0, span], LAST)
    gate = dot(rows[0], w[1, span], LAST)
    d_hidden = dot(rows[1], w[2, span], LAST)
    cdf = 0.5 * (1.0 + lax.erf(gate * 0.7071067811865476))
    density = jnp.exp(-0.5 * gate * gate) * 0.3989422804014327
    gelu = gate * cdf
    acts[0, :, span] = (d_hidden * gelu).astype(BF)
    acts[1, :, span] = (d_hidden * value * (cdf + gate * density)).astype(BF)
    acts[2, :, span] = (value * gelu).astype(BF)


def local(kernel, mib, out_shapes, arrays, scratch=(), scalars=()):
    out = pl.pallas_call(
        kernel,
        out_shape=tuple(jax.ShapeDtypeStruct(s, d) for s, d in out_shapes),
        in_specs=smem(len(scalars)) + vmem(len(arrays)),
        out_specs=tuple(vmem(len(out_shapes))),
        scratch_shapes=[pltpu.VMEM(s, d) for s, d in scratch],
        compiler_params=grant(mib),
    )(*scalars, *arrays)
    return out


CHUNKS = ((0, 256), (256, 256), (512, 256), (768, 192))


def near_own_kernel(meta, rows, wv, wg, wo, below, below2, above, above2, dn, acts, w):
    c = meta[1]
    here = pl.multiple_of(c * 160, 16)
    there = pl.multiple_of((1 - c) * 160, 16)
    for j, ref in enumerate((wv, wg, wo)):
        w[j, :320] = ref[...]
        w[j, pl.ds(320 + here, 160)] = above[j]
        w[j, pl.ds(320 + there, 160)] = above2[j]
        w[j, pl.ds(640 + here, 160)] = below[j]
        w[j, pl.ds(640 + there, 160)] = below2[j]
    for start, width in CHUNKS:
        hidden_part(rows, w, acts, start, width)
    dn[...] = dot(acts[0], w[0]) + dot(acts[1], w[1])


def near_own(meta, *arrays):
    return local(
        near_own_kernel, 12,
        (((352, 640), F32), ((3, 352, 960), BF), ((3, 960, 640), BF)), arrays, (), (meta,),
    )


def near_other_kernel(own, other, own_dn, own_acts, w, dn, acts, rows, turned, half):
    for j in range(2):
        rows[j, :352] = own[j]
        rows[j, 352:] = other[j]
        turned[j] = rows[j].T
    for start, width in CHUNKS:
        hidden_part(other, w, half, start, width)
    dn[:352] = own_dn[...]
    dn[352:] = dot(half[0], w[0]) + dot(half[1], w[1])
    acts[:, :352] = own_acts[...]
    acts[:, 352:] = half[...]


def near_other(*arrays):
    return local(
        near_other_kernel, 14,
        (
            ((704, 640), F32), ((3, 704, 960), BF), ((2, 704, 640), BF), ((2, 640, 704), BF),
        ),
        arrays, [((3, 352, 960), BF)],
    )


def near_grads_kernel(meta, turned, acts, mine, send, keep):
    c = meta[1]
    for j in range(3):
        keep[...] = dot(turned[j // 2], acts[j]).reshape(8, 2, 40, 960)
        for out, side in ((mine, c), (send, 1 - c)):
            both = keep[:, side].reshape(320, 960)
            out[0, j] = both[:, :320].reshape(8, 40, 320).astype(BF)
            mid = pltpu.roll(both[:, 256:640], 320, 1)[:, :320]
            out[1, j] = mid.reshape(8, 40, 320).astype(BF)
            out[2, j] = both[:, 640:].reshape(8, 40, 320).astype(BF)


def near_grads(meta, turned, acts):
    grads = ((3, 3, 8, 40, 320), BF)
    return local(
        near_grads_kernel, 14, (grads, grads), (turned, acts),
        [((8, 2, 40, 960), F32)], (meta,),
    )


def split_gain(g):
    g = jnp.broadcast_to(g, (8, 640))
    low = g[:, :320]
    high = pltpu.roll(g[:, 256:], 320, 1)[:, :320]
    row = lax.broadcasted_iota(jnp.int32, (8, 320), 0)
    value = jnp.where(row % 2 == 0, low, high)
    top = value.astype(BF).astype(F32)
    return jnp.where(row < 2, top, jnp.where(row < 4, value - top, 0.0))


def resplit(g):
    row = lax.broadcasted_iota(jnp.int32, (8, 320), 0)
    value = jnp.where(row < 2, g, pltpu.roll(g, 2, 0))
    top = value.astype(BF).astype(F32)
    return jnp.where(row < 2, top, jnp.where(row < 4, value - top, 0.0))


def joined(rows):
    rows = rows.astype(F32)
    return rows + pltpu.roll(rows, 6, 0)


def far_kernel(meta, rows, gain, near_dn, first, second, dn, dn_send, acts, tail, w):
    c = meta[1]
    here = pl.multiple_of(c * 160, 16)
    there = pl.multiple_of((1 - c) * 160, 16)
    for j in range(3):
        w[j, pl.ds(here, 160)] = first[j]
        w[j, pl.ds(there, 160)] = second[j]
    hidden_part(rows, w, acts, 0, 320)
    total = near_dn[...] + dot(acts[0], w[0]) + dot(acts[1], w[1])
    dn[...] = total[:352]
    dn_send[...] = total[352:].astype(BF)
    gsum = jnp.sum(total * rows[0].astype(F32), axis=0, keepdims=True) / gain[...]
    tail[...] = split_gain(gsum)


def far_forward(meta, *arrays):
    return local(
        far_kernel, 14,
        (((352, 640), F32), ((352, 640), BF), ((3, 704, 320), BF), ((8, 320), F32)),
        arrays, [((3, 320, 640), BF)], (meta,),
    )


def far_grads_kernel(meta, turned, acts, tail, mine, send, keep):
    c = meta[1]
    for j in range(3):
        keep[...] = dot(turned[j // 2], acts[j]).reshape(8, 2, 40, 320)
        for out, side in ((mine, c), (send, 1 - c)):
            out[8 * j : 8 * j + 8] = keep[:, side].astype(BF)
    for out in (mine, send):
        out[24] = jnp.zeros((40, 320), BF)
        out[24, :8] = tail[...].astype(BF)


def far_grads(meta, turned, acts, tail):
    grads = ((25, 40, 320), BF)
    return local(
        far_grads_kernel, 10, (grads, grads), (turned, acts, tail),
        [((8, 2, 40, 320), F32)], (meta,),
    )


def finish_kernel(dest_g, dest_r, dn, got, lat, grad, gain, own, packed, sems):
    def sent(k):
        rank = dest_r[k]
        return (rank >= 0) & (rank < PLACES)

    for k in range(11):
        x_hat, inv_std = normalise(lat[k])
        d_hat = (dn[k] + got[k].astype(F32)) * gain[...]
        out = grad[1, k].astype(F32) + inv_std * (
            d_hat
            - jnp.mean(d_hat, axis=-1, keepdims=True)
            - x_hat * jnp.mean(d_hat * x_hat, axis=-1, keepdims=True)
        )
        own[k] = jnp.where(dest_r[k] >= 0, out, 0.0).astype(BF)

        @pl.when(sent(k))
        def _():
            place = dest_g[k] * PLACES + dest_r[k]
            pltpu.make_async_copy(own.at[k], packed.at[place], sems.at[k]).start()

    for k in range(11):

        @pl.when(sent(k))
        def _():
            pltpu.make_async_copy(own.at[k], packed.at[0], sems.at[k]).wait()


def finish(dest_g, dest_r, dn, got, lat, grad, gain):
    return pl.pallas_call(
        finish_kernel,
        out_shape=(
            jax.ShapeDtypeStruct((11, 32, 640), BF),
            jax.ShapeDtypeStruct((16 * PLACES, 32, 640), BF),
        ),
        in_specs=smem(2) + vmem(5),
        out_specs=(vmem(1)[0], pl.BlockSpec(memory_space=HBM)),
        scratch_shapes=[pltpu.SemaphoreType.DMA((11,))],
        compiler_params=grant(10),
        name="finish",
    )(dest_g, dest_r, dn, got, lat, grad, gain)


def unpack_kernel(src_p, src_r, came, placed, blank, sems):
    blank[...] = jnp.zeros_like(blank)
    for s in range(11):
        rank = src_r[s]

        @pl.when((rank >= 0) & (rank < PLACES))
        def _():
            pltpu.make_async_copy(
                came.at[src_p[s] * PLACES + rank], placed.at[s], sems.at[s]
            ).start()

        @pl.when((rank < 0) | (rank >= PLACES))
        def _():
            pltpu.make_async_copy(blank, placed.at[s], sems.at[s]).start()

    for s in range(11):
        pltpu.make_async_copy(blank, placed.at[s], sems.at[s]).wait()


def unpack(src_p, src_r, came):
    return pl.pallas_call(
        unpack_kernel,
        out_shape=jax.ShapeDtypeStruct((11, 32, 640), BF),
        in_specs=smem(2) + [pl.BlockSpec(memory_space=pl.ANY)],
        out_specs=pl.BlockSpec(memory_space=pl.ANY),
        scratch_shapes=[pltpu.VMEM((32, 640), BF), pltpu.SemaphoreType.DMA((11,))],
        compiler_params=grant(2),
        name="unpack",
    )(src_p, src_r, came)


def near_sums_kernel(mine, got, own, up, down):
    own[...] = mine[0].astype(F32) + got[0].astype(F32)
    up[...] = (mine[1].astype(F32) + got[1].astype(F32)).astype(BF)
    down[...] = (mine[2].astype(F32) + got[2].astype(F32)).astype(BF)


def far_sums_kernel(mine, got, lower, upper, tail):
    for j in range(3):
        for out, at in ((lower, 8 * j), (upper, 8 * j + 4)):
            out[j] = (mine[at : at + 4].astype(F32) + got[at : at + 4].astype(F32)).astype(BF)
    tail[...] = joined(mine[24, :8]) + joined(got[24, :8])


def over_y_kernel(meta, own, from_down, from_up, far_lower, far_upper, g0, g1, g2, g3,
                  keep, up, down, far, parts):
    for j in range(3):
        for half, came in ((0, far_lower), (4, far_upper)):
            at = slice(half, half + 4)
            x = own[j, at] + from_down[j, at].astype(F32)
            x = x + (from_up[j, at].astype(F32) + came[j].astype(F32))
            parts[half // 4, :, 5 * j : 5 * j + 5] = x.reshape(4, 5, 8, 320)
    tail = resplit((g0[...] + g1[...]) + (g2[...] + g3[...]))
    for k in range(2):
        for z in range(4):
            parts[k, z, 15] = tail
    z = meta[2]
    for out, step in ((keep, 0), (up, 1), (down, 3), (far, 2)):
        out[...] = parts[:, lax.rem(z + step, 4)].astype(out.dtype)


def over_z_kernel(meta, own, down, up, far, keep, give, sums):
    sums[...] = (own[...] + far[...].astype(F32)) + (down[...].astype(F32) + up[...].astype(F32))
    for k in range(2):
        sums[k, 15] = resplit(joined(sums[k, 15]))
    keep[...] = sums[meta[3]]
    give[...] = sums[1 - meta[3]].astype(BF)


def last_kernel(keep, got, value, gate, out, tail):
    total = keep[...] + got[...].astype(F32)
    for j, ref in enumerate((value, gate, out)):
        ref[...] = total[5 * j : 5 * j + 5].reshape(40, 320)
    tail[...] = joined(total[15])


def reduce_weights(meta, near_mine, near_got, far_mine, far_got):
    grads = (3, 8, 40, 320)
    half = (3, 4, 40, 320)
    row = ((8, 320), F32)
    own, up, down = local(
        near_sums_kernel, 4, ((grads, F32), (grads, BF), (grads, BF)),
        (near_mine, near_got),
    )
    from_down = ring(up, "y", 1)
    from_up = ring(down, "y", -1)
    lower, upper, tail = local(
        far_sums_kernel, 4, ((half, BF), (half, BF), row), (far_mine, far_got)
    )
    lower = ring(lower, "y", 1)
    upper = ring(upper, "y", -1)
    lower = ring(lower, "y", 1)
    upper = ring(upper, "y", -1)
    tail = tail + swap(tail, "xl")
    tails = [tail] + [ring(tail, "y", d) for d in (2, 1, -1)]
    part = (2, 16, 8, 320)
    own, up, down, far = local(
        over_y_kernel, 6, ((part, F32), (part, BF), (part, BF), (part, BF)),
        (own, from_down, from_up, lower, upper, *tails), [((2, 4, 16, 8, 320), F32)], (meta,),
    )
    came = ring(up, "z", 1), ring(down, "z", -1), ring(far, "z", 2)
    keep, give = local(
        over_z_kernel, 4, ((part[1:], F32), (part[1:], BF)), (own, *came),
        [(part, F32)], (meta,),
    )
    got = swap(give, "xh")
    out = ((40, 320), F32)
    value, gate, proj, tail = local(last_kernel, 2, (out, out, out, row), (keep, got))
    return value, gate, proj, tail[:2].reshape(640)


def route(packed):
    return lax.all_to_all(packed, DP, 0, 0, tiled=True)


def more_rounds(placed, own, most, dest_g, dest_r, src_p, src_r):
    def more(state):
        return state[0] < most[0]

    def one(state):
        t, placed = state
        groups = jnp.arange(16, dtype=jnp.int32)
        hit = (dest_g[None, :] == groups[:, None]) & (dest_r[None, :] == t)
        pick = jnp.sum(jnp.where(hit, jnp.arange(11, dtype=jnp.int32)[None, :], 0), axis=1)
        came = route(jnp.take(own, pick, axis=0))
        here = src_r == t
        new = jnp.take(came, jnp.where(here, src_p, 0), axis=0)
        return t + 1, jnp.where(here[:, None, None], new, placed)

    return lax.while_loop(more, one, (jnp.int32(PLACES), placed))[1]


def per_device(latents, cotangent, trunc, times, tmap, gain, w_value, w_gate, w_out):
    meta = jnp.stack([lax.axis_index(a) for a in (DP, "c", "z", "xh")]).astype(jnp.int32)
    gain = gain[None, :]
    wv, wg, wo = w_value.T, w_gate.T, w_out.T
    half = halves(meta, wv, wg, wo)
    below = ring(half, "y", 1)
    above = ring(half, "y", -1)
    rows = prologue(meta, trunc, times, noise_table(), latents, cotangent, gain)
    other = swap(rows, "xl")
    dest_g, dest_r, src_p, src_r, most = index_work(meta, trunc, tmap)
    below2 = swap(below, "c")
    above2 = swap(above, "c")
    first = ring(below, "y", 1)
    second = ring(above2, "y", -1)
    rows2 = rows.reshape(2, 352, 640)
    other = other.reshape(2, 352, 640)
    own_dn, own_acts, near_w = near_own(meta, rows2, wv, wg, wo, below, below2, above, above2)
    near_dn, near_acts, both, turned = near_other(rows2, other, own_dn, own_acts, near_w)
    near_mine, near_send = near_grads(meta, turned, near_acts)
    near_got = swap(near_send, "c")
    dn, dn_send, far_acts, tail = far_forward(meta, both, gain, near_dn, first, second)
    got = swap(dn_send, "xl")
    far_mine, far_send = far_grads(meta, turned, far_acts, tail)
    far_got = swap(far_send, "c")
    tiles = (11, 32, 640)
    own, packed = finish(
        dest_g, dest_r, dn.reshape(tiles), got.reshape(tiles), latents, rows, gain
    )
    came = route(packed)
    placed = unpack(src_p, src_r, came)
    placed = more_rounds(placed, own, most, dest_g, dest_r, src_p, src_r)
    grads = reduce_weights(meta, near_mine, near_got, far_mine, far_got)
    return placed, *grads


def solution(mesh):
    split = Mesh(mesh.devices.reshape(2, 4, 2, 4, 2), ("xh", "z", "c", "y", "xl"))
    tiles = P(DP, TENSOR, None)
    weights = P(None, TENSOR)

    def step(*args):
        return per_device(*args)

    step = jax.shard_map(
        step,
        mesh=split,
        in_specs=(tiles, tiles, P(), P(), P(), P(), weights, weights, weights),
        out_specs=(tiles, P(DP, TENSOR), P(DP, TENSOR), P(DP, TENSOR), P()),
        check_vma=False,
    )
    return step
```

```python
import jax
import jax.numpy as jnp
import numpy as np
from jax import lax
from jax.experimental import pallas as pl
from jax.experimental.pallas import tpu as pltpu
from jax.sharding import Mesh
from jax.sharding import PartitionSpec as P


TENSOR = ("y", "xl")
DP = ("xh", "z", "c")
EPS = 1e-05
PLACES = 3
BF = jnp.bfloat16
F32 = jnp.float32

VMEM = pltpu.MemorySpace.VMEM
SMEM = pltpu.MemorySpace.SMEM
HBM = pltpu.MemorySpace.HBM


def noise_table():
    betas = np.linspace(0.00085**0.5, 0.012**0.5, 1000) ** 2
    abar = np.exp(np.cumsum(np.log1p(-betas)))
    return jnp.asarray(np.sqrt(1.0 - abar), F32)


def swap(x, axis):
    return lax.ppermute(x, axis, [(0, 1), (1, 0)])


def ring(x, axis, step):
    return lax.ppermute(x, axis, [(i, (i + step) % 4) for i in range(4)])


def grant(mib):
    return pltpu.CompilerParams(vmem_limit_bytes=mib * 2**20)


def vmem(n):
    return [pl.BlockSpec(memory_space=VMEM)] * n


def smem(n):
    return [pl.BlockSpec(memory_space=SMEM)] * n


def index_kernel(meta, trunc, tmap, dest_g, dest_r, src_p, src_r, most, cnt):
    me = meta[0]

    def clear(i, _):
        cnt[i] = 0
        return 0

    lax.fori_loop(0, 256, clear, 0)

    def prompt(p, top):
        alive = trunc[p] - 29

        def slot(k, top):
            m = tmap[p * 11 + k]
            g = lax.div(m, 11)
            s = m - g * 11
            live = k < alive
            at = p * 16 + g
            r = cnt[at]

            @pl.when(live)
            def _():
                cnt[at] = r + 1

            rank = jnp.where(live, r, -1)

            @pl.when(p == me)
            def _():
                dest_g[k] = g
                dest_r[k] = rank

            @pl.when(g == me)
            def _():
                src_p[s] = p
                src_r[s] = rank

            return jnp.maximum(top, rank + 1)

        return lax.fori_loop(0, 11, slot, top)

    most[0] = lax.fori_loop(0, 16, prompt, jnp.int32(0))


def index_work(meta, trunc, tmap):
    i11 = jax.ShapeDtypeStruct((11,), jnp.int32)
    return pl.pallas_call(
        index_kernel,
        out_shape=(i11, i11, i11, i11, jax.ShapeDtypeStruct((1,), jnp.int32)),
        in_specs=smem(3),
        out_specs=tuple(smem(5)),
        scratch_shapes=[pltpu.SMEM((256,), jnp.int32)],
        compiler_params=grant(1),
        name="routes",
    )(meta, trunc, tmap)


def halves(c, *weights):
    return jnp.stack([lax.dynamic_slice_in_dim(w, c * 160, 160, 0) for w in weights])


def normalise(tile):
    x = tile.astype(F32)
    centred = x - jnp.mean(x, axis=-1, keepdims=True)
    inv_std = lax.rsqrt(jnp.mean(centred * centred, axis=-1, keepdims=True) + EPS)
    return centred * inv_std, inv_std


def prologue_kernel(meta, trunc, times, table, lat, cot, gain, rows):
    me = meta[0]
    alive = trunc[me] - 29
    for k in range(11):
        scale = jnp.where(k < alive, table[times[me * 11 + k]], 0.0)
        x_hat, _ = normalise(lat[k])
        rows[0, k] = (x_hat * gain[...]).astype(BF)
        rows[1, k] = (cot[k].astype(F32) * scale).astype(BF)


def prologue(meta, trunc, times, table, lat, cot, gain):
    return pl.pallas_call(
        prologue_kernel,
        out_shape=jax.ShapeDtypeStruct((2, 11, 32, 640), BF),
        in_specs=smem(4) + vmem(3),
        out_specs=vmem(1)[0],
        compiler_params=grant(10),
        name="prologue",
    )(meta, trunc, times, table, lat, cot, gain)


LAST = (((1,), (1,)), ((), ()))
PLAIN = (((1,), (0,)), ((), ()))


def dot(a, b, dims=PLAIN):
    return lax.dot_general(a, b, dims, preferred_element_type=F32)


def hidden_part(rows, w, acts, start, width):
    span = slice(start, start + width)
    value = dot(rows[0], w[0, span], LAST)
    gate = dot(rows[0], w[1, span], LAST)
    d_hidden = dot(rows[1], w[2, span], LAST)
    cdf = 0.5 * (1.0 + lax.erf(gate * 0.7071067811865476))
    density = jnp.exp(-0.5 * gate * gate) * 0.3989422804014327
    gelu = gate * cdf
    acts[0, :, span] = (d_hidden * gelu).astype(BF)
    acts[1, :, span] = (d_hidden * value * (cdf + gate * density)).astype(BF)
    acts[2, :, span] = (value * gelu).astype(BF)


def local(kernel, mib, out_shapes, arrays, scratch=(), scalars=()):
    out = pl.pallas_call(
        kernel,
        out_shape=tuple(jax.ShapeDtypeStruct(s, d) for s, d in out_shapes),
        in_specs=smem(len(scalars)) + vmem(len(arrays)),
        out_specs=tuple(vmem(len(out_shapes))),
        scratch_shapes=[pltpu.VMEM(s, d) for s, d in scratch],
        compiler_params=grant(mib),
    )(*scalars, *arrays)
    return out


CHUNKS = ((0, 256), (256, 256), (512, 256), (768, 192))


def near_own_kernel(meta, rows, wv, wg, wo, below, below2, above, above2, dn, acts, w):
    c = meta[1]
    here = pl.multiple_of(c * 160, 16)
    there = pl.multiple_of((1 - c) * 160, 16)
    for j, ref in enumerate((wv, wg, wo)):
        w[j, :320] = ref[...]
        w[j, pl.ds(320 + here, 160)] = above[j]
        w[j, pl.ds(320 + there, 160)] = above2[j]
        w[j, pl.ds(640 + here, 160)] = below[j]
        w[j, pl.ds(640 + there, 160)] = below2[j]
    for start, width in CHUNKS:
        hidden_part(rows, w, acts, start, width)
    dn[...] = dot(acts[0], w[0]) + dot(acts[1], w[1])


def near_own(meta, *arrays):
    return local(
        near_own_kernel, 12,
        (((352, 640), F32), ((3, 352, 960), BF), ((3, 960, 640), BF)), arrays, (), (meta,),
    )


def near_other_kernel(own, other, own_dn, own_acts, w, dn, acts, rows, turned, half):
    for j in range(2):
        rows[j, :352] = own[j]
        rows[j, 352:] = other[j]
        turned[j] = rows[j].T
    for start, width in CHUNKS:
        hidden_part(other, w, half, start, width)
    dn[:352] = own_dn[...]
    dn[352:] = dot(half[0], w[0]) + dot(half[1], w[1])
    acts[:, :352] = own_acts[...]
    acts[:, 352:] = half[...]


def near_other(*arrays):
    return local(
        near_other_kernel, 14,
        (
            ((704, 640), F32), ((3, 704, 960), BF), ((2, 704, 640), BF), ((2, 640, 704), BF),
        ),
        arrays, [((3, 352, 960), BF)],
    )


def near_grads_kernel(meta, turned, acts, mine, send, keep):
    c = meta[1]
    for j in range(3):
        keep[...] = dot(turned[j // 2], acts[j]).reshape(8, 2, 40, 960)
        for out, side in ((mine, c), (send, 1 - c)):
            both = keep[:, side].reshape(320, 960)
            out[0, j] = both[:, :320].reshape(8, 40, 320).astype(BF)
            mid = pltpu.roll(both[:, 256:640], 320, 1)[:, :320]
            out[1, j] = mid.reshape(8, 40, 320).astype(BF)
            out[2, j] = both[:, 640:].reshape(8, 40, 320).astype(BF)


def near_grads(meta, turned, acts):
    grads = ((3, 3, 8, 40, 320), BF)
    return local(
        near_grads_kernel, 14, (grads, grads), (turned, acts),
        [((8, 2, 40, 960), F32)], (meta,),
    )


def split_gain(g):
    g = jnp.broadcast_to(g, (8, 640))
    low = g[:, :320]
    high = pltpu.roll(g[:, 256:], 320, 1)[:, :320]
    row = lax.broadcasted_iota(jnp.int32, (8, 320), 0)
    value = jnp.where(row % 2 == 0, low, high)
    top = value.astype(BF).astype(F32)
    return jnp.where(row < 2, top, jnp.where(row < 4, value - top, 0.0))


def resplit(g):
    row = lax.broadcasted_iota(jnp.int32, (8, 320), 0)
    value = jnp.where(row < 2, g, pltpu.roll(g, 2, 0))
    top = value.astype(BF).astype(F32)
    return jnp.where(row < 2, top, jnp.where(row < 4, value - top, 0.0))


def joined(rows):
    rows = rows.astype(F32)
    return rows + pltpu.roll(rows, 6, 0)


def far_kernel(meta, rows, gain, near_dn, first, second, dn, dn_send, acts, tail, w):
    c = meta[1]
    here = pl.multiple_of(c * 160, 16)
    there = pl.multiple_of((1 - c) * 160, 16)
    for j in range(3):
        w[j, pl.ds(here, 160)] = first[j]
        w[j, pl.ds(there, 160)] = second[j]
    hidden_part(rows, w, acts, 0, 320)
    total = near_dn[...] + dot(acts[0], w[0]) + dot(acts[1], w[1])
    dn[...] = total[:352]
    dn_send[...] = total[352:].astype(BF)
    gsum = jnp.sum(total * rows[0].astype(F32), axis=0, keepdims=True) / gain[...]
    tail[...] = split_gain(gsum)


def far_forward(meta, *arrays):
    return local(
        far_kernel, 14,
        (((352, 640), F32), ((352, 640), BF), ((3, 704, 320), BF), ((8, 320), F32)),
        arrays, [((3, 320, 640), BF)], (meta,),
    )


def far_grads_kernel(meta, turned, acts, tail, mine, send, keep):
    c = meta[1]
    for j in range(3):
        keep[...] = dot(turned[j // 2], acts[j]).reshape(8, 2, 40, 320)
        for out, side in ((mine, c), (send, 1 - c)):
            out[8 * j : 8 * j + 8] = keep[:, side].astype(BF)
    for out in (mine, send):
        out[24] = jnp.zeros((40, 320), BF)
        out[24, :8] = tail[...].astype(BF)


def far_grads(meta, turned, acts, tail):
    grads = ((25, 40, 320), BF)
    return local(
        far_grads_kernel, 10, (grads, grads), (turned, acts, tail),
        [((8, 2, 40, 320), F32)], (meta,),
    )


def finish_kernel(dest_g, dest_r, dn, got, lat, grad, gain, own, packed, sems):
    def sent(k):
        rank = dest_r[k]
        return (rank >= 0) & (rank < PLACES)

    for k in range(11):
        x_hat, inv_std = normalise(lat[k])
        d_hat = (dn[k] + got[k].astype(F32)) * gain[...]
        out = grad[1, k].astype(F32) + inv_std * (
            d_hat
            - jnp.mean(d_hat, axis=-1, keepdims=True)
            - x_hat * jnp.mean(d_hat * x_hat, axis=-1, keepdims=True)
        )
        own[k] = jnp.where(dest_r[k] >= 0, out, 0.0).astype(BF)

        @pl.when(sent(k))
        def _():
            place = dest_g[k] * PLACES + dest_r[k]
            pltpu.make_async_copy(own.at[k], packed.at[place], sems.at[k]).start()

    for k in range(11):

        @pl.when(sent(k))
        def _():
            pltpu.make_async_copy(own.at[k], packed.at[0], sems.at[k]).wait()


def finish(dest_g, dest_r, dn, got, lat, grad, gain):
    return pl.pallas_call(
        finish_kernel,
        out_shape=(
            jax.ShapeDtypeStruct((11, 32, 640), BF),
            jax.ShapeDtypeStruct((16 * PLACES, 32, 640), BF),
        ),
        in_specs=smem(2) + vmem(5),
        out_specs=(vmem(1)[0], pl.BlockSpec(memory_space=HBM)),
        scratch_shapes=[pltpu.SemaphoreType.DMA((11,))],
        compiler_params=grant(10),
        name="finish",
    )(dest_g, dest_r, dn, got, lat, grad, gain)


def unpack_kernel(src_p, src_r, came, placed, blank, sems):
    blank[...] = jnp.zeros_like(blank)
    for s in range(11):
        rank = src_r[s]

        @pl.when((rank >= 0) & (rank < PLACES))
        def _():
            pltpu.make_async_copy(
                came.at[src_p[s] * PLACES + rank], placed.at[s], sems.at[s]
            ).start()

        @pl.when((rank < 0) | (rank >= PLACES))
        def _():
            pltpu.make_async_copy(blank, placed.at[s], sems.at[s]).start()

    for s in range(11):
        pltpu.make_async_copy(blank, placed.at[s], sems.at[s]).wait()


def unpack(src_p, src_r, came):
    return pl.pallas_call(
        unpack_kernel,
        out_shape=jax.ShapeDtypeStruct((11, 32, 640), BF),
        in_specs=smem(2) + [pl.BlockSpec(memory_space=pl.ANY)],
        out_specs=pl.BlockSpec(memory_space=pl.ANY),
        scratch_shapes=[pltpu.VMEM((32, 640), BF), pltpu.SemaphoreType.DMA((11,))],
        compiler_params=grant(2),
        name="unpack",
    )(src_p, src_r, came)


def near_sums_kernel(mine, got, own, up, down):
    own[...] = mine[0].astype(F32) + got[0].astype(F32)
    up[...] = (mine[1].astype(F32) + got[1].astype(F32)).astype(BF)
    down[...] = (mine[2].astype(F32) + got[2].astype(F32)).astype(BF)


def spread(parts, z, outs):
    for out, step in zip(outs, (0, 1, 3, 2)):
        out[...] = parts[:, lax.rem(z + step, 4)].astype(out.dtype)


def far_sums_kernel(meta, mine, got, keep, up, down, far, tail, parts):
    for j in range(3):
        x = mine[8 * j : 8 * j + 8].astype(F32) + got[8 * j : 8 * j + 8].astype(F32)
        parts[:, :, 5 * j : 5 * j + 5] = x.reshape(2, 4, 5, 8, 320)
    parts[:, :, 15] = jnp.zeros((2, 4, 8, 320), F32)
    spread(parts, meta[2], (keep, up, down, far))
    tail[...] = joined(mine[24, :8]) + joined(got[24, :8])


def far_z_kernel(own, down, up, far, out):
    x = (own[...] + far[...].astype(F32)) + (down[...].astype(F32) + up[...].astype(F32))
    out[...] = x.astype(BF)


def over_y_kernel(meta, own, from_down, from_up, g0, g1, g2, g3, keep, up, down, far, parts):
    for j in range(3):
        x = own[j] + from_down[j].astype(F32) + from_up[j].astype(F32)
        parts[:, :, 5 * j : 5 * j + 5] = x.reshape(2, 4, 5, 8, 320)
    tail = resplit((g0[...] + g1[...]) + (g2[...] + g3[...]))
    for k in range(2):
        for z in range(4):
            parts[k, z, 15] = tail
    spread(parts, meta[2], (keep, up, down, far))


def over_z_kernel(meta, own, down, up, far, across, keep, give, sums):
    sums[...] = (own[...] + far[...].astype(F32)) + (down[...].astype(F32) + up[...].astype(F32))
    for k in range(2):
        sums[k, :15] += across[k, :15].astype(F32)
        sums[k, 15] = resplit(joined(sums[k, 15]))
    keep[...] = sums[meta[3]]
    give[...] = sums[1 - meta[3]].astype(BF)


def last_kernel(keep, got, value, gate, out, tail):
    total = keep[...] + got[...].astype(F32)
    for j, ref in enumerate((value, gate, out)):
        ref[...] = total[5 * j : 5 * j + 5].reshape(40, 320)
    tail[...] = joined(total[15])


def over_ring(up, down, far):
    return ring(up, "z", 1), ring(down, "z", -1), ring(far, "z", 2)


def reduce_weights(meta, near_mine, near_got, far_mine, far_got):
    grads = (3, 8, 40, 320)
    row = ((8, 320), F32)
    part = (2, 16, 8, 320)
    parts = ((part, F32), (part, BF), (part, BF), (part, BF))
    whole = [((2, 4, 16, 8, 320), F32)]
    own, up, down = local(
        near_sums_kernel, 4, ((grads, F32), (grads, BF), (grads, BF)),
        (near_mine, near_got),
    )
    from_down = ring(up, "y", 1)
    from_up = ring(down, "y", -1)
    far_own, *far_sent, tail = local(
        far_sums_kernel, 6, (*parts, row), (far_mine, far_got), whole, (meta,)
    )
    tail = tail + swap(tail, "xl")
    came = over_ring(*far_sent)
    (across,) = local(far_z_kernel, 3, ((part, BF),), (far_own, *came))
    across = ring(across, "y", 2)
    tails = [tail] + [ring(tail, "y", d) for d in (2, 1, -1)]
    own, *sent = local(over_y_kernel, 6, parts, (own, from_down, from_up, *tails), whole, (meta,))
    came = over_ring(*sent)
    keep, give = local(
        over_z_kernel, 4, ((part[1:], F32), (part[1:], BF)), (own, *came, across),
        [(part, F32)], (meta,),
    )
    got = swap(give, "xh")
    out = ((40, 320), F32)
    value, gate, proj, tail = local(last_kernel, 2, (out, out, out, row), (keep, got))
    return value, gate, proj, tail[:2].reshape(640)


def route(packed):
    return lax.all_to_all(packed, DP, 0, 0, tiled=True)


def more_rounds(placed, own, most, dest_g, dest_r, src_p, src_r):
    def more(state):
        return state[0] < most[0]

    def one(state):
        t, placed = state
        groups = jnp.arange(16, dtype=jnp.int32)
        hit = (dest_g[None, :] == groups[:, None]) & (dest_r[None, :] == t)
        pick = jnp.sum(jnp.where(hit, jnp.arange(11, dtype=jnp.int32)[None, :], 0), axis=1)
        came = route(jnp.take(own, pick, axis=0))
        here = src_r == t
        new = jnp.take(came, jnp.where(here, src_p, 0), axis=0)
        return t + 1, jnp.where(here[:, None, None], new, placed)

    return lax.while_loop(more, one, (jnp.int32(PLACES), placed))[1]


def per_device(latents, cotangent, trunc, times, tmap, gain, w_value, w_gate, w_out):
    meta = jnp.stack([lax.axis_index(a) for a in (DP, "c", "z", "xh")]).astype(jnp.int32)
    gain = gain[None, :]
    wv, wg, wo = w_value.T, w_gate.T, w_out.T
    half = halves(lax.axis_index("c"), wv, wg, wo)
    below = ring(half, "y", 1)
    above = ring(half, "y", -1)
    rows = prologue(meta, trunc, times, noise_table(), latents, cotangent, gain)
    other = swap(rows, "xl")
    dest_g, dest_r, src_p, src_r, most = index_work(meta, trunc, tmap)
    below2 = swap(below, "c")
    above2 = swap(above, "c")
    first = ring(below, "y", 1)
    second = ring(above2, "y", -1)
    rows2 = rows.reshape(2, 352, 640)
    other = other.reshape(2, 352, 640)
    own_dn, own_acts, near_w = near_own(meta, rows2, wv, wg, wo, below, below2, above, above2)
    near_dn, near_acts, both, turned = near_other(rows2, other, own_dn, own_acts, near_w)
    near_mine, near_send = near_grads(meta, turned, near_acts)
    near_got = swap(near_send, "c")
    dn, dn_send, far_acts, tail = far_forward(meta, both, gain, near_dn, first, second)
    got = swap(dn_send, "xl")
    far_mine, far_send = far_grads(meta, turned, far_acts, tail)
    far_got = swap(far_send, "c")
    tiles = (11, 32, 640)
    own, packed = finish(
        dest_g, dest_r, dn.reshape(tiles), got.reshape(tiles), latents, rows, gain
    )
    came = route(packed)
    placed = unpack(src_p, src_r, came)
    placed = more_rounds(placed, own, most, dest_g, dest_r, src_p, src_r)
    grads = reduce_weights(meta, near_mine, near_got, far_mine, far_got)
    return placed, *grads


def solution(mesh):
    split = Mesh(mesh.devices.reshape(2, 4, 2, 4, 2), ("xh", "z", "c", "y", "xl"))
    tiles = P(DP, TENSOR, None)
    weights = P(None, TENSOR)

    def step(*args):
        return per_device(*args)

    step = jax.shard_map(
        step,
        mesh=split,
        in_specs=(tiles, tiles, P(), P(), P(), P(), weights, weights, weights),
        out_specs=(tiles, P(DP, TENSOR), P(DP, TENSOR), P(DP, TENSOR), P()),
        check_vma=False,
    )
    return step
```

```python
import jax
import jax.numpy as jnp
import numpy as np
from jax import lax
from jax.experimental import pallas as pl
from jax.experimental.pallas import tpu as pltpu
from jax.sharding import Mesh
from jax.sharding import PartitionSpec as P


TENSOR = ("y", "xl")
DP = ("xh", "z", "c")
CHIP = ("xh", "z")
EPS = 1e-05
PLACES = 4
BF = jnp.bfloat16
F32 = jnp.float32

VMEM = pltpu.MemorySpace.VMEM
SMEM = pltpu.MemorySpace.SMEM
HBM = pltpu.MemorySpace.HBM


def noise_table():
    betas = np.linspace(0.00085**0.5, 0.012**0.5, 1000) ** 2
    abar = np.exp(np.cumsum(np.log1p(-betas)))
    return jnp.asarray(np.sqrt(1.0 - abar), F32)


def swap(x, axis):
    return lax.ppermute(x, axis, [(0, 1), (1, 0)])


def ring(x, axis, step):
    return lax.ppermute(x, axis, [(i, (i + step) % 4) for i in range(4)])


def grant(mib):
    return pltpu.CompilerParams(vmem_limit_bytes=mib * 2**20)


def vmem(n):
    return [pl.BlockSpec(memory_space=VMEM)] * n


def smem(n):
    return [pl.BlockSpec(memory_space=SMEM)] * n


def index_kernel(meta, trunc, tmap, dest_g, dest_r, src_p, src_r, most, cnt):
    me = meta[0]

    def clear(i, _):
        cnt[i] = 0
        return 0

    lax.fori_loop(0, 256, clear, 0)

    def prompt(p, top):
        alive = trunc[p] - 29

        def slot(k, top):
            m = tmap[p * 11 + k]
            g = lax.div(m, 11)
            s = m - g * 11
            live = k < alive
            at = lax.shift_right_logical(p, 1) * 16 + g
            r = cnt[at]

            @pl.when(live)
            def _():
                cnt[at] = r + 1

            rank = jnp.where(live, r, -1)

            @pl.when(lax.shift_right_logical(p, 1) == lax.shift_right_logical(me, 1))
            def _():
                q = jnp.where(p == me, k, k + 11)
                dest_g[q] = lax.shift_right_logical(g, 1)
                dest_r[q] = jnp.where((g & 1) == (me & 1), rank, -1)

            @pl.when(g == me)
            def _():
                src_p[s] = lax.shift_right_logical(p, 1)
                src_r[s] = rank

            return jnp.maximum(top, rank + 1)

        return lax.fori_loop(0, 11, slot, top)

    most[0] = lax.fori_loop(0, 16, prompt, jnp.int32(0))


def index_work(meta, trunc, tmap):
    i11 = jax.ShapeDtypeStruct((11,), jnp.int32)
    i22 = jax.ShapeDtypeStruct((22,), jnp.int32)
    return pl.pallas_call(
        index_kernel,
        out_shape=(i22, i22, i11, i11, jax.ShapeDtypeStruct((1,), jnp.int32)),
        in_specs=smem(3),
        out_specs=tuple(smem(5)),
        scratch_shapes=[pltpu.SMEM((256,), jnp.int32)],
        compiler_params=grant(1),
        name="routes",
    )(meta, trunc, tmap)


def halves(c, *weights):
    return jnp.stack([lax.dynamic_slice_in_dim(w, c * 160, 160, 0) for w in weights])


def normalise(tile):
    x = tile.astype(F32)
    centred = x - jnp.mean(x, axis=-1, keepdims=True)
    inv_std = lax.rsqrt(jnp.mean(centred * centred, axis=-1, keepdims=True) + EPS)
    return centred * inv_std, inv_std


def prologue_kernel(meta, trunc, times, table, lat, cot, gain, rows):
    me = meta[0]
    alive = trunc[me] - 29
    for k in range(11):
        scale = jnp.where(k < alive, table[times[me * 11 + k]], 0.0)
        x_hat, _ = normalise(lat[k])
        rows[0, k] = (x_hat * gain[...]).astype(BF)
        rows[1, k] = (cot[k].astype(F32) * scale).astype(BF)


def prologue(meta, trunc, times, table, lat, cot, gain):
    return pl.pallas_call(
        prologue_kernel,
        out_shape=jax.ShapeDtypeStruct((2, 11, 32, 640), BF),
        in_specs=smem(4) + vmem(3),
        out_specs=vmem(1)[0],
        compiler_params=grant(10),
        name="prologue",
    )(meta, trunc, times, table, lat, cot, gain)


LAST = (((1,), (1,)), ((), ()))
PLAIN = (((1,), (0,)), ((), ()))


def dot(a, b, dims=PLAIN):
    return lax.dot_general(a, b, dims, preferred_element_type=F32)


def hidden_part(rows, w, acts, start, width):
    span = slice(start, start + width)
    value = dot(rows[0], w[0, span], LAST)
    gate = dot(rows[0], w[1, span], LAST)
    d_hidden = dot(rows[1], w[2, span], LAST)
    cdf = 0.5 * (1.0 + lax.erf(gate * 0.7071067811865476))
    density = jnp.exp(-0.5 * gate * gate) * 0.3989422804014327
    gelu = gate * cdf
    acts[0, :, span] = (d_hidden * gelu).astype(BF)
    acts[1, :, span] = (d_hidden * value * (cdf + gate * density)).astype(BF)
    acts[2, :, span] = (value * gelu).astype(BF)


def local(kernel, mib, out_shapes, arrays, scratch=(), scalars=()):
    out = pl.pallas_call(
        kernel,
        out_shape=tuple(jax.ShapeDtypeStruct(s, d) for s, d in out_shapes),
        in_specs=smem(len(scalars)) + vmem(len(arrays)),
        out_specs=tuple(vmem(len(out_shapes))),
        scratch_shapes=[pltpu.VMEM(s, d) for s, d in scratch],
        compiler_params=grant(mib),
    )(*scalars, *arrays)
    return out


CHUNKS = ((0, 256), (256, 256), (512, 256), (768, 192))


def near_own_kernel(meta, rows, wv, wg, wo, below, below2, above, above2, dn, acts, w):
    c = meta[1]
    here = pl.multiple_of(c * 160, 16)
    there = pl.multiple_of((1 - c) * 160, 16)
    for j, ref in enumerate((wv, wg, wo)):
        w[j, :320] = ref[...]
        w[j, pl.ds(320 + here, 160)] = above[j]
        w[j, pl.ds(320 + there, 160)] = above2[j]
        w[j, pl.ds(640 + here, 160)] = below[j]
        w[j, pl.ds(640 + there, 160)] = below2[j]
    for start, width in CHUNKS:
        hidden_part(rows, w, acts, start, width)
    dn[...] = dot(acts[0], w[0]) + dot(acts[1], w[1])


def near_own(meta, *arrays):
    return local(
        near_own_kernel, 12,
        (((352, 640), F32), ((3, 352, 960), BF), ((3, 960, 640), BF)), arrays, (), (meta,),
    )


def near_other_kernel(own, other, own_dn, own_acts, w, dn, acts, rows, turned, half):
    for j in range(2):
        rows[j, :352] = own[j]
        rows[j, 352:] = other[j]
        turned[j] = rows[j].T
    for start, width in CHUNKS:
        hidden_part(other, w, half, start, width)
    dn[:352] = own_dn[...]
    dn[352:] = dot(half[0], w[0]) + dot(half[1], w[1])
    acts[:, :352] = own_acts[...]
    acts[:, 352:] = half[...]


def near_other(*arrays):
    return local(
        near_other_kernel, 14,
        (
            ((704, 640), F32), ((3, 704, 960), BF), ((2, 704, 640), BF), ((2, 640, 704), BF),
        ),
        arrays, [((3, 352, 960), BF)],
    )


def near_grads_kernel(meta, turned, acts, mine, send, keep):
    c = meta[1]
    for j in range(3):
        keep[...] = dot(turned[j // 2], acts[j]).reshape(8, 2, 40, 960)
        for out, side in ((mine, c), (send, 1 - c)):
            both = keep[:, side].reshape(320, 960)
            out[0, j] = both[:, :320].reshape(8, 40, 320).astype(BF)
            mid = pltpu.roll(both[:, 256:640], 320, 1)[:, :320]
            out[1, j] = mid.reshape(8, 40, 320).astype(BF)
            out[2, j] = both[:, 640:].reshape(8, 40, 320).astype(BF)


def near_grads(meta, turned, acts):
    grads = ((3, 3, 8, 40, 320), BF)
    return local(
        near_grads_kernel, 14, (grads, grads), (turned, acts),
        [((8, 2, 40, 960), F32)], (meta,),
    )


def split_gain(g):
    g = jnp.broadcast_to(g, (8, 640))
    low = g[:, :320]
    high = pltpu.roll(g[:, 256:], 320, 1)[:, :320]
    row = lax.broadcasted_iota(jnp.int32, (8, 320), 0)
    value = jnp.where(row % 2 == 0, low, high)
    top = value.astype(BF).astype(F32)
    return jnp.where(row < 2, top, jnp.where(row < 4, value - top, 0.0))


def resplit(g):
    row = lax.broadcasted_iota(jnp.int32, (8, 320), 0)
    value = jnp.where(row < 2, g, pltpu.roll(g, 2, 0))
    top = value.astype(BF).astype(F32)
    return jnp.where(row < 2, top, jnp.where(row < 4, value - top, 0.0))


def joined(rows):
    rows = rows.astype(F32)
    return rows + pltpu.roll(rows, 6, 0)


def far_kernel(meta, rows, gain, near_dn, first, second, dn, dn_send, acts, tail, w):
    c = meta[1]
    here = pl.multiple_of(c * 160, 16)
    there = pl.multiple_of((1 - c) * 160, 16)
    for j in range(3):
        w[j, pl.ds(here, 160)] = first[j]
        w[j, pl.ds(there, 160)] = second[j]
    hidden_part(rows, w, acts, 0, 320)
    total = near_dn[...] + dot(acts[0], w[0]) + dot(acts[1], w[1])
    dn[...] = total[:352]
    dn_send[...] = total[352:].astype(BF)
    gsum = jnp.sum(total * rows[0].astype(F32), axis=0, keepdims=True) / gain[...]
    tail[...] = split_gain(gsum)


def far_forward(meta, *arrays):
    return local(
        far_kernel, 14,
        (((352, 640), F32), ((352, 640), BF), ((3, 704, 320), BF), ((8, 320), F32)),
        arrays, [((3, 320, 640), BF)], (meta,),
    )


def far_grads_kernel(meta, turned, acts, tail, mine, send, keep):
    c = meta[1]
    for j in range(3):
        keep[...] = dot(turned[j // 2], acts[j]).reshape(8, 2, 40, 320)
        for out, side in ((mine, c), (send, 1 - c)):
            out[8 * j : 8 * j + 8] = keep[:, side].astype(BF)
    for out in (mine, send):
        out[24] = jnp.zeros((40, 320), BF)
        out[24, :8] = tail[...].astype(BF)


def far_grads(meta, turned, acts, tail):
    grads = ((25, 40, 320), BF)
    return local(
        far_grads_kernel, 10, (grads, grads), (turned, acts, tail),
        [((8, 2, 40, 320), F32)], (meta,),
    )


def finish_kernel(alive, dn, got, lat, grad, gain, own):
    for k in range(11):
        x_hat, inv_std = normalise(lat[k])
        d_hat = (dn[k] + got[k].astype(F32)) * gain[...]
        out = grad[1, k].astype(F32) + inv_std * (
            d_hat
            - jnp.mean(d_hat, axis=-1, keepdims=True)
            - x_hat * jnp.mean(d_hat * x_hat, axis=-1, keepdims=True)
        )
        own[k] = jnp.where(k < alive[0], out, 0.0).astype(BF)


def finish(alive, *arrays):
    return local(finish_kernel, 10, (((11, 32, 640), BF),), arrays, (), (alive,))[0]


def pack_kernel(dest_g, dest_r, own, peer, packed, sems):
    def each(act):
        for q in range(22):
            rank = dest_r[q]

            @pl.when((rank >= 0) & (rank < PLACES))
            def _():
                tile = own.at[q] if q < 11 else peer.at[q - 11]
                act(pltpu.make_async_copy(tile, packed.at[dest_g[q] * PLACES + rank], sems.at[q]))

    each(lambda copy: copy.start())
    each(lambda copy: copy.wait())


def pack(dest_g, dest_r, own, peer):
    return pl.pallas_call(
        pack_kernel,
        out_shape=HBM((8 * PLACES, 32, 640), BF),
        in_specs=smem(2) + vmem(2),
        out_specs=pl.BlockSpec(memory_space=HBM),
        scratch_shapes=[pltpu.SemaphoreType.DMA((22,))],
        compiler_params=grant(3),
        name="pack",
    )(dest_g, dest_r, own, peer)


def unpack_kernel(src_p, src_r, came, placed, blank, sems):
    blank[...] = jnp.zeros_like(blank)
    for s in range(11):
        rank = src_r[s]

        @pl.when((rank >= 0) & (rank < PLACES))
        def _():
            pltpu.make_async_copy(
                came.at[src_p[s] * PLACES + rank], placed.at[s], sems.at[s]
            ).start()

        @pl.when((rank < 0) | (rank >= PLACES))
        def _():
            pltpu.make_async_copy(blank, placed.at[s], sems.at[s]).start()

    for s in range(11):
        pltpu.make_async_copy(blank, placed.at[s], sems.at[s]).wait()


def unpack(src_p, src_r, came):
    return pl.pallas_call(
        unpack_kernel,
        out_shape=jax.ShapeDtypeStruct((11, 32, 640), BF),
        in_specs=smem(2) + [pl.BlockSpec(memory_space=pl.ANY)],
        out_specs=pl.BlockSpec(memory_space=pl.ANY),
        scratch_shapes=[pltpu.VMEM((32, 640), BF), pltpu.SemaphoreType.DMA((11,))],
        compiler_params=grant(2),
        name="unpack",
    )(src_p, src_r, came)


def near_sums_kernel(mine, got, own, up, down):
    own[...] = mine[0].astype(F32) + got[0].astype(F32)
    up[...] = (mine[1].astype(F32) + got[1].astype(F32)).astype(BF)
    down[...] = (mine[2].astype(F32) + got[2].astype(F32)).astype(BF)


def spread(parts, z, outs):
    for out, step in zip(outs, (0, 1, 3, 2)):
        out[...] = parts[:, lax.rem(z + step, 4)].astype(out.dtype)


def far_sums_kernel(meta, mine, got, keep, up, down, far, tail, parts):
    for j in range(3):
        x = mine[8 * j : 8 * j + 8].astype(F32) + got[8 * j : 8 * j + 8].astype(F32)
        parts[:, :, 5 * j : 5 * j + 5] = x.reshape(2, 4, 5, 8, 320)
    parts[:, :, 15] = jnp.zeros((2, 4, 8, 320), F32)
    spread(parts, meta[2], (keep, up, down, far))
    tail[...] = joined(mine[24, :8]) + joined(got[24, :8])


def far_z_kernel(own, down, up, far, out):
    x = (own[...] + far[...].astype(F32)) + (down[...].astype(F32) + up[...].astype(F32))
    out[...] = x.astype(BF)


def over_y_kernel(meta, own, from_down, from_up, near, across, keep, up, down, far, parts):
    for j in range(3):
        x = own[j] + from_down[j].astype(F32) + from_up[j].astype(F32)
        parts[:, :, 5 * j : 5 * j + 5] = x.reshape(2, 4, 5, 8, 320)
    tail = resplit(near[...] + across[...])
    for k in range(2):
        for z in range(4):
            parts[k, z, 15] = tail
    spread(parts, meta[2], (keep, up, down, far))


def over_z_kernel(meta, own, down, up, far, across, keep, give, sums):
    sums[...] = (own[...] + far[...].astype(F32)) + (down[...].astype(F32) + up[...].astype(F32))
    for k in range(2):
        sums[k, :15] += across[k, :15].astype(F32)
        sums[k, 15] = resplit(joined(sums[k, 15]))
    keep[...] = sums[meta[3]]
    give[...] = sums[1 - meta[3]].astype(BF)


def last_kernel(keep, got, value, gate, out, tail):
    total = keep[...] + got[...].astype(F32)
    for j, ref in enumerate((value, gate, out)):
        ref[...] = total[5 * j : 5 * j + 5].reshape(40, 320)
    tail[...] = joined(total[15])


def over_ring(up, down, far):
    return ring(up, "z", 1), ring(down, "z", -1), ring(far, "z", 2)


def reduce_weights(meta, near_mine, near_got, far_mine, far_got):
    grads = (3, 8, 40, 320)
    row = ((8, 320), F32)
    part = (2, 16, 8, 320)
    parts = ((part, F32), (part, BF), (part, BF), (part, BF))
    whole = [((2, 4, 16, 8, 320), F32)]
    own, up, down = local(
        near_sums_kernel, 4, ((grads, F32), (grads, BF), (grads, BF)),
        (near_mine, near_got),
    )
    from_down = ring(up, "y", 1)
    from_up = ring(down, "y", -1)
    far_own, *far_sent, tail = local(
        far_sums_kernel, 6, (*parts, row), (far_mine, far_got), whole, (meta,)
    )
    tail = tail + swap(tail, "xl")
    came = over_ring(*far_sent)
    (across,) = local(far_z_kernel, 3, ((part, BF),), (far_own, *came))
    across = ring(across, "y", 2)
    tail = tail + lax.ppermute(tail, "y", [(0, 1), (1, 0), (2, 3), (3, 2)])
    across_y = lax.ppermute(tail, "y", [(0, 3), (3, 0), (1, 2), (2, 1)])
    own, *sent = local(
        over_y_kernel, 6, parts, (own, from_down, from_up, tail, across_y), whole, (meta,)
    )
    came = over_ring(*sent)
    keep, give = local(
        over_z_kernel, 4, ((part[1:], F32), (part[1:], BF)), (own, *came, across),
        [(part, F32)], (meta,),
    )
    got = swap(give, "xh")
    out = ((40, 320), F32)
    value, gate, proj, tail = local(last_kernel, 2, (out, out, out, row), (keep, got))
    return value, gate, proj, tail[:2].reshape(640)


def route(packed):
    return lax.all_to_all(packed, CHIP, 0, 0, tiled=True)


def more_rounds(placed, own, peer, most, dest_g, dest_r, src_p, src_r):
    def more(state):
        return state[0] < most[0]

    def one(state):
        t, placed = state
        groups = jnp.arange(8, dtype=jnp.int32)
        hit = (dest_g[None, :] == groups[:, None]) & (dest_r[None, :] == t)
        pick = jnp.sum(jnp.where(hit, jnp.arange(22, dtype=jnp.int32)[None, :], 0), axis=1)
        came = route(jnp.take(jnp.concatenate([own, peer]), pick, axis=0))
        here = src_r == t
        new = jnp.take(came, jnp.where(here, src_p, 0), axis=0)
        return t + 1, jnp.where(here[:, None, None], new, placed)

    return lax.while_loop(more, one, (jnp.int32(PLACES), placed))[1]


def per_device(latents, cotangent, trunc, times, tmap, gain, w_value, w_gate, w_out):
    meta = jnp.stack([lax.axis_index(a) for a in (DP, "c", "z", "xh")]).astype(jnp.int32)
    gain = gain[None, :]
    wv, wg, wo = w_value.T, w_gate.T, w_out.T
    half = halves(lax.axis_index("c"), wv, wg, wo)
    below = ring(half, "y", 1)
    above = ring(half, "y", -1)
    rows = prologue(meta, trunc, times, noise_table(), latents, cotangent, gain)
    other = swap(rows, "xl")
    dest_g, dest_r, src_p, src_r, most = index_work(meta, trunc, tmap)
    below2 = swap(below, "c")
    above2 = swap(above, "c")
    first = ring(below, "y", 1)
    second = ring(above2, "y", -1)
    rows2 = rows.reshape(2, 352, 640)
    other = other.reshape(2, 352, 640)
    own_dn, own_acts, near_w = near_own(meta, rows2, wv, wg, wo, below, below2, above, above2)
    near_dn, near_acts, both, turned = near_other(rows2, other, own_dn, own_acts, near_w)
    near_mine, near_send = near_grads(meta, turned, near_acts)
    near_got = swap(near_send, "c")
    dn, dn_send, far_acts, tail = far_forward(meta, both, gain, near_dn, first, second)
    got = swap(dn_send, "xl")
    far_mine, far_send = far_grads(meta, turned, far_acts, tail)
    far_got = swap(far_send, "c")
    tiles = (11, 32, 640)
    alive = lax.dynamic_slice_in_dim(trunc, lax.axis_index(DP), 1) - 29
    own = finish(alive, dn.reshape(tiles), got.reshape(tiles), latents, rows, gain)
    peer = swap(own, "c")
    packed = pack(dest_g, dest_r, own, peer)
    came = route(packed)
    placed = unpack(src_p, src_r, came)
    placed = more_rounds(placed, own, peer, most, dest_g, dest_r, src_p, src_r)
    grads = reduce_weights(meta, near_mine, near_got, far_mine, far_got)
    return placed, *grads


def solution(mesh):
    split = Mesh(mesh.devices.reshape(2, 4, 2, 4, 2), ("xh", "z", "c", "y", "xl"))
    tiles = P(DP, TENSOR, None)
    weights = P(None, TENSOR)

    def step(*args):
        return per_device(*args)

    step = jax.shard_map(
        step,
        mesh=split,
        in_specs=(tiles, tiles, P(), P(), P(), P(), weights, weights, weights),
        out_specs=(tiles, P(DP, TENSOR), P(DP, TENSOR), P(DP, TENSOR), P()),
        check_vma=False,
    )
    return step
```

```python
import jax
import jax.numpy as jnp
import numpy as np
from jax import lax
from jax.experimental import pallas as pl
from jax.experimental.pallas import tpu as pltpu
from jax.sharding import Mesh
from jax.sharding import PartitionSpec as P


TENSOR = ("y", "xl")
DP = ("xh", "z", "c")
CHIP = ("xh", "z")
EPS = 1e-05
PLACES = 4
BF = jnp.bfloat16
F32 = jnp.float32

VMEM = pltpu.MemorySpace.VMEM
SMEM = pltpu.MemorySpace.SMEM
HBM = pltpu.MemorySpace.HBM


def noise_table():
    betas = np.linspace(0.00085**0.5, 0.012**0.5, 1000) ** 2
    abar = np.exp(np.cumsum(np.log1p(-betas)))
    return jnp.asarray(np.sqrt(1.0 - abar), F32)


def swap(x, axis):
    return lax.ppermute(x, axis, [(0, 1), (1, 0)])


def ring(x, axis, step):
    return lax.ppermute(x, axis, [(i, (i + step) % 4) for i in range(4)])


def in_hbm(x):
    return pltpu.with_memory_space_constraint(x, HBM)


def grant(mib):
    return pltpu.CompilerParams(vmem_limit_bytes=mib * 2**20)


def vmem(n):
    return [pl.BlockSpec(memory_space=VMEM)] * n


def smem(n):
    return [pl.BlockSpec(memory_space=SMEM)] * n


def index_kernel(meta, trunc, tmap, dest_g, dest_r, src_p, src_r, most, cnt):
    me = meta[0]

    def clear(i, _):
        cnt[i] = 0
        return 0

    lax.fori_loop(0, 256, clear, 0)

    def prompt(p, top):
        alive = trunc[p] - 29

        def slot(k, top):
            m = tmap[p * 11 + k]
            g = lax.div(m, 11)
            s = m - g * 11
            live = k < alive
            at = lax.shift_right_logical(p, 1) * 16 + g
            r = cnt[at]

            @pl.when(live)
            def _():
                cnt[at] = r + 1

            rank = jnp.where(live, r, -1)

            @pl.when(lax.shift_right_logical(p, 1) == lax.shift_right_logical(me, 1))
            def _():
                q = jnp.where(p == me, k, k + 11)
                dest_g[q] = lax.shift_right_logical(g, 1)
                dest_r[q] = jnp.where((g & 1) == (me & 1), rank, -1)

            @pl.when(g == me)
            def _():
                src_p[s] = lax.shift_right_logical(p, 1)
                src_r[s] = rank

            return jnp.maximum(top, rank + 1)

        return lax.fori_loop(0, 11, slot, top)

    most[0] = lax.fori_loop(0, 16, prompt, jnp.int32(0))


def index_work(meta, trunc, tmap):
    i11 = jax.ShapeDtypeStruct((11,), jnp.int32)
    i22 = jax.ShapeDtypeStruct((22,), jnp.int32)
    return pl.pallas_call(
        index_kernel,
        out_shape=(i22, i22, i11, i11, jax.ShapeDtypeStruct((1,), jnp.int32)),
        in_specs=smem(3),
        out_specs=tuple(smem(5)),
        scratch_shapes=[pltpu.SMEM((256,), jnp.int32)],
        compiler_params=grant(1),
        name="routes",
    )(meta, trunc, tmap)


def halves_kernel(meta, wv, wg, wo, half, sems):
    start = pl.multiple_of(meta[1] * 160, 16)
    copies = [
        pltpu.make_async_copy(w.at[pl.ds(start, 160), :], half.at[j], sems.at[j])
        for j, w in enumerate((wv, wg, wo))
    ]
    for copy in copies:
        copy.start()
    for copy in copies:
        copy.wait()


def halves(meta, *weights):
    return pl.pallas_call(
        halves_kernel,
        out_shape=jax.ShapeDtypeStruct((3, 160, 640), BF),
        in_specs=smem(1) + [pl.BlockSpec(memory_space=HBM)] * 3,
        out_specs=vmem(1)[0],
        scratch_shapes=[pltpu.SemaphoreType.DMA((3,))],
        compiler_params=grant(4),
        name="halves",
    )(meta, *(in_hbm(w) for w in weights))


def normalise(tile):
    x = tile.astype(F32)
    centred = x - jnp.mean(x, axis=-1, keepdims=True)
    inv_std = lax.rsqrt(jnp.mean(centred * centred, axis=-1, keepdims=True) + EPS)
    return centred * inv_std, inv_std


def prologue_kernel(meta, trunc, times, table, lat, cot, gain, rows):
    me = meta[0]
    alive = trunc[me] - 29
    for k in range(11):
        scale = jnp.where(k < alive, table[times[me * 11 + k]], 0.0)
        x_hat, _ = normalise(lat[k])
        rows[0, k] = (x_hat * gain[...]).astype(BF)
        rows[1, k] = (cot[k].astype(F32) * scale).astype(BF)


def prologue(meta, trunc, times, table, lat, cot, gain):
    return pl.pallas_call(
        prologue_kernel,
        out_shape=jax.ShapeDtypeStruct((2, 11, 32, 640), BF),
        in_specs=smem(4) + vmem(3),
        out_specs=vmem(1)[0],
        compiler_params=grant(10),
        name="prologue",
    )(meta, *(in_hbm(x) for x in (trunc, times, table, lat, cot)), gain)


LAST = (((1,), (1,)), ((), ()))
PLAIN = (((1,), (0,)), ((), ()))


def dot(a, b, dims=PLAIN):
    return lax.dot_general(a, b, dims, preferred_element_type=F32)


def hidden_part(rows, w, acts, start, width):
    span = slice(start, start + width)
    value = dot(rows[0], w[0, span], LAST)
    gate = dot(rows[0], w[1, span], LAST)
    d_hidden = dot(rows[1], w[2, span], LAST)
    cdf = 0.5 * (1.0 + lax.erf(gate * 0.7071067811865476))
    density = jnp.exp(-0.5 * gate * gate) * 0.3989422804014327
    gelu = gate * cdf
    acts[0, :, span] = (d_hidden * gelu).astype(BF)
    acts[1, :, span] = (d_hidden * value * (cdf + gate * density)).astype(BF)
    acts[2, :, span] = (value * gelu).astype(BF)


def local(kernel, mib, out_shapes, arrays, scratch=(), scalars=()):
    out = pl.pallas_call(
        kernel,
        out_shape=tuple(jax.ShapeDtypeStruct(s, d) for s, d in out_shapes),
        in_specs=smem(len(scalars)) + vmem(len(arrays)),
        out_specs=tuple(vmem(len(out_shapes))),
        scratch_shapes=[pltpu.VMEM(s, d) for s, d in scratch],
        compiler_params=grant(mib),
    )(*scalars, *arrays)
    return out


CHUNKS = ((0, 256), (256, 256), (512, 256), (768, 192))


def near_own_kernel(meta, rows, wv, wg, wo, below, below2, above, above2, dn, acts, w):
    c = meta[1]
    here = pl.multiple_of(c * 160, 16)
    there = pl.multiple_of((1 - c) * 160, 16)
    for j, ref in enumerate((wv, wg, wo)):
        w[j, :320] = ref[...]
        w[j, pl.ds(320 + here, 160)] = above[j]
        w[j, pl.ds(320 + there, 160)] = above2[j]
        w[j, pl.ds(640 + here, 160)] = below[j]
        w[j, pl.ds(640 + there, 160)] = below2[j]
    for start, width in CHUNKS:
        hidden_part(rows, w, acts, start, width)
    dn[...] = dot(acts[0], w[0]) + dot(acts[1], w[1])


def near_own(meta, *arrays):
    return local(
        near_own_kernel, 12,
        (((352, 640), F32), ((3, 352, 960), BF), ((3, 960, 640), BF)), arrays, (), (meta,),
    )


def near_other_kernel(own, other, own_dn, own_acts, w, dn, acts, rows, turned, half):
    for j in range(2):
        rows[j, :352] = own[j]
        rows[j, 352:] = other[j]
        turned[j] = rows[j].T
    for start, width in CHUNKS:
        hidden_part(other, w, half, start, width)
    dn[:352] = own_dn[...]
    dn[352:] = dot(half[0], w[0]) + dot(half[1], w[1])
    acts[:, :352] = own_acts[...]
    acts[:, 352:] = half[...]


def near_other(*arrays):
    return local(
        near_other_kernel, 14,
        (
            ((704, 640), F32), ((3, 704, 960), BF), ((2, 704, 640), BF), ((2, 640, 704), BF),
        ),
        arrays, [((3, 352, 960), BF)],
    )


def near_grads_kernel(meta, turned, acts, mine, send, keep):
    c = meta[1]
    for j in range(3):
        keep[...] = dot(turned[j // 2], acts[j]).reshape(8, 2, 40, 960)
        for out, side in ((mine, c), (send, 1 - c)):
            both = keep[:, side].reshape(320, 960)
            out[0, j] = both[:, :320].reshape(8, 40, 320).astype(BF)
            mid = pltpu.roll(both[:, 256:640], 320, 1)[:, :320]
            out[1, j] = mid.reshape(8, 40, 320).astype(BF)
            out[2, j] = both[:, 640:].reshape(8, 40, 320).astype(BF)


def near_grads(meta, turned, acts):
    grads = ((3, 3, 8, 40, 320), BF)
    return local(
        near_grads_kernel, 14, (grads, grads), (turned, acts),
        [((8, 2, 40, 960), F32)], (meta,),
    )


def split_gain(g):
    g = jnp.broadcast_to(g, (8, 640))
    low = g[:, :320]
    high = pltpu.roll(g[:, 256:], 320, 1)[:, :320]
    row = lax.broadcasted_iota(jnp.int32, (8, 320), 0)
    value = jnp.where(row % 2 == 0, low, high)
    top = value.astype(BF).astype(F32)
    return jnp.where(row < 2, top, jnp.where(row < 4, value - top, 0.0))


def resplit(g):
    row = lax.broadcasted_iota(jnp.int32, (8, 320), 0)
    value = jnp.where(row < 2, g, pltpu.roll(g, 2, 0))
    top = value.astype(BF).astype(F32)
    return jnp.where(row < 2, top, jnp.where(row < 4, value - top, 0.0))


def joined(rows):
    rows = rows.astype(F32)
    return rows + pltpu.roll(rows, 6, 0)


def far_kernel(meta, rows, gain, near_dn, first, second, dn, dn_send, acts, tail, w):
    c = meta[1]
    here = pl.multiple_of(c * 160, 16)
    there = pl.multiple_of((1 - c) * 160, 16)
    for j in range(3):
        w[j, pl.ds(here, 160)] = first[j]
        w[j, pl.ds(there, 160)] = second[j]
    hidden_part(rows, w, acts, 0, 320)
    total = near_dn[...] + dot(acts[0], w[0]) + dot(acts[1], w[1])
    dn[...] = total[:352].reshape(11, 32, 640)
    dn_send[...] = total[352:].reshape(11, 32, 640).astype(BF)
    gsum = jnp.sum(total * rows[0].astype(F32), axis=0, keepdims=True) / gain[...]
    tail[...] = split_gain(gsum)


def far_forward(meta, *arrays):
    return local(
        far_kernel, 14,
        (((11, 32, 640), F32), ((11, 32, 640), BF), ((3, 704, 320), BF), ((8, 320), F32)),
        arrays, [((3, 320, 640), BF)], (meta,),
    )


def far_grads_kernel(meta, turned, acts, tail, mine, send, keep):
    c = meta[1]
    for j in range(3):
        keep[...] = dot(turned[j // 2], acts[j]).reshape(8, 2, 40, 320)
        for out, side in ((mine, c), (send, 1 - c)):
            out[8 * j : 8 * j + 8] = keep[:, side].astype(BF)
    for out in (mine, send):
        out[24] = jnp.zeros((40, 320), BF)
        out[24, :8] = tail[...].astype(BF)


def far_grads(meta, turned, acts, tail):
    grads = ((25, 40, 320), BF)
    return local(
        far_grads_kernel, 10, (grads, grads), (turned, acts, tail),
        [((8, 2, 40, 320), F32)], (meta,),
    )


def finish_kernel(meta, trunc, dn, got, lat, grad, gain, own):
    for k in range(11):
        x_hat, inv_std = normalise(lat[k])
        d_hat = (dn[k] + got[k].astype(F32)) * gain[...]
        out = grad[1, k].astype(F32) + inv_std * (
            d_hat
            - jnp.mean(d_hat, axis=-1, keepdims=True)
            - x_hat * jnp.mean(d_hat * x_hat, axis=-1, keepdims=True)
        )
        own[k] = jnp.where(k < trunc[meta[0]] - 29, out, 0.0).astype(BF)


def finish(meta, trunc, *arrays):
    return local(finish_kernel, 10, (((11, 32, 640), BF),), arrays, (), (meta, trunc))[0]


def pack_kernel(dest_g, dest_r, own, peer, packed, sems):
    def each(act):
        for q in range(22):
            rank = dest_r[q]

            @pl.when((rank >= 0) & (rank < PLACES))
            def _():
                tile = own.at[q] if q < 11 else peer.at[q - 11]
                act(pltpu.make_async_copy(tile, packed.at[dest_g[q] * PLACES + rank], sems.at[q]))

    each(lambda copy: copy.start())
    each(lambda copy: copy.wait())


def pack(dest_g, dest_r, own, peer):
    return pl.pallas_call(
        pack_kernel,
        out_shape=HBM((8 * PLACES, 32, 640), BF),
        in_specs=smem(2) + vmem(2),
        out_specs=pl.BlockSpec(memory_space=HBM),
        scratch_shapes=[pltpu.SemaphoreType.DMA((22,))],
        compiler_params=grant(3),
        name="pack",
    )(dest_g, dest_r, own, peer)


def unpack_kernel(src_p, src_r, came, placed, blank, sems):
    blank[...] = jnp.zeros_like(blank)
    for s in range(11):
        rank = src_r[s]

        @pl.when((rank >= 0) & (rank < PLACES))
        def _():
            pltpu.make_async_copy(
                came.at[src_p[s] * PLACES + rank], placed.at[s], sems.at[s]
            ).start()

        @pl.when((rank < 0) | (rank >= PLACES))
        def _():
            pltpu.make_async_copy(blank, placed.at[s], sems.at[s]).start()

    for s in range(11):
        pltpu.make_async_copy(blank, placed.at[s], sems.at[s]).wait()


def unpack(src_p, src_r, came):
    return pl.pallas_call(
        unpack_kernel,
        out_shape=jax.ShapeDtypeStruct((11, 32, 640), BF),
        in_specs=smem(2) + [pl.BlockSpec(memory_space=pl.ANY)],
        out_specs=pl.BlockSpec(memory_space=pl.ANY),
        scratch_shapes=[pltpu.VMEM((32, 640), BF), pltpu.SemaphoreType.DMA((11,))],
        compiler_params=grant(2),
        name="unpack",
    )(src_p, src_r, came)


def near_sums_kernel(mine, got, own, up, down):
    own[...] = mine[0].astype(F32) + got[0].astype(F32)
    up[...] = (mine[1].astype(F32) + got[1].astype(F32)).astype(BF)
    down[...] = (mine[2].astype(F32) + got[2].astype(F32)).astype(BF)


def spread(parts, z, outs):
    for out, step in zip(outs, (0, 1, 3, 2)):
        out[...] = parts[:, lax.rem(z + step, 4)].astype(out.dtype)


def far_sums_kernel(meta, mine, got, keep, up, down, far, tail, parts):
    for j in range(3):
        x = mine[8 * j : 8 * j + 8].astype(F32) + got[8 * j : 8 * j + 8].astype(F32)
        parts[:, :, 5 * j : 5 * j + 5] = x.reshape(2, 4, 5, 8, 320)
    parts[:, :, 15] = jnp.zeros((2, 4, 8, 320), F32)
    spread(parts, meta[2], (keep, up, down, far))
    tail[...] = joined(mine[24, :8]) + joined(got[24, :8])


def far_z_kernel(own, down, up, far, out):
    x = (own[...] + far[...].astype(F32)) + (down[...].astype(F32) + up[...].astype(F32))
    out[...] = x.astype(BF)


def over_y_kernel(meta, own, from_down, from_up, near, across, keep, up, down, far, parts):
    for j in range(3):
        x = own[j] + from_down[j].astype(F32) + from_up[j].astype(F32)
        parts[:, :, 5 * j : 5 * j + 5] = x.reshape(2, 4, 5, 8, 320)
    tail = resplit(near[...] + across[...])
    for k in range(2):
        for z in range(4):
            parts[k, z, 15] = tail
    spread(parts, meta[2], (keep, up, down, far))


def over_z_kernel(meta, own, down, up, far, across, keep, give, sums):
    sums[...] = (own[...] + far[...].astype(F32)) + (down[...].astype(F32) + up[...].astype(F32))
    for k in range(2):
        sums[k, :15] += across[k, :15].astype(F32)
        sums[k, 15] = resplit(joined(sums[k, 15]))
    keep[...] = sums[meta[3]]
    give[...] = sums[1 - meta[3]].astype(BF)


def last_kernel(keep, got, value, gate, out, tail):
    total = keep[...] + got[...].astype(F32)
    for j, ref in enumerate((value, gate, out)):
        ref[...] = total[5 * j : 5 * j + 5].reshape(40, 320)
    tail[...] = joined(total[15])


def over_ring(up, down, far):
    up = ring(up, "z", 1)
    down = ring(down, "z", -1)
    far = ring(far, "z", 2)
    return up, down, far


def reduce_weights(meta, near_mine, near_got, far_mine, far_got):
    grads = (3, 8, 40, 320)
    row = ((8, 320), F32)
    part = (2, 16, 8, 320)
    parts = ((part, F32), (part, BF), (part, BF), (part, BF))
    whole = [((2, 4, 16, 8, 320), F32)]
    own, up, down = local(
        near_sums_kernel, 4, ((grads, F32), (grads, BF), (grads, BF)),
        (near_mine, near_got),
    )
    from_down = ring(up, "y", 1)
    from_up = ring(down, "y", -1)
    far_own, *far_sent, tail = local(
        far_sums_kernel, 6, (*parts, row), (far_mine, far_got), whole, (meta,)
    )
    tail = tail + swap(tail, "xl")
    came = over_ring(*far_sent)
    (across,) = local(far_z_kernel, 3, ((part, BF),), (far_own, *came))
    across = ring(across, "y", 2)
    tail = tail + lax.ppermute(tail, "y", [(0, 1), (1, 0), (2, 3), (3, 2)])
    across_y = lax.ppermute(tail, "y", [(0, 3), (3, 0), (1, 2), (2, 1)])
    own, *sent = local(
        over_y_kernel, 6, parts, (own, from_down, from_up, tail, across_y), whole, (meta,)
    )
    came = over_ring(*sent)
    keep, give = local(
        over_z_kernel, 4, ((part[1:], F32), (part[1:], BF)), (own, *came, across),
        [(part, F32)], (meta,),
    )
    got = swap(give, "xh")
    out = ((40, 320), F32)
    value, gate, proj, tail = local(last_kernel, 2, (out, out, out, row), (keep, got))
    return value, gate, proj, tail[:2].reshape(640)


def route(packed):
    return lax.all_to_all(packed, CHIP, 0, 0, tiled=True)


def more_rounds(placed, own, peer, most, dest_g, dest_r, src_p, src_r):
    def more(state):
        return state[0] < most[0]

    def one(state):
        t, placed = state
        groups = jnp.arange(8, dtype=jnp.int32)
        hit = (dest_g[None, :] == groups[:, None]) & (dest_r[None, :] == t)
        pick = jnp.sum(jnp.where(hit, jnp.arange(22, dtype=jnp.int32)[None, :], 0), axis=1)
        came = route(jnp.take(jnp.concatenate([own, peer]), pick, axis=0))
        here = src_r == t
        new = jnp.take(came, jnp.where(here, src_p, 0), axis=0)
        return t + 1, jnp.where(here[:, None, None], new, placed)

    return lax.while_loop(more, one, (jnp.int32(PLACES), placed))[1]


def per_device(latents, cotangent, trunc, times, tmap, gain, w_value, w_gate, w_out):
    meta = jnp.stack([lax.axis_index(a) for a in (DP, "c", "z", "xh")]).astype(jnp.int32)
    gain = gain[None, :]
    wv, wg, wo = w_value.T, w_gate.T, w_out.T
    half = halves(meta, wv, wg, wo)
    below = ring(half, "y", 1)
    above = ring(half, "y", -1)
    rows = prologue(meta, trunc, times, noise_table(), latents, cotangent, gain)
    other = swap(rows, "xl")
    dest_g, dest_r, src_p, src_r, most = index_work(meta, trunc, tmap)
    below2 = swap(below, "c")
    above2 = swap(above, "c")
    first = ring(below, "y", 1)
    second = ring(above2, "y", -1)
    rows2 = rows.reshape(2, 352, 640)
    other = other.reshape(2, 352, 640)
    own_dn, own_acts, near_w = near_own(meta, rows2, wv, wg, wo, below, below2, above, above2)
    near_dn, near_acts, both, turned = near_other(rows2, other, own_dn, own_acts, near_w)
    near_mine, near_send = near_grads(meta, turned, near_acts)
    near_got = swap(near_send, "c")
    dn, dn_send, far_acts, tail = far_forward(meta, both, gain, near_dn, first, second)
    got = swap(dn_send, "xl")
    far_mine, far_send = far_grads(meta, turned, far_acts, tail)
    far_got = swap(far_send, "c")
    own = finish(meta, trunc, dn, got, latents, rows, gain)
    peer = swap(own, "c")
    packed = pack(dest_g, dest_r, own, peer)
    came = route(packed)
    placed = unpack(src_p, src_r, came)
    placed = more_rounds(placed, own, peer, most, dest_g, dest_r, src_p, src_r)
    grads = reduce_weights(meta, near_mine, near_got, far_mine, far_got)
    return placed, *grads


def solution(mesh):
    split = Mesh(mesh.devices.reshape(2, 4, 2, 4, 2), ("xh", "z", "c", "y", "xl"))
    tiles = P(DP, TENSOR, None)
    weights = P(None, TENSOR)

    def step(*args):
        return per_device(*args)

    step = jax.shard_map(
        step,
        mesh=split,
        in_specs=(tiles, tiles, P(), P(), P(), P(), weights, weights, weights),
        out_specs=(tiles, P(DP, TENSOR), P(DP, TENSOR), P(DP, TENSOR), P()),
        check_vma=False,
    )
    return step
```

```python
import jax
import jax.numpy as jnp
import numpy as np
from jax import lax
from jax.experimental import pallas as pl
from jax.experimental.pallas import tpu as pltpu
from jax.sharding import Mesh
from jax.sharding import PartitionSpec as P


TENSOR = ("y", "xl")
DP = ("xh", "z", "c")
CHIP = ("xh", "z")
EPS = 1e-05
PLACES = 4
BF = jnp.bfloat16
F32 = jnp.float32

VMEM = pltpu.MemorySpace.VMEM
SMEM = pltpu.MemorySpace.SMEM
HBM = pltpu.MemorySpace.HBM


def noise_table():
    betas = np.linspace(0.00085**0.5, 0.012**0.5, 1000) ** 2
    abar = np.exp(np.cumsum(np.log1p(-betas)))
    return jnp.asarray(np.sqrt(1.0 - abar), F32)


def swap(x, axis):
    return lax.ppermute(x, axis, [(0, 1), (1, 0)])


def ring(x, axis, step):
    return lax.ppermute(x, axis, [(i, (i + step) % 4) for i in range(4)])


def in_hbm(x):
    return pltpu.with_memory_space_constraint(x, HBM)


def grant(mib):
    return pltpu.CompilerParams(vmem_limit_bytes=mib * 2**20)


def vmem(n):
    return [pl.BlockSpec(memory_space=VMEM)] * n


def smem(n):
    return [pl.BlockSpec(memory_space=SMEM)] * n


def index_kernel(meta, trunc, tmap, dest_g, dest_r, src_p, src_r, most, cnt):
    me = meta[0]

    def clear(i, _):
        cnt[i] = 0
        return 0

    lax.fori_loop(0, 256, clear, 0)

    def prompt(p, top):
        alive = trunc[p] - 29

        def slot(k, top):
            m = tmap[p * 11 + k]
            g = lax.div(m, 11)
            s = m - g * 11
            live = k < alive
            at = lax.shift_right_logical(p, 1) * 16 + g
            r = cnt[at]

            @pl.when(live)
            def _():
                cnt[at] = r + 1

            rank = jnp.where(live, r, -1)

            @pl.when(lax.shift_right_logical(p, 1) == lax.shift_right_logical(me, 1))
            def _():
                q = jnp.where(p == me, k, k + 11)
                dest_g[q] = lax.shift_right_logical(g, 1)
                dest_r[q] = jnp.where((g & 1) == (me & 1), rank, -1)

            @pl.when(g == me)
            def _():
                src_p[s] = lax.shift_right_logical(p, 1)
                src_r[s] = rank

            return jnp.maximum(top, rank + 1)

        return lax.fori_loop(0, 11, slot, top)

    most[0] = lax.fori_loop(0, 16, prompt, jnp.int32(0))


def index_work(meta, trunc, tmap):
    i11 = jax.ShapeDtypeStruct((11,), jnp.int32)
    i22 = jax.ShapeDtypeStruct((22,), jnp.int32)
    return pl.pallas_call(
        index_kernel,
        out_shape=(i22, i22, i11, i11, jax.ShapeDtypeStruct((1,), jnp.int32)),
        in_specs=smem(3),
        out_specs=tuple(smem(5)),
        scratch_shapes=[pltpu.SMEM((256,), jnp.int32)],
        compiler_params=grant(1),
        name="routes",
    )(meta, trunc, tmap)


def halves_kernel(meta, wv, wg, wo, half, sems):
    start = pl.multiple_of(meta[1] * 160, 16)
    copies = [
        pltpu.make_async_copy(w.at[pl.ds(start, 160), :], half.at[j], sems.at[j])
        for j, w in enumerate((wv, wg, wo))
    ]
    for copy in copies:
        copy.start()
    for copy in copies:
        copy.wait()


def halves(meta, *weights):
    return pl.pallas_call(
        halves_kernel,
        out_shape=jax.ShapeDtypeStruct((3, 160, 640), BF),
        in_specs=smem(1) + [pl.BlockSpec(memory_space=HBM)] * 3,
        out_specs=vmem(1)[0],
        scratch_shapes=[pltpu.SemaphoreType.DMA((3,))],
        compiler_params=grant(4),
        name="halves",
    )(meta, *(in_hbm(w) for w in weights))


def normalise(tile):
    x = tile.astype(F32)
    centred = x - jnp.mean(x, axis=-1, keepdims=True)
    inv_std = lax.rsqrt(jnp.mean(centred * centred, axis=-1, keepdims=True) + EPS)
    return centred * inv_std, inv_std


def prologue_kernel(meta, trunc, times, table, lat, cot, gain, rows):
    me = meta[0]
    alive = trunc[me] - 29
    for k in range(11):
        scale = jnp.where(k < alive, table[times[me * 11 + k]], 0.0)
        x_hat, _ = normalise(lat[k])
        rows[0, k] = (x_hat * gain[...]).astype(BF)
        rows[1, k] = (cot[k].astype(F32) * scale).astype(BF)


def prologue(meta, trunc, times, table, lat, cot, gain):
    return pl.pallas_call(
        prologue_kernel,
        out_shape=jax.ShapeDtypeStruct((2, 11, 32, 640), BF),
        in_specs=smem(4) + vmem(3),
        out_specs=vmem(1)[0],
        compiler_params=grant(10),
        name="prologue",
    )(meta, *(in_hbm(x) for x in (trunc, times, table, lat, cot)), gain)


LAST = (((1,), (1,)), ((), ()))
PLAIN = (((1,), (0,)), ((), ()))


def dot(a, b, dims=PLAIN):
    return lax.dot_general(a, b, dims, preferred_element_type=F32)


def hidden_part(rows, w, acts, start, width):
    span = slice(start, start + width)
    value = dot(rows[0], w[0, span], LAST)
    gate = dot(rows[0], w[1, span], LAST)
    d_hidden = dot(rows[1], w[2, span], LAST)
    cdf = 0.5 * (1.0 + lax.erf(gate * 0.7071067811865476))
    density = jnp.exp(-0.5 * gate * gate) * 0.3989422804014327
    gelu = gate * cdf
    acts[0, :, span] = (d_hidden * gelu).astype(BF)
    acts[1, :, span] = (d_hidden * value * (cdf + gate * density)).astype(BF)
    acts[2, :, span] = (value * gelu).astype(BF)


def local(kernel, mib, out_shapes, arrays, scratch=(), scalars=()):
    out = pl.pallas_call(
        kernel,
        out_shape=tuple(jax.ShapeDtypeStruct(s, d) for s, d in out_shapes),
        in_specs=smem(len(scalars)) + vmem(len(arrays)),
        out_specs=tuple(vmem(len(out_shapes))),
        scratch_shapes=[pltpu.VMEM(s, d) for s, d in scratch],
        compiler_params=grant(mib),
    )(*scalars, *arrays)
    return out


CHUNKS = ((0, 256), (256, 256), (512, 256), (768, 192))


def near_own_kernel(meta, rows, wv, wg, wo, below, below2, above, above2, dn, acts, w):
    c = meta[1]
    here = pl.multiple_of(c * 160, 16)
    there = pl.multiple_of((1 - c) * 160, 16)
    for j, ref in enumerate((wv, wg, wo)):
        w[j, :320] = ref[...]
        w[j, pl.ds(320 + here, 160)] = above[j]
        w[j, pl.ds(320 + there, 160)] = above2[j]
        w[j, pl.ds(640 + here, 160)] = below[j]
        w[j, pl.ds(640 + there, 160)] = below2[j]
    for start, width in CHUNKS:
        hidden_part(rows, w, acts, start, width)
    dn[...] = dot(acts[0], w[0]) + dot(acts[1], w[1])


def near_own(meta, *arrays):
    return local(
        near_own_kernel, 12,
        (((352, 640), F32), ((3, 352, 960), BF), ((3, 960, 640), BF)), arrays, (), (meta,),
    )


def near_other_kernel(own, other, own_dn, own_acts, w, dn, acts, rows, turned, half):
    for j in range(2):
        rows[j, :352] = own[j]
        rows[j, 352:] = other[j]
        turned[j] = rows[j].T
    for start, width in CHUNKS:
        hidden_part(other, w, half, start, width)
    dn[:352] = own_dn[...]
    dn[352:] = dot(half[0], w[0]) + dot(half[1], w[1])
    acts[:, :352] = own_acts[...]
    acts[:, 352:] = half[...]


def near_other(*arrays):
    return local(
        near_other_kernel, 14,
        (
            ((704, 640), F32), ((3, 704, 960), BF), ((2, 704, 640), BF), ((2, 640, 704), BF),
        ),
        arrays, [((3, 352, 960), BF)],
    )


def near_grads_kernel(meta, turned, acts, mine, send, keep):
    c = meta[1]
    for j in range(3):
        keep[...] = dot(turned[j // 2], acts[j]).reshape(8, 2, 40, 960)
        for out, side in ((mine, c), (send, 1 - c)):
            both = keep[:, side].reshape(320, 960)
            out[0, j] = both[:, :320].reshape(8, 40, 320).astype(BF)
            mid = pltpu.roll(both[:, 256:640], 320, 1)[:, :320]
            out[1, j] = mid.reshape(8, 40, 320).astype(BF)
            out[2, j] = both[:, 640:].reshape(8, 40, 320).astype(BF)


def near_grads(meta, turned, acts):
    grads = ((3, 3, 8, 40, 320), BF)
    return local(
        near_grads_kernel, 14, (grads, grads), (turned, acts),
        [((8, 2, 40, 960), F32)], (meta,),
    )


def split_gain(g):
    g = jnp.broadcast_to(g, (8, 640))
    low = g[:, :320]
    high = pltpu.roll(g[:, 256:], 320, 1)[:, :320]
    row = lax.broadcasted_iota(jnp.int32, (8, 320), 0)
    value = jnp.where(row % 2 == 0, low, high)
    top = value.astype(BF).astype(F32)
    return jnp.where(row < 2, top, jnp.where(row < 4, value - top, 0.0))


def resplit(g):
    row = lax.broadcasted_iota(jnp.int32, (8, 320), 0)
    value = jnp.where(row < 2, g, pltpu.roll(g, 2, 0))
    top = value.astype(BF).astype(F32)
    return jnp.where(row < 2, top, jnp.where(row < 4, value - top, 0.0))


def joined(rows):
    rows = rows.astype(F32)
    return rows + pltpu.roll(rows, 6, 0)


def far_kernel(meta, rows, gain, near_dn, first, second, dn, dn_send, acts, tail, w):
    c = meta[1]
    here = pl.multiple_of(c * 160, 16)
    there = pl.multiple_of((1 - c) * 160, 16)
    for j in range(3):
        w[j, pl.ds(here, 160)] = first[j]
        w[j, pl.ds(there, 160)] = second[j]
    hidden_part(rows, w, acts, 0, 320)
    total = near_dn[...] + dot(acts[0], w[0]) + dot(acts[1], w[1])
    dn[...] = total[:352].reshape(11, 32, 640)
    dn_send[...] = total[352:].reshape(11, 32, 640).astype(BF)
    gsum = jnp.sum(total * rows[0].astype(F32), axis=0, keepdims=True) / gain[...]
    tail[...] = joined(split_gain(gsum))


def far_forward(meta, *arrays):
    return local(
        far_kernel, 14,
        (((11, 32, 640), F32), ((11, 32, 640), BF), ((3, 704, 320), BF), ((8, 320), F32)),
        arrays, [((3, 320, 640), BF)], (meta,),
    )


def far_grads_kernel(meta, turned, acts, tail, mine, send, keep):
    c = meta[1]
    for j in range(3):
        keep[...] = dot(turned[j // 2], acts[j]).reshape(8, 2, 40, 320)
        for out, side in ((mine, c), (send, 1 - c)):
            out[8 * j : 8 * j + 8] = keep[:, side].astype(BF)
    for out in (mine, send):
        out[24] = jnp.zeros((40, 320), BF)
        out[24, :8] = resplit(tail[...]).astype(BF)


def far_grads(meta, turned, acts, tail):
    grads = ((25, 40, 320), BF)
    return local(
        far_grads_kernel, 10, (grads, grads), (turned, acts, tail),
        [((8, 2, 40, 320), F32)], (meta,),
    )


def finish_kernel(meta, trunc, dn, got, lat, grad, gain, own):
    for k in range(11):
        x_hat, inv_std = normalise(lat[k])
        d_hat = (dn[k] + got[k].astype(F32)) * gain[...]
        out = grad[1, k].astype(F32) + inv_std * (
            d_hat
            - jnp.mean(d_hat, axis=-1, keepdims=True)
            - x_hat * jnp.mean(d_hat * x_hat, axis=-1, keepdims=True)
        )
        own[k] = jnp.where(k < trunc[meta[0]] - 29, out, 0.0).astype(BF)


def finish(meta, trunc, *arrays):
    return local(finish_kernel, 10, (((11, 32, 640), BF),), arrays, (), (meta, trunc))[0]


def pack_kernel(dest_g, dest_r, own, peer, packed, sems):
    def each(act):
        for q in range(22):
            rank = dest_r[q]

            @pl.when((rank >= 0) & (rank < PLACES))
            def _():
                tile = own.at[q] if q < 11 else peer.at[q - 11]
                act(pltpu.make_async_copy(tile, packed.at[dest_g[q] * PLACES + rank], sems.at[q]))

    each(lambda copy: copy.start())
    each(lambda copy: copy.wait())


def pack(dest_g, dest_r, own, peer):
    return pl.pallas_call(
        pack_kernel,
        out_shape=HBM((8 * PLACES, 32, 640), BF),
        in_specs=smem(2) + vmem(2),
        out_specs=pl.BlockSpec(memory_space=HBM),
        scratch_shapes=[pltpu.SemaphoreType.DMA((22,))],
        compiler_params=grant(3),
        name="pack",
    )(dest_g, dest_r, own, peer)


def unpack_kernel(src_p, src_r, came, placed, blank, sems):
    blank[...] = jnp.zeros_like(blank)
    for s in range(11):
        rank = src_r[s]

        @pl.when((rank >= 0) & (rank < PLACES))
        def _():
            pltpu.make_async_copy(
                came.at[src_p[s] * PLACES + rank], placed.at[s], sems.at[s]
            ).start()

        @pl.when((rank < 0) | (rank >= PLACES))
        def _():
            pltpu.make_async_copy(blank, placed.at[s], sems.at[s]).start()

    for s in range(11):
        pltpu.make_async_copy(blank, placed.at[s], sems.at[s]).wait()


def unpack(src_p, src_r, came):
    return pl.pallas_call(
        unpack_kernel,
        out_shape=jax.ShapeDtypeStruct((11, 32, 640), BF),
        in_specs=smem(2) + [pl.BlockSpec(memory_space=pl.ANY)],
        out_specs=pl.BlockSpec(memory_space=pl.ANY),
        scratch_shapes=[pltpu.VMEM((32, 640), BF), pltpu.SemaphoreType.DMA((11,))],
        compiler_params=grant(2),
        name="unpack",
    )(src_p, src_r, came)


def near_sums_kernel(mine, got, own, up, down):
    own[...] = mine[0].astype(F32) + got[0].astype(F32)
    up[...] = (mine[1].astype(F32) + got[1].astype(F32)).astype(BF)
    down[...] = (mine[2].astype(F32) + got[2].astype(F32)).astype(BF)


def spread(parts, z, outs):
    for out, step in zip(outs, (0, 1, 3, 2)):
        out[...] = parts[:, lax.rem(z + step, 4)].astype(out.dtype)


def far_sums_kernel(meta, mine, got, keep, up, down, far, parts):
    for j in range(3):
        x = mine[8 * j : 8 * j + 8].astype(F32) + got[8 * j : 8 * j + 8].astype(F32)
        parts[:, :, 5 * j : 5 * j + 5] = x.reshape(2, 4, 5, 8, 320)
    tail = resplit(joined(mine[24, :8]) + joined(got[24, :8]))
    for k in range(2):
        for z in range(4):
            parts[k, z, 15] = tail
    spread(parts, meta[2], (keep, up, down, far))


def far_z_kernel(own, down, up, far, out, tail):
    x = (own[...] + far[...].astype(F32)) + (down[...].astype(F32) + up[...].astype(F32))
    out[...] = x.astype(BF)
    tail[...] = joined(x[0, 15])


def over_y_kernel(meta, own, from_down, from_up, keep, up, down, far, parts):
    for j in range(3):
        x = own[j] + from_down[j].astype(F32) + from_up[j].astype(F32)
        parts[:, :, 5 * j : 5 * j + 5] = x.reshape(2, 4, 5, 8, 320)
    parts[:, :, 15] = jnp.zeros((2, 4, 8, 320), F32)
    spread(parts, meta[2], (keep, up, down, far))


def over_z_kernel(meta, own, down, up, far, across, gain, gain2, keep, give, sums):
    sums[...] = (own[...] + far[...].astype(F32)) + (down[...].astype(F32) + up[...].astype(F32))
    for k in range(2):
        sums[k, :15] += across[k, :15].astype(F32)
        sums[k, 15] = resplit(gain[...] + gain2[...])
    keep[...] = sums[meta[3]]
    give[...] = sums[1 - meta[3]].astype(BF)


def last_kernel(keep, got, value, gate, out, tail):
    total = keep[...] + got[...].astype(F32)
    for j, ref in enumerate((value, gate, out)):
        ref[...] = total[5 * j : 5 * j + 5].reshape(40, 320)
    tail[...] = joined(total[15])


def over_ring(up, down, far):
    up = ring(up, "z", 1)
    down = ring(down, "z", -1)
    far = ring(far, "z", 2)
    return up, down, far


def reduce_weights(meta, near_mine, near_got, far_mine, far_got):
    grads = (3, 8, 40, 320)
    row = ((8, 320), F32)
    part = (2, 16, 8, 320)
    parts = ((part, F32), (part, BF), (part, BF), (part, BF))
    whole = [((2, 4, 16, 8, 320), F32)]
    own, up, down = local(
        near_sums_kernel, 4, ((grads, F32), (grads, BF), (grads, BF)),
        (near_mine, near_got),
    )
    from_down = ring(up, "y", 1)
    from_up = ring(down, "y", -1)
    far_own, *far_sent = local(far_sums_kernel, 6, parts, (far_mine, far_got), whole, (meta,))
    came = over_ring(*far_sent)
    across, tail = local(far_z_kernel, 3, ((part, BF), row), (far_own, *came))
    across = ring(across, "y", 2)
    tail = tail + lax.ppermute(tail, "y", [(0, 1), (1, 0), (2, 3), (3, 2)])
    tail2 = lax.ppermute(tail, "y", [(0, 3), (3, 0), (1, 2), (2, 1)])
    own, *sent = local(over_y_kernel, 6, parts, (own, from_down, from_up), whole, (meta,))
    came = over_ring(*sent)
    keep, give = local(
        over_z_kernel, 4, ((part[1:], F32), (part[1:], BF)), (own, *came, across, tail, tail2),
        [(part, F32)], (meta,),
    )
    got = swap(give, "xh")
    out = ((40, 320), F32)
    value, gate, proj, tail = local(last_kernel, 2, (out, out, out, row), (keep, got))
    return value, gate, proj, tail[:2].reshape(640)


def route(packed):
    return lax.all_to_all(packed, CHIP, 0, 0, tiled=True)


def more_rounds(placed, own, peer, most, dest_g, dest_r, src_p, src_r):
    def more(state):
        return state[0] < most[0]

    def one(state):
        t, placed = state
        groups = jnp.arange(8, dtype=jnp.int32)
        hit = (dest_g[None, :] == groups[:, None]) & (dest_r[None, :] == t)
        pick = jnp.sum(jnp.where(hit, jnp.arange(22, dtype=jnp.int32)[None, :], 0), axis=1)
        came = route(jnp.take(jnp.concatenate([own, peer]), pick, axis=0))
        here = src_r == t
        new = jnp.take(came, jnp.where(here, src_p, 0), axis=0)
        return t + 1, jnp.where(here[:, None, None], new, placed)

    return lax.while_loop(more, one, (jnp.int32(PLACES), placed))[1]


def per_device(latents, cotangent, trunc, times, tmap, gain, w_value, w_gate, w_out):
    meta = jnp.stack([lax.axis_index(a) for a in (DP, "c", "z", "xh")]).astype(jnp.int32)
    gain = gain[None, :]
    wv, wg, wo = w_value.T, w_gate.T, w_out.T
    half = halves(meta, wv, wg, wo)
    below = ring(half, "y", 1)
    above = ring(half, "y", -1)
    rows = prologue(meta, trunc, times, noise_table(), latents, cotangent, gain)
    other = swap(rows, "xl")
    dest_g, dest_r, src_p, src_r, most = index_work(meta, trunc, tmap)
    below2 = swap(below, "c")
    above2 = swap(above, "c")
    first = ring(below, "y", 1)
    second = ring(above2, "y", -1)
    rows2 = rows.reshape(2, 352, 640)
    other = other.reshape(2, 352, 640)
    own_dn, own_acts, near_w = near_own(meta, rows2, wv, wg, wo, below, below2, above, above2)
    near_dn, near_acts, both, turned = near_other(rows2, other, own_dn, own_acts, near_w)
    near_mine, near_send = near_grads(meta, turned, near_acts)
    near_got = swap(near_send, "c")
    dn, dn_send, far_acts, tail = far_forward(meta, both, gain, near_dn, first, second)
    tail = tail + swap(tail, "xl")
    got = swap(dn_send, "xl")
    far_mine, far_send = far_grads(meta, turned, far_acts, tail)
    far_got = swap(far_send, "c")
    own = finish(meta, trunc, dn, got, latents, rows, gain)
    peer = swap(own, "c")
    packed = pack(dest_g, dest_r, own, peer)
    came = route(packed)
    placed = unpack(src_p, src_r, came)
    placed = more_rounds(placed, own, peer, most, dest_g, dest_r, src_p, src_r)
    grads = reduce_weights(meta, near_mine, near_got, far_mine, far_got)
    return placed, *grads


def solution(mesh):
    split = Mesh(mesh.devices.reshape(2, 4, 2, 4, 2), ("xh", "z", "c", "y", "xl"))
    tiles = P(DP, TENSOR, None)
    weights = P(None, TENSOR)

    def step(*args):
        return per_device(*args)

    step = jax.shard_map(
        step,
        mesh=split,
        in_specs=(tiles, tiles, P(), P(), P(), P(), weights, weights, weights),
        out_specs=(tiles, P(DP, TENSOR), P(DP, TENSOR), P(DP, TENSOR), P()),
        check_vma=False,
    )
    return step
```
